8 devices in a mesh: dp: 1 (over z), sp2: 2 (over y), sp: 4 (over x, core).
Axes of the slice: x: 2, y: 2, z: 1, core: 2. Of those that a mesh axis runs over, the one named last changes fastest.
Arguments:
- x: bfloat16 [4, 64, 64, 640], P('dp', 'sp', 'sp2')
- time_emb: bfloat16 [4, 1280], P('dp')
- gn_scale: bfloat16 [5, 640], replicated
- gn_shift: bfloat16 [5, 640], replicated
- conv_w: bfloat16 [4, 3, 3, 640, 640], replicated
- time_w: bfloat16 [2, 1280, 640], replicated
- w_qkv: bfloat16 [3, 640, 8, 80], replicated
- w_out: bfloat16 [8, 80, 640], replicated
Outputs:
- output: bfloat16 [4, 64, 64, 640], P('dp', 'sp', 'sp2')
All inputs are finite; a program needn't handle non-finite values.
Results may differ from the reference program's by a relative error of at most 0.0115244.
Values are sent between devices in bfloat16 or wider.
A program may use at most 1 GiB of HBM per device.

```python
import jax
import jax.numpy as jnp
from jax import lax

IMAGES = 4
LAT_ROWS = 64
LAT_COLS = 64
CHANNELS = 640
NUM_HEADS = 8
TEMB_DIM = 1280
QUERY_BLOCK = 512
GROUPS = 32
NORM_EPS = 1e-5


def setup_inputs(seed: int = 0, part: int = 0) -> dict:
    base = jax.random.key(seed)
    part_keys = jax.random.split(jax.random.fold_in(base, part), 4)
    shared = jax.random.split(base, 6)
    head_dim = CHANNELS // NUM_HEADS
    ramp_rows = (jnp.arange(LAT_ROWS, dtype=jnp.float32) + 0.5) / LAT_ROWS * 2.0 - 1.0
    ramp_cols = (jnp.arange(LAT_COLS, dtype=jnp.float32) + 0.5) / LAT_COLS * 2.0 - 1.0
    slope_rows = jax.random.normal(part_keys[0], (IMAGES, 1, 1, CHANNELS), jnp.float32)
    slope_cols = jax.random.normal(part_keys[1], (IMAGES, 1, 1, CHANNELS), jnp.float32)
    noise = jax.random.normal(part_keys[2], (IMAGES, LAT_ROWS, LAT_COLS, CHANNELS), jnp.float32)
    latent = noise + 1.2 * (slope_rows * ramp_rows[None, :, None, None] + slope_cols * ramp_cols[None, None, :, None])
    time_emb = jax.random.normal(part_keys[3], (IMAGES, TEMB_DIM), jnp.float32)
    gn_scale = 1.0 + 0.3 * jax.random.normal(shared[0], (5, CHANNELS), jnp.float32)
    gn_shift = 0.5 * jax.random.normal(shared[1], (5, CHANNELS), jnp.float32)
    conv_w = jax.random.normal(shared[2], (4, 3, 3, CHANNELS, CHANNELS), jnp.float32) * (9 * CHANNELS) ** -0.5
    time_w = jax.random.normal(shared[3], (2, TEMB_DIM, CHANNELS), jnp.float32) * TEMB_DIM ** -0.5
    qkv_gain = jnp.array([1.5, 1.5, 1.0], jnp.float32)[:, None, None, None]
    w_qkv = jax.random.normal(shared[4], (3, CHANNELS, NUM_HEADS, head_dim), jnp.float32) * CHANNELS ** -0.5 * qkv_gain
    w_out = jax.random.normal(shared[5], (NUM_HEADS, head_dim, CHANNELS), jnp.float32) * CHANNELS ** -0.5
    return {
        "x": latent.astype(jnp.bfloat16),
        "time_emb": time_emb.astype(jnp.bfloat16),
        "gn_scale": gn_scale.astype(jnp.bfloat16),
        "gn_shift": gn_shift.astype(jnp.bfloat16),
        "conv_w": conv_w.astype(jnp.bfloat16),
        "time_w": time_w.astype(jnp.bfloat16),
        "w_qkv": w_qkv.astype(jnp.bfloat16),
        "w_out": w_out.astype(jnp.bfloat16),
    }


def group_norm(latent, scale, shift):
    batch, height, width, channels = latent.shape
    grouped = latent.astype(jnp.float32).reshape(batch, height, width, GROUPS, channels // GROUPS)
    mean = jnp.mean(grouped, axis=(1, 2, 4), keepdims=True)
    mean_sq = jnp.mean(grouped * grouped, axis=(1, 2, 4), keepdims=True)
    normed = (grouped - mean) * lax.rsqrt(mean_sq - mean * mean + NORM_EPS)
    return normed.reshape(latent.shape) * scale.astype(jnp.float32) + shift.astype(jnp.float32)


def conv3x3(latent, kernel):
    return lax.conv_general_dilated(latent.astype(jnp.float32), kernel.astype(jnp.float32), (1, 1), "SAME", dimension_numbers=("NHWC", "HWIO", "NHWC"))


def res_block(latent, time_vec, gn_scale, gn_shift, conv_w, norm_idx, conv_idx):
    first = jax.nn.silu(group_norm(latent, gn_scale[norm_idx], gn_shift[norm_idx])).astype(jnp.bfloat16)
    hidden = (conv3x3(first, conv_w[conv_idx]) + time_vec[:, None, None, :]).astype(jnp.bfloat16)
    second = jax.nn.silu(group_norm(hidden, gn_scale[norm_idx + 1], gn_shift[norm_idx + 1])).astype(jnp.bfloat16)
    return (latent.astype(jnp.float32) + conv3x3(second, conv_w[conv_idx + 1])).astype(jnp.bfloat16)


def attention_block(latent, scale, shift, w_qkv, w_out):
    batch = latent.shape[0]
    tokens = LAT_ROWS * LAT_COLS
    head_dim = CHANNELS // NUM_HEADS
    normed = group_norm(latent, scale, shift).astype(jnp.bfloat16).reshape(batch, tokens, CHANNELS)
    projected = jnp.einsum("bnc,schd->sbnhd", normed.astype(jnp.float32), w_qkv.astype(jnp.float32)).astype(jnp.bfloat16)
    keys = projected[1].astype(jnp.float32)
    values = projected[2].astype(jnp.float32)
    w_out32 = w_out.astype(jnp.float32)
    query_blocks = jnp.moveaxis(projected[0].reshape(batch, tokens // QUERY_BLOCK, QUERY_BLOCK, NUM_HEADS, head_dim), 1, 0)

    def one_block(q_blk):
        logits = jnp.einsum("bqhd,bkhd->bhqk", q_blk.astype(jnp.float32), keys) * head_dim ** -0.5
        weights = jnp.exp(logits - jnp.max(logits, axis=-1, keepdims=True))
        weight_sum = jnp.sum(weights, axis=-1)
        attended = jnp.einsum("bhqk,bkhd->bhqd", weights.astype(jnp.bfloat16).astype(jnp.float32), values) / weight_sum[..., None]
        return jnp.einsum("bhqd,hdc->bqc", attended.astype(jnp.bfloat16).astype(jnp.float32), w_out32)

    out = jnp.moveaxis(lax.map(one_block, query_blocks), 0, 1).reshape(latent.shape)
    return (latent.astype(jnp.float32) + out).astype(jnp.bfloat16)


def reference(x, time_emb, gn_scale, gn_shift, conv_w, time_w, w_qkv, w_out):
    time_act = jax.nn.silu(time_emb.astype(jnp.float32)).astype(jnp.bfloat16)
    time_first = jnp.dot(time_act, time_w[0], preferred_element_type=jnp.float32)
    time_second = jnp.dot(time_act, time_w[1], preferred_element_type=jnp.float32)
    first = res_block(x, time_first, gn_scale, gn_shift, conv_w, 0, 0)
    middle = attention_block(first, gn_scale[2], gn_shift[2], w_qkv, w_out)
    return res_block(middle, time_second, gn_scale, gn_shift, conv_w, 3, 2)
```

```python
import functools

import jax
import jax.numpy as jnp
from jax import lax
from jax.experimental import pallas as pl
from jax.experimental.pallas import tpu as pltpu
from jax.sharding import PartitionSpec as P

GROUPS = 32
NORM_EPS = 1e-5
LANES = 128
CHUNK_ROWS = 4
QUERY_BLOCK = 512
KEY_BLOCK = 512
MESH = pl.DeviceIdType.MESH
F32 = jnp.float32
BF16 = jnp.bfloat16


def position():
    sp = lax.axis_index("sp")
    return lax.div(sp, 2), lax.rem(sp, 2), lax.axis_index("sp2")


def partner_id():
    chip_x, core, _ = position()
    return {"sp": 2 * chip_x + 1 - core}


def barrier_pair():
    sem = pltpu.get_barrier_semaphore()
    pl.semaphore_signal(sem, inc=1, device_id=partner_id(), device_id_type=MESH)
    pl.semaphore_wait(sem, 1)


def barrier_all():
    sem = pltpu.get_barrier_semaphore()
    sp, col = lax.axis_index("sp"), lax.axis_index("sp2")
    for i in range(4):
        for j in range(2):
            if i or j:
                target = {"sp": lax.rem(sp + i, 4), "sp2": lax.rem(col + j, 2)}
                pl.semaphore_signal(sem, inc=1, device_id=target, device_id_type=MESH)
    pl.semaphore_wait(sem, 7)


def split3(value):
    high = value.astype(BF16).astype(F32)
    rest = value - high
    mid = rest.astype(BF16).astype(F32)
    low = rest - mid
    return jnp.concatenate([high, mid, low, jnp.zeros_like(value)], axis=0).astype(BF16)


def exact_dot(value, one_hot):
    out = jnp.dot(split3(value), one_hot, preferred_element_type=F32)
    return out[0:8] + out[8:16] + out[16:24]


def group_matrices(channels):
    width = channels // GROUPS
    chan = lax.broadcasted_iota(jnp.int32, (channels, LANES), 0)
    grp = lax.broadcasted_iota(jnp.int32, (channels, LANES), 1) * width
    gather = jnp.where((chan >= grp) & (chan < grp + width), 1.0, 0.0).astype(BF16)
    chan_t = lax.broadcasted_iota(jnp.int32, (LANES, channels), 1)
    grp_t = lax.broadcasted_iota(jnp.int32, (LANES, channels), 0) * width
    spread = jnp.where((chan_t >= grp_t) & (chan_t < grp_t + width), 1.0, 0.0).astype(BF16)
    return gather, spread


def norm_params(sums, count):
    gather, spread = group_matrices(sums.shape[1])
    group_sums = exact_dot(sums, gather)
    mean = group_sums[0:1] / count
    inv_std = lax.rsqrt(group_sums[1:2] / count - mean * mean + NORM_EPS)
    stacked = jnp.concatenate([mean, inv_std, jnp.zeros((6, LANES), F32)], axis=0)
    per_channel = exact_dot(stacked, spread)
    return per_channel[0:1], per_channel[1:2]


def fold_rows(value):
    rows, channels = value.shape
    return jnp.sum(value.reshape(rows // 8, 8, channels), axis=0)


def add_moments(acc_ref, value):
    acc_ref[0] += fold_rows(value)
    acc_ref[1] += fold_rows(value * value)


def moment_rows(acc_ref):
    total = jnp.sum(acc_ref[0], axis=0, keepdims=True)
    square = jnp.sum(acc_ref[1], axis=0, keepdims=True)
    return jnp.concatenate([total, square, jnp.zeros((6, total.shape[1]), F32)], axis=0)


def exchange(slot, send_ref, recv_ref, send_sem, recv_sem):
    copy = pltpu.make_async_remote_copy(
        src_ref=send_ref.at[slot],
        dst_ref=recv_ref.at[slot],
        send_sem=send_sem.at[slot],
        recv_sem=recv_sem.at[slot],
        device_id=partner_id(),
        device_id_type=MESH,
    )
    copy.start()
    copy.wait()
    return send_ref[slot] + recv_ref[slot]


def silu(value):
    half = 0.5 * value
    return half + half * jnp.tanh(half)


def res_kernel(norm_idx, conv_idx, count, first, *refs):
    if first:
        (x_ref, time_ref, scale_ref, shift_ref, w_ref, out_ref, stat_ref,
         a_ref, u_ref, h_ref, w_vmem, acc_ref, st_send, st_recv,
         w_sem, st_ssem, st_rsem, halo_ssem, halo_rsem, tile_ssem, tile_rsem) = refs
    else:
        (a_hbm, stat_in, time_ref, scale_ref, shift_ref, w_ref, out_ref,
         a_ref, u_ref, h_ref, w_vmem, acc_ref, st_send, st_recv,
         w_sem, st_ssem, st_rsem, halo_ssem, halo_rsem, tile_ssem, tile_rsem, a_sem) = refs
    rows, cols, channels = a_ref.shape
    tile_rows, tile_cols = rows // 2, cols // 2
    chip_x, core, chip_y = position()
    sp = lax.axis_index("sp")

    weights = [pltpu.make_async_copy(w_ref.at[conv_idx + k], w_vmem.at[k], w_sem.at[k]) for k in range(2)]
    for copy in weights:
        copy.start()
    if not first:
        a_copy = pltpu.make_async_copy(a_hbm, a_ref, a_sem)
        a_copy.start()
    barrier_all()

    def tile_of(ref, part_row, part_col):
        return ref.at[pl.ds(part_row * tile_rows, tile_rows), pl.ds(part_col * tile_cols, tile_cols)]

    if first:
        slot = 2 * chip_y + core
        for k in (3, 2, 1, 0):
            to_x, to_y = lax.rem(chip_x + k // 2, 2), lax.rem(chip_y + k % 2, 2)
            to_sp = 2 * to_x + chip_x
            here = (to_sp == sp) & (to_y == chip_y)
            src = x_ref.at[2 * to_x + to_y]
            dst = tile_of(a_ref, core, chip_y)
            remote = pltpu.make_async_remote_copy(
                src_ref=src, dst_ref=dst, send_sem=tile_ssem.at[k], recv_sem=tile_rsem.at[slot],
                device_id={"sp": to_sp, "sp2": to_y}, device_id_type=MESH)
            if k:
                remote.start()
            else:
                @pl.when(here)
                def _():
                    pltpu.make_async_copy(src, dst, tile_rsem.at[slot]).start()

                @pl.when(jnp.logical_not(here))
                def _():
                    remote.start()
        acc_ref[...] = jnp.zeros_like(acc_ref)
        for part in range(4):
            landed = tile_of(a_ref, part % 2, part // 2)
            pltpu.make_async_copy(landed, landed, tile_rsem.at[part]).wait()

        def add_row(row, carry):
            add_moments(acc_ref, a_ref[row].astype(F32))
            return carry

        lax.fori_loop(0, rows, add_row, 0)
        st_send[0] = moment_rows(acc_ref)
    else:
        st_send[0] = stat_in[...]
        a_copy.wait()

    def fill(src_ref, mean, gain, shift):
        place = lax.broadcasted_iota(jnp.int32, (cols, channels), 0)

        def fill_row(i, carry):
            row = core * i + (1 - core) * (rows - 1 - i)
            value = silu((src_ref[row].astype(F32) - mean) * gain + shift)
            before = jnp.where(place == 0, 0.0, pltpu.roll(value, 1, 0))
            after = jnp.where(place == cols - 1, 0.0, pltpu.roll(value, cols - 1, 0))
            u_ref[row + 1, :, 0:channels] = before.astype(BF16)
            u_ref[row + 1, :, channels:2 * channels] = value.astype(BF16)
            u_ref[row + 1, :, 2 * channels:3 * channels] = after.astype(BF16)
            return carry

        lax.fori_loop(0, 4, fill_row, 0)
        return fill_row

    for k in range(2):
        src_ref = a_ref if k == 0 else h_ref
        sums = exchange(k, st_send, st_recv, st_ssem, st_rsem)
        mean, inv_std = norm_params(sums, count)
        gain = inv_std * scale_ref[norm_idx + k:norm_idx + k + 1].astype(F32)
        shift = shift_ref[norm_idx + k:norm_idx + k + 1].astype(F32)
        fill_row = fill(src_ref, mean, gain, shift)
        halo = pltpu.make_async_remote_copy(
            src_ref=u_ref.at[rows - (rows - 1) * core],
            dst_ref=u_ref.at[(rows + 1) * core],
            send_sem=halo_ssem.at[k],
            recv_sem=halo_rsem.at[k],
            device_id=partner_id(),
            device_id_type=MESH,
        )
        if k == 0:
            u_ref[(rows + 1) * core] = jnp.zeros((cols, 3 * channels), BF16)
        halo.start()
        lax.fori_loop(4, rows, fill_row, 0)
        weights[k].wait()
        acc_ref[...] = jnp.zeros_like(acc_ref)
        halo.wait()

        def conv_chunk(i, carry):
            chunk = i * CHUNK_ROWS
            total = None
            for dy in range(3):
                lhs = u_ref[pl.ds(chunk + dy, CHUNK_ROWS)].reshape(CHUNK_ROWS * cols, 3 * channels)
                term = jnp.dot(lhs, w_vmem[k, dy], preferred_element_type=F32)
                total = term if total is None else total + term
            if k == 0:
                hidden = (total + time_ref[0:1]).astype(BF16)
                h_ref[pl.ds(chunk, CHUNK_ROWS)] = hidden.reshape(CHUNK_ROWS, cols, channels)
                add_moments(acc_ref, hidden.astype(F32))
            else:
                old = a_ref[pl.ds(chunk, CHUNK_ROWS)].reshape(CHUNK_ROWS * cols, channels)
                new = (old.astype(F32) + total).astype(BF16)
                if first:
                    out_ref[pl.ds(chunk, CHUNK_ROWS)] = new.reshape(CHUNK_ROWS, cols, channels)
                    add_moments(acc_ref, new.astype(F32))
                else:
                    h_ref[pl.ds(chunk, CHUNK_ROWS)] = new.reshape(CHUNK_ROWS, cols, channels)
            return carry

        lax.fori_loop(0, rows // CHUNK_ROWS, conv_chunk, 0)
        if k == 0:
            st_send[1] = moment_rows(acc_ref)

    if first:
        stat_ref[...] = moment_rows(acc_ref)
        for k in range(1, 4):
            pltpu.make_async_remote_copy(
                src_ref=x_ref.at[0], dst_ref=tile_of(a_ref, 0, 0), send_sem=tile_ssem.at[k],
                recv_sem=tile_rsem.at[0], device_id=partner_id(), device_id_type=MESH).wait_send()

        @pl.when(core != chip_x)
        def _():
            pltpu.make_async_remote_copy(
                src_ref=x_ref.at[0], dst_ref=tile_of(a_ref, 0, 0), send_sem=tile_ssem.at[0],
                recv_sem=tile_rsem.at[0], device_id=partner_id(), device_id_type=MESH).wait_send()
    else:
        image = 2 * chip_x + chip_y
        copies = []
        for part in range(4):
            part_row, part_col = part % 2, part // 2
            to_sp = 2 * core + part_row
            here = (to_sp == sp) & (chip_y == part_col)
            src = tile_of(h_ref, part_row, part_col)
            remote = pltpu.make_async_remote_copy(
                src_ref=src, dst_ref=out_ref.at[image], send_sem=tile_ssem.at[part], recv_sem=tile_rsem.at[image],
                device_id={"sp": to_sp, "sp2": part_col}, device_id_type=MESH)
            local = pltpu.make_async_copy(src, out_ref.at[image], tile_rsem.at[image])
            pl.when(here)(local.start)
            pl.when(jnp.logical_not(here))(remote.start)
            copies.append((here, remote))
        for here, remote in copies:
            pl.when(jnp.logical_not(here))(remote.wait_send)
        for slot in range(4):
            pltpu.make_async_copy(out_ref.at[slot], out_ref.at[slot], tile_rsem.at[slot]).wait()


def attention_kernel(norm_idx, count, logit_scale, a_hbm, stat_in, scale_ref, shift_ref, w_hbm, wo_hbm,
                     out_ref, stat_ref, a_ref, n_ref, q_ref, k_ref, v_ref, s_ref, o_ref, w_ref, wo_ref, acc_ref,
                     st_send, st_recv, load_sem, st_ssem, st_rsem, kv_ssem, kv_rsem):
    tokens, channels = a_ref.shape
    heads = q_ref.shape[0]
    step = 256
    loads = [pltpu.make_async_copy(src, dst, load_sem.at[i])
             for i, (src, dst) in enumerate(((a_hbm, a_ref), (w_hbm, w_ref), (wo_hbm, wo_ref)))]
    for load in loads:
        load.start()
    st_send[0] = stat_in[...]
    barrier_pair()
    sums = exchange(0, st_send, st_recv, st_ssem, st_rsem)
    mean, inv_std = norm_params(sums, count)
    gain = inv_std * scale_ref[norm_idx:norm_idx + 1].astype(F32)
    shift = shift_ref[norm_idx:norm_idx + 1].astype(F32)
    loads[0].wait()
    loads[1].wait()

    def kv_copy(which, chunk):
        ref = (k_ref, v_ref)[which]
        return pltpu.make_async_remote_copy(
            src_ref=ref.at[:, pl.ds(chunk * step, step)],
            dst_ref=ref.at[:, pl.ds(tokens + chunk * step, step)],
            send_sem=kv_ssem.at[which, chunk],
            recv_sem=kv_rsem.at[which, chunk],
            device_id=partner_id(),
            device_id_type=MESH,
        )

    chunks = tokens // step

    def key_values(i, carry):
        here = pl.ds(i * step, step)
        normed = ((a_ref[here].astype(F32) - mean) * gain + shift).astype(BF16)
        n_ref[here] = normed
        for which, ref in ((1, k_ref), (2, v_ref)):
            part = jnp.dot(normed, w_ref[which], preferred_element_type=F32).astype(BF16)
            for head in range(heads):
                ref[head, here] = part[:, head * LANES:(head + 1) * LANES]

        @pl.when(i > 0)
        def _():
            kv_copy(0, i - 1).start()
            kv_copy(1, i - 1).start()
        return carry

    lax.fori_loop(0, chunks, key_values, 0)

    def queries(i, carry):
        here = pl.ds(i * step, step)
        part = jnp.dot(n_ref[here], w_ref[0], preferred_element_type=F32).astype(BF16)
        for head in range(heads):
            q_ref[head, here] = part[:, head * LANES:(head + 1) * LANES]

        @pl.when(i == 0)
        def _():
            kv_copy(0, chunks - 1).start()
            kv_copy(1, chunks - 1).start()
        return carry

    lax.fori_loop(0, chunks, queries, 0)

    def arrived(i, carry):
        kv_copy(0, i).wait()
        kv_copy(1, i).wait()
        return carry

    lax.fori_loop(0, chunks, arrived, 0)

    blocks = tokens // QUERY_BLOCK
    key_blocks = 2 * tokens // KEY_BLOCK

    def attend(i, carry):
        head, block = lax.div(i, blocks), lax.rem(i, blocks)
        here = pl.ds(pl.multiple_of(block * QUERY_BLOCK, QUERY_BLOCK), QUERY_BLOCK)
        query = q_ref[head, here]
        peak = None
        for j in range(key_blocks):
            keys = k_ref[head, j * KEY_BLOCK:(j + 1) * KEY_BLOCK]
            scores = lax.dot_general(query, keys, (((1,), (1,)), ((), ())), preferred_element_type=F32)
            s_ref[:, j * KEY_BLOCK:(j + 1) * KEY_BLOCK] = scores
            for part in range(KEY_BLOCK // LANES):
                piece = scores[:, part * LANES:(part + 1) * LANES]
                peak = piece if peak is None else jnp.maximum(peak, piece)
        peak = jnp.max(peak, axis=1, keepdims=True)
        total, attended = None, None
        for j in range(key_blocks):
            weights = jnp.exp2((s_ref[:, j * KEY_BLOCK:(j + 1) * KEY_BLOCK] - peak) * logit_scale)
            for part in range(KEY_BLOCK // LANES):
                piece = weights[:, part * LANES:(part + 1) * LANES]
                total = piece if total is None else total + piece
            term = jnp.dot(weights.astype(BF16), v_ref[head, j * KEY_BLOCK:(j + 1) * KEY_BLOCK], preferred_element_type=F32)
            attended = term if attended is None else attended + term
        total = jnp.sum(total, axis=1, keepdims=True)
        o_ref[here, pl.ds(pl.multiple_of(head * LANES, LANES), LANES)] = (attended / total).astype(BF16)
        return carry

    lax.fori_loop(0, heads * blocks, attend, 0)
    loads[2].wait()
    acc_ref[...] = jnp.zeros_like(acc_ref)

    def project(i, carry):
        here = pl.ds(i * step, step)
        new = (a_ref[here].astype(F32) + jnp.dot(o_ref[here], wo_ref[...], preferred_element_type=F32)).astype(BF16)
        out_ref[here] = new
        add_moments(acc_ref, new.astype(F32))
        return carry

    lax.fori_loop(0, chunks, project, 0)
    stat_ref[...] = moment_rows(acc_ref)


VMEM_SPEC = pl.BlockSpec(memory_space=pltpu.VMEM)
ANY_SPEC = pl.BlockSpec(memory_space=pl.ANY)


def params(collective_id):
    return pltpu.CompilerParams(collective_id=collective_id, has_side_effects=True, vmem_limit_bytes=60 * 2**20)


def res_call(first, norm_idx, conv_idx, count, rows, cols, channels, tile_shape, data, time_vec, scale, shift, w):
    scratch = [
        pltpu.VMEM((rows, cols, channels), BF16),
        pltpu.VMEM((rows + 2, cols, 3 * channels), BF16),
        pltpu.VMEM((rows, cols, channels), BF16),
        pltpu.VMEM((2, 3, 3 * channels, channels), BF16),
        pltpu.VMEM((2, 8, channels), F32),
        pltpu.VMEM((2, 8, channels), F32),
        pltpu.VMEM((2, 8, channels), F32),
        pltpu.SemaphoreType.DMA((2,)),
        pltpu.SemaphoreType.DMA((2,)),
        pltpu.SemaphoreType.DMA((2,)),
        pltpu.SemaphoreType.DMA((2,)),
        pltpu.SemaphoreType.DMA((2,)),
        pltpu.SemaphoreType.DMA((4,)),
        pltpu.SemaphoreType.DMA((4,)),
    ]
    kernel = functools.partial(res_kernel, norm_idx, conv_idx, count, first)
    if first:
        return pl.pallas_call(
            kernel,
            out_shape=[jax.ShapeDtypeStruct((rows, cols, channels), BF16), jax.ShapeDtypeStruct((8, channels), F32)],
            in_specs=[ANY_SPEC, VMEM_SPEC, VMEM_SPEC, VMEM_SPEC, ANY_SPEC],
            out_specs=[VMEM_SPEC, VMEM_SPEC],
            scratch_shapes=scratch,
            compiler_params=params(0),
            name="res_first",
        )(*data, time_vec, scale, shift, w)
    return pl.pallas_call(
        kernel,
        out_shape=jax.ShapeDtypeStruct(tile_shape, BF16),
        in_specs=[ANY_SPEC, VMEM_SPEC, VMEM_SPEC, VMEM_SPEC, VMEM_SPEC, ANY_SPEC],
        out_specs=ANY_SPEC,
        scratch_shapes=scratch + [pltpu.SemaphoreType.DMA],
        compiler_params=params(2),
        name="res_second",
    )(*data, time_vec, scale, shift, w)


def attention_call(norm_idx, count, head_dim, a, stats, scale, shift, w, wo):
    tokens, channels = a.shape
    heads = wo.shape[0] // LANES
    logit_scale = head_dim ** -0.5 * 1.4426950408889634
    return pl.pallas_call(
        functools.partial(attention_kernel, norm_idx, count, logit_scale),
        out_shape=[jax.ShapeDtypeStruct((tokens, channels), BF16), jax.ShapeDtypeStruct((8, channels), F32)],
        in_specs=[ANY_SPEC, VMEM_SPEC, VMEM_SPEC, VMEM_SPEC, ANY_SPEC, ANY_SPEC],
        out_specs=[VMEM_SPEC, VMEM_SPEC],
        scratch_shapes=[
            pltpu.VMEM((tokens, channels), BF16),
            pltpu.VMEM((tokens, channels), BF16),
            pltpu.VMEM((heads, tokens, LANES), BF16),
            pltpu.VMEM((heads, 2 * tokens, LANES), BF16),
            pltpu.VMEM((heads, 2 * tokens, LANES), BF16),
            pltpu.VMEM((QUERY_BLOCK, 2 * tokens), F32),
            pltpu.VMEM((tokens, heads * LANES), BF16),
            pltpu.VMEM(w.shape, BF16),
            pltpu.VMEM(wo.shape, BF16),
            pltpu.VMEM((2, 8, channels), F32),
            pltpu.VMEM((1, 8, channels), F32),
            pltpu.VMEM((1, 8, channels), F32),
            pltpu.SemaphoreType.DMA((3,)),
            pltpu.SemaphoreType.DMA((1,)),
            pltpu.SemaphoreType.DMA((1,)),
            pltpu.SemaphoreType.DMA((2, tokens // 256)),
            pltpu.SemaphoreType.DMA((2, tokens // 256)),
        ],
        compiler_params=params(1),
        name="attention",
    )(a, stats, scale, shift, w, wo)


def solution(mesh):
    lat_spec = P("dp", "sp", "sp2", None)

    def local(x, time_emb, gn_scale, gn_shift, conv_w, time_w, w_qkv, w_out):
        images, tile_rows, tile_cols, channels = x.shape
        rows, cols = 2 * tile_rows, 2 * tile_cols
        count = 2 * rows * cols * (channels // GROUPS)
        heads, head_dim = w_out.shape[0], w_out.shape[1]
        chip_x, _, chip_y = position()
        image = 2 * chip_x + chip_y
        time_act = jax.nn.silu(time_emb.astype(F32)).astype(BF16)
        time_vecs = jnp.einsum("bt,stc->sbc", time_act, time_w, preferred_element_type=F32)
        time_vec = lax.dynamic_slice_in_dim(time_vecs, image, 1, axis=1)
        w = conv_w.reshape(4, 3, 3 * channels, channels)
        pad = LANES - head_dim
        qkv = jnp.pad(w_qkv, ((0, 0), (0, 0), (0, 0), (0, pad))).reshape(3, channels, heads * LANES)
        wo = jnp.pad(w_out, ((0, 0), (0, pad), (0, 0))).reshape(heads * LANES, channels)
        sizes = (count, rows, cols, channels, x.shape)
        first, stats = res_call(True, 0, 0, *sizes, (x,), time_vec[0], gn_scale, gn_shift, w)
        middle, stats = attention_call(2, count, head_dim, first.reshape(rows * cols, channels), stats, gn_scale, gn_shift, qkv, wo)
        return res_call(False, 3, 2, *sizes, (middle.reshape(rows, cols, channels), stats), time_vec[1], gn_scale, gn_shift, w)

    return jax.shard_map(local, mesh=mesh, in_specs=(lat_spec, P("dp", None), P(), P(), P(), P(), P(), P()), out_specs=lat_spec, check_vma=False)
```

```python
import functools

import jax
import jax.numpy as jnp
from jax import lax
from jax.experimental import pallas as pl
from jax.experimental.pallas import tpu as pltpu
from jax.sharding import PartitionSpec as P

GROUPS = 32
NORM_EPS = 1e-5
LANES = 128
CHUNK_ROWS = 4
QUERY_BLOCK = 512
KEY_BLOCK = 512
TOKEN_BLOCK = 512
MESH = pl.DeviceIdType.MESH
F32 = jnp.float32
BF16 = jnp.bfloat16


def position():
    sp = lax.axis_index("sp")
    return lax.div(sp, 2), lax.rem(sp, 2), lax.axis_index("sp2")


def partner_id():
    chip_x, core, _ = position()
    return {"sp": 2 * chip_x + 1 - core}


def barrier_pair():
    sem = pltpu.get_barrier_semaphore()
    pl.semaphore_signal(sem, inc=1, device_id=partner_id(), device_id_type=MESH)
    pl.semaphore_wait(sem, 1)


def barrier_all():
    sem = pltpu.get_barrier_semaphore()
    sp, col = lax.axis_index("sp"), lax.axis_index("sp2")
    for i in range(4):
        for j in range(2):
            if i or j:
                target = {"sp": lax.rem(sp + i, 4), "sp2": lax.rem(col + j, 2)}
                pl.semaphore_signal(sem, inc=1, device_id=target, device_id_type=MESH)
    pl.semaphore_wait(sem, 7)


def split3(value):
    high = value.astype(BF16).astype(F32)
    rest = value - high
    mid = rest.astype(BF16).astype(F32)
    low = rest - mid
    return jnp.concatenate([high, mid, low, jnp.zeros_like(value)], axis=0).astype(BF16)


def exact_dot(value, one_hot):
    out = jnp.dot(split3(value), one_hot, preferred_element_type=F32)
    return out[0:8] + out[8:16] + out[16:24]


def group_matrices(channels):
    width = channels // GROUPS
    chan = lax.broadcasted_iota(jnp.int32, (channels, LANES), 0)
    grp = lax.broadcasted_iota(jnp.int32, (channels, LANES), 1) * width
    gather = jnp.where((chan >= grp) & (chan < grp + width), 1.0, 0.0).astype(BF16)
    chan_t = lax.broadcasted_iota(jnp.int32, (LANES, channels), 1)
    grp_t = lax.broadcasted_iota(jnp.int32, (LANES, channels), 0) * width
    spread = jnp.where((chan_t >= grp_t) & (chan_t < grp_t + width), 1.0, 0.0).astype(BF16)
    return gather, spread


def norm_params(sums, count):
    gather, spread = group_matrices(sums.shape[1])
    group_sums = exact_dot(sums, gather)
    mean = group_sums[0:1] / count
    inv_std = lax.rsqrt(group_sums[1:2] / count - mean * mean + NORM_EPS)
    stacked = jnp.concatenate([mean, inv_std, jnp.zeros((6, LANES), F32)], axis=0)
    per_channel = exact_dot(stacked, spread)
    return per_channel[0:1], per_channel[1:2]


def fold_rows(value):
    rows, channels = value.shape
    return jnp.sum(value.reshape(rows // 8, 8, channels), axis=0)


def add_moments(acc_ref, value):
    acc_ref[0] += fold_rows(value)
    acc_ref[1] += fold_rows(value * value)


def moment_rows(acc_ref):
    total = jnp.sum(acc_ref[0], axis=0, keepdims=True)
    square = jnp.sum(acc_ref[1], axis=0, keepdims=True)
    return jnp.concatenate([total, square, jnp.zeros((6, total.shape[1]), F32)], axis=0)


def exchange(slot, send_ref, recv_ref, send_sem, recv_sem):
    copy = pltpu.make_async_remote_copy(
        src_ref=send_ref.at[slot],
        dst_ref=recv_ref.at[slot],
        send_sem=send_sem.at[slot],
        recv_sem=recv_sem.at[slot],
        device_id=partner_id(),
        device_id_type=MESH,
    )
    copy.start()
    copy.wait()
    return send_ref[slot] + recv_ref[slot]


def silu(value):
    half = 0.5 * value
    return half + half * jnp.tanh(half)


def res_kernel(norm_idx, conv_idx, count, first, *refs):
    if first:
        (x_ref, time_ref, scale_ref, shift_ref, w_ref, out_ref, stat_ref,
         a_ref, u_ref, h_ref, w_vmem, acc_ref, st_send, st_recv,
         w_sem, st_ssem, st_rsem, halo_ssem, halo_rsem, tile_ssem, tile_rsem) = refs
    else:
        (a_hbm, stat_in, time_ref, scale_ref, shift_ref, w_ref, out_ref,
         a_ref, u_ref, h_ref, w_vmem, acc_ref, st_send, st_recv,
         w_sem, st_ssem, st_rsem, halo_ssem, halo_rsem, tile_ssem, tile_rsem, a_sem) = refs
    rows, cols, channels = a_ref.shape
    tile_rows, tile_cols = rows // 2, cols // 2
    chip_x, core, chip_y = position()
    sp = lax.axis_index("sp")

    weights = [pltpu.make_async_copy(w_ref.at[conv_idx + k], w_vmem.at[k], w_sem.at[k]) for k in range(2)]
    for copy in weights:
        copy.start()
    if not first:
        a_copy = pltpu.make_async_copy(a_hbm, a_ref, a_sem)
        a_copy.start()
    barrier_all()

    def tile_of(ref, part_row, part_col):
        return ref.at[pl.ds(part_row * tile_rows, tile_rows), pl.ds(part_col * tile_cols, tile_cols)]

    if first:
        slot = 2 * chip_y + core
        for k in (3, 2, 1, 0):
            to_x, to_y = lax.rem(chip_x + k // 2, 2), lax.rem(chip_y + k % 2, 2)
            to_sp = 2 * to_x + chip_x
            here = (to_sp == sp) & (to_y == chip_y)
            src = x_ref.at[2 * to_x + to_y]
            dst = tile_of(a_ref, core, chip_y)
            remote = pltpu.make_async_remote_copy(
                src_ref=src, dst_ref=dst, send_sem=tile_ssem.at[k], recv_sem=tile_rsem.at[slot],
                device_id={"sp": to_sp, "sp2": to_y}, device_id_type=MESH)
            if k:
                remote.start()
            else:
                @pl.when(here)
                def _():
                    pltpu.make_async_copy(src, dst, tile_rsem.at[slot]).start()

                @pl.when(jnp.logical_not(here))
                def _():
                    remote.start()
        acc_ref[...] = jnp.zeros_like(acc_ref)
        for part in range(4):
            landed = tile_of(a_ref, part % 2, part // 2)
            pltpu.make_async_copy(landed, landed, tile_rsem.at[part]).wait()

        def add_row(row, carry):
            add_moments(acc_ref, a_ref[row].astype(F32))
            return carry

        lax.fori_loop(0, rows, add_row, 0)
        st_send[0] = moment_rows(acc_ref)
    else:
        st_send[0] = stat_in[...]
        a_copy.wait()

    def fill(src_ref, mean, gain, shift):
        place = lax.broadcasted_iota(jnp.int32, (cols, channels), 0)

        def fill_row(i, carry):
            row = core * i + (1 - core) * (rows - 1 - i)
            value = silu((src_ref[row].astype(F32) - mean) * gain + shift)
            before = jnp.where(place == 0, 0.0, pltpu.roll(value, 1, 0))
            after = jnp.where(place == cols - 1, 0.0, pltpu.roll(value, cols - 1, 0))
            u_ref[row + 1, :, 0:channels] = before.astype(BF16)
            u_ref[row + 1, :, channels:2 * channels] = value.astype(BF16)
            u_ref[row + 1, :, 2 * channels:3 * channels] = after.astype(BF16)
            return carry

        lax.fori_loop(0, 4, fill_row, 0)
        return fill_row

    for k in range(2):
        src_ref = a_ref if k == 0 else h_ref
        sums = exchange(k, st_send, st_recv, st_ssem, st_rsem)
        mean, inv_std = norm_params(sums, count)
        gain = inv_std * scale_ref[norm_idx + k:norm_idx + k + 1].astype(F32)
        shift = shift_ref[norm_idx + k:norm_idx + k + 1].astype(F32)
        fill_row = fill(src_ref, mean, gain, shift)
        halo = pltpu.make_async_remote_copy(
            src_ref=u_ref.at[rows - (rows - 1) * core],
            dst_ref=u_ref.at[(rows + 1) * core],
            send_sem=halo_ssem.at[k],
            recv_sem=halo_rsem.at[k],
            device_id=partner_id(),
            device_id_type=MESH,
        )
        if k == 0:
            u_ref[(rows + 1) * core] = jnp.zeros((cols, 3 * channels), BF16)
        halo.start()
        lax.fori_loop(4, rows, fill_row, 0)
        weights[k].wait()
        acc_ref[...] = jnp.zeros_like(acc_ref)
        halo.wait()

        def conv_chunk(i, carry):
            chunk = i * CHUNK_ROWS
            total = None
            for dy in range(3):
                lhs = u_ref[pl.ds(chunk + dy, CHUNK_ROWS)].reshape(CHUNK_ROWS * cols, 3 * channels)
                term = jnp.dot(lhs, w_vmem[k, dy], preferred_element_type=F32)
                total = term if total is None else total + term
            if k == 0:
                hidden = (total + time_ref[0:1]).astype(BF16)
                h_ref[pl.ds(chunk, CHUNK_ROWS)] = hidden.reshape(CHUNK_ROWS, cols, channels)
                add_moments(acc_ref, hidden.astype(F32))
            else:
                old = a_ref[pl.ds(chunk, CHUNK_ROWS)].reshape(CHUNK_ROWS * cols, channels)
                new = (old.astype(F32) + total).astype(BF16)
                if first:
                    out_ref[pl.ds(chunk, CHUNK_ROWS)] = new.reshape(CHUNK_ROWS, cols, channels)
                    add_moments(acc_ref, new.astype(F32))
                else:
                    h_ref[pl.ds(chunk, CHUNK_ROWS)] = new.reshape(CHUNK_ROWS, cols, channels)
            return carry

        lax.fori_loop(0, rows // CHUNK_ROWS, conv_chunk, 0)
        if k == 0:
            st_send[1] = moment_rows(acc_ref)

    if first:
        stat_ref[...] = moment_rows(acc_ref)
        for k in range(1, 4):
            pltpu.make_async_remote_copy(
                src_ref=x_ref.at[0], dst_ref=tile_of(a_ref, 0, 0), send_sem=tile_ssem.at[k],
                recv_sem=tile_rsem.at[0], device_id=partner_id(), device_id_type=MESH).wait_send()

        @pl.when(core != chip_x)
        def _():
            pltpu.make_async_remote_copy(
                src_ref=x_ref.at[0], dst_ref=tile_of(a_ref, 0, 0), send_sem=tile_ssem.at[0],
                recv_sem=tile_rsem.at[0], device_id=partner_id(), device_id_type=MESH).wait_send()
    else:
        image = 2 * chip_x + chip_y
        copies = []
        for part in range(4):
            part_row, part_col = part % 2, part // 2
            to_sp = 2 * core + part_row
            here = (to_sp == sp) & (chip_y == part_col)
            src = tile_of(h_ref, part_row, part_col)
            remote = pltpu.make_async_remote_copy(
                src_ref=src, dst_ref=out_ref.at[image], send_sem=tile_ssem.at[part], recv_sem=tile_rsem.at[image],
                device_id={"sp": to_sp, "sp2": part_col}, device_id_type=MESH)
            local = pltpu.make_async_copy(src, out_ref.at[image], tile_rsem.at[image])
            pl.when(here)(local.start)
            pl.when(jnp.logical_not(here))(remote.start)
            copies.append((here, remote))
        for here, remote in copies:
            pl.when(jnp.logical_not(here))(remote.wait_send)
        for slot in range(4):
            pltpu.make_async_copy(out_ref.at[slot], out_ref.at[slot], tile_rsem.at[slot]).wait()


def attention_kernel(norm_idx, count, logit_scale, a_hbm, stat_in, scale_ref, shift_ref, w_hbm, wo_hbm,
                     out_ref, stat_ref, a_ref, n_ref, q_ref, k_ref, v_ref, s_even, s_odd, peak_ref, o_ref,
                     wq_ref, wk_ref, wv_ref, wo_ref, acc_ref,
                     st_send, st_recv, load_sem, head_sem, st_ssem, st_rsem, kv_ssem, kv_rsem):
    tokens, channels = a_ref.shape
    heads, head_dim, _ = v_ref.shape
    loads = [pltpu.make_async_copy(src, dst, load_sem.at[i])
             for i, (src, dst) in enumerate(((a_hbm, a_ref), (w_hbm.at[2], wv_ref), (w_hbm.at[0], wq_ref), (wo_hbm, wo_ref)))]
    head_loads = [pltpu.make_async_copy(w_hbm.at[1, pl.ds(head * head_dim, head_dim)],
                                        wk_ref.at[pl.ds(head * LANES, head_dim)], head_sem.at[head])
                  for head in range(heads)]
    for load in loads[:2] + head_loads + loads[2:]:
        load.start()
    for head in range(heads):
        wk_ref[head * LANES + head_dim:(head + 1) * LANES] = jnp.zeros((LANES - head_dim, channels), BF16)
        q_ref[head, head_dim:] = jnp.zeros((LANES - head_dim, tokens), BF16)
    st_send[0] = stat_in[...]
    barrier_pair()
    sums = exchange(0, st_send, st_recv, st_ssem, st_rsem)
    mean, inv_std = norm_params(sums, count)
    gain = inv_std * scale_ref[norm_idx:norm_idx + 1].astype(F32)
    shift = shift_ref[norm_idx:norm_idx + 1].astype(F32)
    loads[0].wait()
    loads[1].wait()
    for load in head_loads:
        load.wait()

    step = TOKEN_BLOCK
    chunks = tokens // step
    transposed = (((1,), (1,)), ((), ()))

    def kv_copy(which, chunk):
        if which:
            ref, axis_index = v_ref, (slice(None), slice(None))
        else:
            ref, axis_index = k_ref, (slice(None),)
        return pltpu.make_async_remote_copy(
            src_ref=ref.at[axis_index + (pl.ds(pl.multiple_of(chunk * step, step), step),)],
            dst_ref=ref.at[axis_index + (pl.ds(pl.multiple_of(tokens + chunk * step, step), step),)],
            send_sem=kv_ssem.at[which, chunk],
            recv_sem=kv_rsem.at[which, chunk],
            device_id=partner_id(),
            device_id_type=MESH,
        )

    def key_values(i, carry):
        here = pl.ds(pl.multiple_of(i * step, step), step)
        normed = ((a_ref[here].astype(F32) - mean) * gain + shift).astype(BF16)
        n_ref[here] = normed
        part = lax.dot_general(normed, wk_ref[...], transposed, preferred_element_type=F32).astype(BF16)
        for head in range(heads):
            k_ref[head, here] = part[:, head * LANES:(head + 1) * LANES]
        part = lax.dot_general(wv_ref[...], normed, transposed, preferred_element_type=F32).astype(BF16)
        for head in range(heads):
            v_ref[head, :, here] = part[head * head_dim:(head + 1) * head_dim]

        @pl.when(i > 0)
        def _():
            kv_copy(0, i - 1).start()
            kv_copy(1, i - 1).start()
        return carry

    lax.fori_loop(0, chunks, key_values, 0)
    loads[2].wait()

    def queries(i, carry):
        here = pl.ds(pl.multiple_of(i * step, step), step)
        part = lax.dot_general(wq_ref[...], n_ref[here], transposed, preferred_element_type=F32).astype(BF16)
        for head in range(heads):
            q_ref[head, 0:head_dim, here] = part[head * head_dim:(head + 1) * head_dim]

        @pl.when(i == 0)
        def _():
            kv_copy(0, chunks - 1).start()
            kv_copy(1, chunks - 1).start()
        return carry

    lax.fori_loop(0, chunks, queries, 0)

    def arrived(i, carry):
        kv_copy(0, i).wait()
        kv_copy(1, i).wait()
        return carry

    lax.fori_loop(0, chunks, arrived, 0)

    blocks = tokens // QUERY_BLOCK
    key_blocks = 2 * tokens // KEY_BLOCK

    def fold(value, combine):
        return combine(value.reshape(KEY_BLOCK // 8, 8, QUERY_BLOCK), axis=0)

    def interleaved(i, s_ref, s_next, slot):
        if i is not None:
            head = lax.div(i, blocks)
            here = pl.ds(pl.multiple_of(lax.rem(i, blocks) * QUERY_BLOCK, QUERY_BLOCK), QUERY_BLOCK)
            peak = jnp.max(peak_ref[slot], axis=0, keepdims=True)
            after = jnp.minimum(i + 1, heads * blocks - 1)
        else:
            after = 0
        next_head = lax.div(after, blocks)
        next_here = pl.ds(pl.multiple_of(lax.rem(after, blocks) * QUERY_BLOCK, QUERY_BLOCK), QUERY_BLOCK)
        query = q_ref[next_head, :, next_here]
        next_peak, total, attended = None, None, None
        for j in range(key_blocks):
            keys = slice(j * KEY_BLOCK, (j + 1) * KEY_BLOCK)
            scores = jnp.dot(k_ref[next_head, keys], query, preferred_element_type=F32)
            s_next[keys] = scores
            piece = fold(scores, jnp.max)
            next_peak = piece if next_peak is None else jnp.maximum(next_peak, piece)
            if i is not None:
                weights = jnp.exp2((s_ref[keys] - peak) * logit_scale)
                piece = fold(weights, jnp.sum)
                total = piece if total is None else total + piece
                term = jnp.dot(v_ref[head, :, keys], weights.astype(BF16), preferred_element_type=F32)
                attended = term if attended is None else attended + term
        peak_ref[1 - slot] = next_peak
        if i is not None:
            total = jnp.sum(total, axis=0, keepdims=True)
            rows = pl.ds(pl.multiple_of(head * head_dim, 16), head_dim)
            o_ref[rows, here] = (attended / total).astype(BF16)

    interleaved(None, None, s_even, 1)

    def attend(i, carry):
        interleaved(2 * i, s_even, s_odd, 0)
        interleaved(2 * i + 1, s_odd, s_even, 1)
        return carry

    lax.fori_loop(0, heads * blocks // 2, attend, 0)
    loads[3].wait()
    acc_ref[...] = jnp.zeros_like(acc_ref)

    def project(i, carry):
        here = pl.ds(pl.multiple_of(i * step, step), step)
        added = lax.dot_general(o_ref[:, here], wo_ref[...], (((0,), (0,)), ((), ())), preferred_element_type=F32)
        new = (a_ref[here].astype(F32) + added).astype(BF16)
        out_ref[here] = new
        add_moments(acc_ref, new.astype(F32))
        return carry

    lax.fori_loop(0, chunks, project, 0)
    stat_ref[...] = moment_rows(acc_ref)


VMEM_SPEC = pl.BlockSpec(memory_space=pltpu.VMEM)
ANY_SPEC = pl.BlockSpec(memory_space=pl.ANY)


def params(collective_id):
    return pltpu.CompilerParams(collective_id=collective_id, has_side_effects=True, vmem_limit_bytes=60 * 2**20)


def res_call(first, norm_idx, conv_idx, count, rows, cols, channels, tile_shape, data, time_vec, scale, shift, w):
    scratch = [
        pltpu.VMEM((rows, cols, channels), BF16),
        pltpu.VMEM((rows + 2, cols, 3 * channels), BF16),
        pltpu.VMEM((rows, cols, channels), BF16),
        pltpu.VMEM((2, 3, 3 * channels, channels), BF16),
        pltpu.VMEM((2, 8, channels), F32),
        pltpu.VMEM((2, 8, channels), F32),
        pltpu.VMEM((2, 8, channels), F32),
        pltpu.SemaphoreType.DMA((2,)),
        pltpu.SemaphoreType.DMA((2,)),
        pltpu.SemaphoreType.DMA((2,)),
        pltpu.SemaphoreType.DMA((2,)),
        pltpu.SemaphoreType.DMA((2,)),
        pltpu.SemaphoreType.DMA((4,)),
        pltpu.SemaphoreType.DMA((4,)),
    ]
    kernel = functools.partial(res_kernel, norm_idx, conv_idx, count, first)
    if first:
        return pl.pallas_call(
            kernel,
            out_shape=[jax.ShapeDtypeStruct((rows, cols, channels), BF16), jax.ShapeDtypeStruct((8, channels), F32)],
            in_specs=[ANY_SPEC, VMEM_SPEC, VMEM_SPEC, VMEM_SPEC, ANY_SPEC],
            out_specs=[VMEM_SPEC, VMEM_SPEC],
            scratch_shapes=scratch,
            compiler_params=params(0),
            name="res_first",
        )(*data, time_vec, scale, shift, w)
    return pl.pallas_call(
        kernel,
        out_shape=jax.ShapeDtypeStruct(tile_shape, BF16),
        in_specs=[ANY_SPEC, VMEM_SPEC, VMEM_SPEC, VMEM_SPEC, VMEM_SPEC, ANY_SPEC],
        out_specs=ANY_SPEC,
        scratch_shapes=scratch + [pltpu.SemaphoreType.DMA],
        compiler_params=params(2),
        name="res_second",
    )(*data, time_vec, scale, shift, w)


def attention_call(norm_idx, count, heads, a, stats, scale, shift, w, wo):
    tokens, channels = a.shape
    head_dim = channels // heads
    logit_scale = head_dim ** -0.5 * 1.4426950408889634
    return pl.pallas_call(
        functools.partial(attention_kernel, norm_idx, count, logit_scale),
        out_shape=[jax.ShapeDtypeStruct((tokens, channels), BF16), jax.ShapeDtypeStruct((8, channels), F32)],
        in_specs=[ANY_SPEC, VMEM_SPEC, VMEM_SPEC, VMEM_SPEC, ANY_SPEC, ANY_SPEC],
        out_specs=[VMEM_SPEC, VMEM_SPEC],
        scratch_shapes=[
            pltpu.VMEM((tokens, channels), BF16),
            pltpu.VMEM((tokens, channels), BF16),
            pltpu.VMEM((heads, LANES, tokens), BF16),
            pltpu.VMEM((heads, 2 * tokens, LANES), BF16),
            pltpu.VMEM((heads, head_dim, 2 * tokens), BF16),
            pltpu.VMEM((2 * tokens, QUERY_BLOCK), F32),
            pltpu.VMEM((2 * tokens, QUERY_BLOCK), F32),
            pltpu.VMEM((2, 8, QUERY_BLOCK), F32),
            pltpu.VMEM((channels, tokens), BF16),
            pltpu.VMEM((channels, channels), BF16),
            pltpu.VMEM((heads * LANES, channels), BF16),
            pltpu.VMEM((channels, channels), BF16),
            pltpu.VMEM((channels, channels), BF16),
            pltpu.VMEM((2, 8, channels), F32),
            pltpu.VMEM((1, 8, channels), F32),
            pltpu.VMEM((1, 8, channels), F32),
            pltpu.SemaphoreType.DMA((4,)),
            pltpu.SemaphoreType.DMA((heads,)),
            pltpu.SemaphoreType.DMA((1,)),
            pltpu.SemaphoreType.DMA((1,)),
            pltpu.SemaphoreType.DMA((2, tokens // TOKEN_BLOCK)),
            pltpu.SemaphoreType.DMA((2, tokens // TOKEN_BLOCK)),
        ],
        compiler_params=params(1),
        name="attention",
    )(a, stats, scale, shift, w, wo)


def solution(mesh):
    lat_spec = P("dp", "sp", "sp2", None)

    def local(x, time_emb, gn_scale, gn_shift, conv_w, time_w, w_qkv, w_out):
        images, tile_rows, tile_cols, channels = x.shape
        rows, cols = 2 * tile_rows, 2 * tile_cols
        count = 2 * rows * cols * (channels // GROUPS)
        heads = w_out.shape[0]
        chip_x, _, chip_y = position()
        image = 2 * chip_x + chip_y
        time_act = jax.nn.silu(time_emb.astype(F32)).astype(BF16)
        time_vecs = jnp.einsum("bt,stc->sbc", time_act, time_w, preferred_element_type=F32)
        time_vec = lax.dynamic_slice_in_dim(time_vecs, image, 1, axis=1)
        w = conv_w.reshape(4, 3, 3 * channels, channels)
        qkv = jnp.transpose(w_qkv, (0, 2, 3, 1)).reshape(3, channels, channels)
        wo = w_out.reshape(channels, channels)
        sizes = (count, rows, cols, channels, x.shape)
        first, stats = res_call(True, 0, 0, *sizes, (x,), time_vec[0], gn_scale, gn_shift, w)
        middle, stats = attention_call(2, count, heads, first.reshape(rows * cols, channels), stats, gn_scale, gn_shift, qkv, wo)
        return res_call(False, 3, 2, *sizes, (middle.reshape(rows, cols, channels), stats), time_vec[1], gn_scale, gn_shift, w)

    return jax.shard_map(local, mesh=mesh, in_specs=(lat_spec, P("dp", None), P(), P(), P(), P(), P(), P()), out_specs=lat_spec, check_vma=False)
```

```python
import functools

import jax
import jax.numpy as jnp
from jax import lax
from jax.experimental import pallas as pl
from jax.experimental.pallas import tpu as pltpu
from jax.sharding import PartitionSpec as P

GROUPS = 32
NORM_EPS = 1e-5
LANES = 128
CHUNK_ROWS = 4
CHUNKS = 8
PIECES = ((0, 5), (5, 4), (9, 4), (13, 3))
QUERY_BLOCK = 512
KEY_BLOCK = 512
TOKEN_BLOCK = 512
MESH = pl.DeviceIdType.MESH
F32 = jnp.float32
BF16 = jnp.bfloat16


def position():
    sp = lax.axis_index("sp")
    return lax.div(sp, 2), lax.rem(sp, 2), lax.axis_index("sp2")


def partner_id():
    chip_x, core, _ = position()
    return {"sp": 2 * chip_x + 1 - core}


def barrier_pair():
    sem = pltpu.get_barrier_semaphore()
    pl.semaphore_signal(sem, inc=1, device_id=partner_id(), device_id_type=MESH)
    pl.semaphore_wait(sem, 1)


def others():
    sp, col = lax.axis_index("sp"), lax.axis_index("sp2")
    return [(lax.rem(sp + i, 4), lax.rem(col + j, 2)) for i in range(4) for j in range(2) if i or j]


def signal_all():
    for sp, col in others():
        pl.semaphore_signal(pltpu.get_barrier_semaphore(), inc=1, device_id={"sp": sp, "sp2": col}, device_id_type=MESH)


def wait_all():
    pl.semaphore_wait(pltpu.get_barrier_semaphore(), 7)


def split3(value):
    high = value.astype(BF16).astype(F32)
    rest = value - high
    mid = rest.astype(BF16).astype(F32)
    low = rest - mid
    return jnp.concatenate([high, mid, low, jnp.zeros_like(value)], axis=0).astype(BF16)


def exact_dot(value, one_hot):
    out = jnp.dot(split3(value), one_hot, preferred_element_type=F32)
    return out[0:8] + out[8:16] + out[16:24]


def group_matrices(channels):
    width = channels // GROUPS
    chan = lax.broadcasted_iota(jnp.int32, (channels, LANES), 0)
    grp = lax.broadcasted_iota(jnp.int32, (channels, LANES), 1) * width
    gather = jnp.where((chan >= grp) & (chan < grp + width), 1.0, 0.0).astype(BF16)
    chan_t = lax.broadcasted_iota(jnp.int32, (LANES, channels), 1)
    grp_t = lax.broadcasted_iota(jnp.int32, (LANES, channels), 0) * width
    spread = jnp.where((chan_t >= grp_t) & (chan_t < grp_t + width), 1.0, 0.0).astype(BF16)
    return gather, spread


def spread_groups(group_sums, spread, count):
    mean = group_sums[0:1] / count
    inv_std = lax.rsqrt(group_sums[1:2] / count - mean * mean + NORM_EPS)
    stacked = jnp.concatenate([mean, inv_std, jnp.zeros((6, LANES), F32)], axis=0)
    per_channel = exact_dot(stacked, spread)
    return per_channel[0:1], per_channel[1:2]


def norm_params(sums, count):
    gather, spread = group_matrices(sums.shape[1])
    return spread_groups(exact_dot(sums, gather)[0:2], spread, count)


def fold_rows(value):
    rows, channels = value.shape
    return jnp.sum(value.reshape(rows // 8, 8, channels), axis=0)


def add_moments(acc_ref, value):
    acc_ref[0] += fold_rows(value)
    acc_ref[1] += fold_rows(value * value)


def moment_rows(acc_ref):
    total = jnp.sum(acc_ref[0], axis=0, keepdims=True)
    square = jnp.sum(acc_ref[1], axis=0, keepdims=True)
    return jnp.concatenate([total, square, jnp.zeros((6, total.shape[1]), F32)], axis=0)


def exchange(slot, send_ref, recv_ref, send_sem, recv_sem):
    copy = pltpu.make_async_remote_copy(
        src_ref=send_ref.at[slot],
        dst_ref=recv_ref.at[slot],
        send_sem=send_sem.at[slot],
        recv_sem=recv_sem.at[slot],
        device_id=partner_id(),
        device_id_type=MESH,
    )
    copy.start()
    copy.wait()
    return send_ref[slot] + recv_ref[slot]


def silu(value):
    half = 0.5 * value
    return half + half * jnp.tanh(half)


def fill_chunk(u_ref, src_ref, chunk, params, top_edge, bottom_edge):
    mean, gain, shift = params
    _, cols, channels = src_ref.shape
    place = lax.broadcasted_iota(jnp.int32, (cols, channels), 0)
    last = CHUNK_ROWS + 1
    for j in range(CHUNK_ROWS + 2):
        value = silu((src_ref[chunk * CHUNK_ROWS + j].astype(F32) - mean) * gain + shift)
        if j == 0:
            value = jnp.where(top_edge & (chunk == 0), 0.0, value)
        if j == last:
            value = jnp.where(bottom_edge & (chunk == CHUNKS - 1), 0.0, value)
        before = jnp.where(place == 0, 0.0, pltpu.roll(value, 1, 0))
        after = jnp.where(place == cols - 1, 0.0, pltpu.roll(value, cols - 1, 0))
        u_ref[j, :, 0:channels] = before.astype(BF16)
        u_ref[j, :, channels:2 * channels] = value.astype(BF16)
        u_ref[j, :, 2 * channels:3 * channels] = after.astype(BF16)


def conv_chunk(u_ref, w):
    _, cols, depth = u_ref.shape
    lhs = jnp.concatenate([u_ref[dy:dy + CHUNK_ROWS].reshape(CHUNK_ROWS * cols, depth) for dy in range(3)], axis=1)
    return jnp.dot(lhs, w[...], preferred_element_type=F32)


def conv_loop(order, ready, fill, finish, u_even, u_odd, w):
    def step(i, half, parity, u_now, u_next):
        after = jnp.minimum(i + 1, CHUNKS - 1)
        ready(half, parity)
        fill(u_next, order(after))
        finish(order(i), conv_chunk(u_now, w))

    def pair(half, carry):
        step(2 * half, half, 0, u_even, u_odd)
        step(2 * half + 1, half, 1, u_odd, u_even)
        return carry

    fill(u_even, order(jnp.int32(0)))
    lax.fori_loop(0, CHUNKS // 2, pair, 0)


def in_order(i):
    return i


def from_ends(i):
    return lax.rem(i + 1, 2) * lax.div(i, 2) + lax.rem(i, 2) * (CHUNKS - 1 - lax.div(i, 2))


def rows_of(ref, chunk, first=0):
    value = ref[pl.ds(chunk * CHUNK_ROWS + first, CHUNK_ROWS)]
    return value.reshape(value.shape[0] * value.shape[1], value.shape[2])


def send_edge_row(ref, send_sem, recv_sem, src_ref=None, src_row=None):
    rows = ref.shape[0] - 2
    core = position()[1]
    src = ref.at[rows - (rows - 1) * core] if src_ref is None else src_ref.at[src_row]
    return pltpu.make_async_remote_copy(
        src_ref=src, dst_ref=ref.at[(rows + 1) * core],
        send_sem=send_sem, recv_sem=recv_sem, device_id=partner_id(), device_id_type=MESH)


def first_kernel(count, x_ref, emb_ref, scale_ref, shift_ref, w_ref, tw_ref, out_ref, stat_ref, time_ref,
                 x_vmem, a_ref, h_ref, u_even, u_odd, w_vmem, tw_vmem, acc_ref, time_all, grp_recv, grp_total, st_send, st_recv,
                 load_sem, grp_ssem, grp_rsem, st_ssem, st_rsem, edge_ssem, edge_rsem, piece_ssem, piece_rsem, halo_ssem, halo_rsem):
    images, tile_rows, tile_cols, channels = x_ref.shape
    rows = 2 * tile_rows
    chip_x, core, chip_y = position()
    sp = lax.axis_index("sp")
    me = 2 * sp + chip_y
    image = 2 * chip_x + chip_y

    signal_all()
    x_load = pltpu.make_async_copy(x_ref, x_vmem, load_sem.at[0])
    x_load.start()
    weights = [pltpu.make_async_copy(w_ref.at[k], w_vmem.at[k], load_sem.at[1 + k]) for k in range(2)]
    tw_load = pltpu.make_async_copy(tw_ref, tw_vmem, load_sem.at[3])
    for copy in weights[:1] + [tw_load] + weights[1:]:
        copy.start()

    gather, spread = group_matrices(channels)
    x_load.wait()
    moments = []
    for i in range(images):
        acc_ref[...] = jnp.zeros_like(acc_ref)

        def add_row(row, carry):
            add_moments(acc_ref, x_vmem[i, row].astype(F32))
            return carry

        lax.fori_loop(0, tile_rows, add_row, 0)
        moments += [jnp.sum(acc_ref[0], axis=0, keepdims=True), jnp.sum(acc_ref[1], axis=0, keepdims=True)]
    grp_recv[me] = exact_dot(jnp.concatenate(moments, axis=0), gather)
    wait_all()
    group_copies = []
    for k, (to_sp, to_y) in enumerate(others()):
        copy = pltpu.make_async_remote_copy(
            src_ref=grp_recv.at[me], dst_ref=grp_recv.at[me], send_sem=grp_ssem.at[k], recv_sem=grp_rsem.at[me],
            device_id={"sp": to_sp, "sp2": to_y}, device_id_type=MESH)
        copy.start()
        group_copies.append((copy, 2 * to_sp + to_y))

    def piece(part, source_core):
        low, high = PIECES[part]
        start = (1 - source_core) * low + source_core * (tile_rows - low - high)
        return pl.ds(start, high), pl.ds(1 + source_core * tile_rows + start, high)

    def piece_copies(k, part):
        to_x, to_y = lax.rem(chip_x + k // 2, 2), lax.rem(chip_y + k % 2, 2)
        src_rows, dst_rows = piece(part, core)
        src = x_ref.at[2 * to_x + to_y, src_rows]
        dst = a_ref.at[dst_rows, pl.ds(chip_y * tile_cols, tile_cols)]
        landed = piece_rsem.at[part, 2 * chip_y + core]
        remote = pltpu.make_async_remote_copy(
            src_ref=src, dst_ref=dst, send_sem=piece_ssem.at[k, part], recv_sem=landed,
            device_id={"sp": 2 * to_x + chip_x, "sp2": to_y}, device_id_type=MESH)
        return remote, pltpu.make_async_copy(src, dst, landed)

    def halo_copies(k):
        to_x, to_y = lax.rem(chip_x + k // 2, 2), lax.rem(chip_y + k % 2, 2)
        src = x_ref.at[2 * to_x + to_y, (tile_rows - 1) * core]
        dst = a_ref.at[(rows + 1) * chip_x, pl.ds(chip_y * tile_cols, tile_cols)]
        remote = pltpu.make_async_remote_copy(
            src_ref=src, dst_ref=dst, send_sem=halo_ssem.at[k], recv_sem=halo_rsem.at[chip_y],
            device_id={"sp": 2 * to_x + 1 - chip_x, "sp2": to_y}, device_id_type=MESH)
        return remote, pltpu.make_async_copy(src, dst, halo_rsem.at[chip_y])

    at_home = core == chip_x
    far_first = (3, 2, 1, 0)

    @pl.when(jnp.logical_not(at_home))
    def _():
        for k in far_first:
            halo_copies(k)[0 if k else 1].start()

    for part in range(len(PIECES)):
        for k in far_first:
            remote, local = piece_copies(k, part)
            if k:
                remote.start()
            else:
                pl.when(at_home)(local.start)
                pl.when(jnp.logical_not(at_home))(remote.start)

    tw_load.wait()
    emb = silu(emb_ref[...].astype(F32)).astype(BF16)
    for k in range(2):
        time_all[k, 0:images] = jnp.dot(emb, tw_vmem[k], preferred_element_type=F32)
    time_ref[...] = jnp.broadcast_to(time_all[1, pl.ds(image, 1)], time_ref.shape)
    time_vec = time_all[0, pl.ds(image, 1)]

    total = jnp.zeros((8, LANES), F32)
    for copy, _ in group_copies:
        copy.wait_send()
    for copy, sender in group_copies:
        pltpu.make_async_copy(grp_recv.at[sender], grp_recv.at[sender], grp_rsem.at[sender]).wait()
    for slot in range(8):
        total = total + grp_recv[slot]
    grp_total[...] = total
    mean, inv_std = spread_groups(grp_total[pl.ds(2 * image, 2)], spread, count)

    def wait_piece(part, source_core):
        for col in range(2):
            landed = a_ref.at[piece(part, source_core)[1], pl.ds(col * tile_cols, tile_cols)]
            pltpu.make_async_copy(landed, landed, piece_rsem.at[part, 2 * col + source_core]).wait()

    def ready(half, parity):
        if parity == 0:
            for part in range(3):
                pl.when(half == part)(functools.partial(wait_piece, part, 1))
        else:
            for part in range(1, 4):
                pl.when(half + 1 == part)(functools.partial(wait_piece, part, 0))
            pl.when(half + 1 == 3)(functools.partial(wait_piece, 3, 1))

    top_edge, bottom_edge = core == 0, core == 1

    def norm(k, mean, inv_std):
        return mean, inv_std * scale_ref[k:k + 1].astype(F32), shift_ref[k:k + 1].astype(F32)

    params = norm(0, mean, inv_std)
    for col in range(2):
        landed = a_ref.at[(rows + 1) * (1 - core), pl.ds(col * tile_cols, tile_cols)]
        pltpu.make_async_copy(landed, landed, halo_rsem.at[col]).wait()
    wait_piece(0, 0)
    acc_ref[...] = jnp.zeros_like(acc_ref)
    weights[0].wait()

    def finish_first(chunk, total):
        hidden = (total + time_vec).astype(BF16)
        h_ref[pl.ds(chunk * CHUNK_ROWS + 1, CHUNK_ROWS)] = hidden.reshape(CHUNK_ROWS, 2 * tile_cols, channels)
        add_moments(acc_ref, hidden.astype(F32))

    conv_loop(from_ends, ready, lambda u_ref, chunk: fill_chunk(u_ref, a_ref, chunk, params, top_edge, bottom_edge),
              finish_first, u_even, u_odd, w_vmem.at[0])

    edge = send_edge_row(h_ref, edge_ssem, edge_rsem)
    edge.start()
    st_send[0] = moment_rows(acc_ref)
    acc_ref[...] = jnp.zeros_like(acc_ref)
    weights[1].wait()
    second = norm(1, *norm_params(exchange(0, st_send, st_recv, st_ssem, st_rsem), count))
    edge.wait()

    def finish_second(chunk, total):
        new = (rows_of(a_ref, chunk, 1).astype(F32) + total).astype(BF16)
        out_ref[pl.ds(chunk * CHUNK_ROWS, CHUNK_ROWS)] = new.reshape(CHUNK_ROWS, 2 * tile_cols, channels)
        add_moments(acc_ref, new.astype(F32))

    conv_loop(in_order, lambda half, parity: None,
              lambda u_ref, chunk: fill_chunk(u_ref, h_ref, chunk, second, top_edge, bottom_edge),
              finish_second, u_even, u_odd, w_vmem.at[1])
    stat_ref[...] = moment_rows(acc_ref)

    @pl.when(jnp.logical_not(at_home))
    def _():
        for k in (1, 2, 3):
            halo_copies(k)[0].wait_send()

    for part in range(len(PIECES)):
        for k in range(4):
            remote, _ = piece_copies(k, part)
            if k:
                remote.wait_send()
            else:
                pl.when(jnp.logical_not(at_home))(remote.wait_send)


def second_kernel(count, a_hbm, stat_in, time_ref, scale_ref, shift_ref, w_ref, out_ref,
                  a_ref, h_ref, u_even, u_odd, w_vmem, acc_ref, res_ref, st_send, st_recv,
                  load_sem, st_ssem, st_rsem, edge_ssem, edge_rsem, tile_ssem, tile_rsem):
    rows, cols, channels = res_ref.shape
    tile_rows, tile_cols = rows // 2, cols // 2
    chip_x, core, chip_y = position()
    sp = lax.axis_index("sp")
    image = 2 * chip_x + chip_y

    signal_all()
    a_load = pltpu.make_async_copy(a_hbm, a_ref.at[pl.ds(1, rows)], load_sem.at[0])
    a_load.start()
    weights = [pltpu.make_async_copy(w_ref.at[2 + k], w_vmem.at[k], load_sem.at[1 + k]) for k in range(2)]
    for copy in weights:
        copy.start()
    st_send[0] = stat_in[...]
    acc_ref[...] = jnp.zeros_like(acc_ref)
    wait_all()
    edge = send_edge_row(a_ref, edge_ssem.at[0], edge_rsem.at[0], a_hbm, (rows - 1) * (1 - core))
    edge.start()
    top_edge, bottom_edge = core == 0, core == 1

    def norm(k, sums):
        mean, inv_std = norm_params(sums, count)
        return mean, inv_std * scale_ref[3 + k:4 + k].astype(F32), shift_ref[3 + k:4 + k].astype(F32)

    params = norm(0, exchange(0, st_send, st_recv, st_ssem, st_rsem))
    a_load.wait()
    edge.wait()
    weights[0].wait()
    time_vec = time_ref[0:1]

    def finish_first(chunk, total):
        hidden = (total + time_vec).astype(BF16)
        h_ref[pl.ds(chunk * CHUNK_ROWS + 1, CHUNK_ROWS)] = hidden.reshape(CHUNK_ROWS, cols, channels)
        add_moments(acc_ref, hidden.astype(F32))

    conv_loop(in_order, lambda half, parity: None,
              lambda u_ref, chunk: fill_chunk(u_ref, a_ref, chunk, params, top_edge, bottom_edge),
              finish_first, u_even, u_odd, w_vmem.at[0])

    edge = send_edge_row(h_ref, edge_ssem.at[1], edge_rsem.at[1])
    edge.start()
    st_send[1] = moment_rows(acc_ref)
    weights[1].wait()
    second = norm(1, exchange(1, st_send, st_recv, st_ssem, st_rsem))
    edge.wait()

    per_tile = CHUNKS // 2

    def home_copies(chunk, col):
        to_sp = 2 * core + lax.div(chunk, per_tile)
        slot = lax.rem(chunk, per_tile)
        here = (to_sp == sp) & (chip_y == col)
        src = res_ref.at[pl.ds(chunk * CHUNK_ROWS, CHUNK_ROWS), pl.ds(col * tile_cols, tile_cols)]
        dst = out_ref.at[image, pl.ds(slot * CHUNK_ROWS, CHUNK_ROWS)]
        landed = tile_rsem.at[image, slot]
        remote = pltpu.make_async_remote_copy(
            src_ref=src, dst_ref=dst, send_sem=tile_ssem.at[chunk, col], recv_sem=landed,
            device_id={"sp": to_sp, "sp2": col}, device_id_type=MESH)
        return here, remote, pltpu.make_async_copy(src, dst, landed)

    def send_home(chunk):
        for col in range(2):
            here, remote, local = home_copies(chunk, col)
            pl.when(here)(local.start)
            pl.when(jnp.logical_not(here))(remote.start)

    def ready(half, parity):
        if parity:
            send_home(2 * half)
        else:
            pl.when(half > 0)(lambda: send_home(2 * half - 1))

    def finish_second(chunk, total):
        new = (rows_of(a_ref, chunk, 1).astype(F32) + total).astype(BF16)
        res_ref[pl.ds(chunk * CHUNK_ROWS, CHUNK_ROWS)] = new.reshape(CHUNK_ROWS, cols, channels)

    conv_loop(in_order, ready, lambda u_ref, chunk: fill_chunk(u_ref, h_ref, chunk, second, top_edge, bottom_edge),
              finish_second, u_even, u_odd, w_vmem.at[1])
    send_home(jnp.int32(CHUNKS - 1))
    for chunk in range(CHUNKS):
        for col in range(2):
            here, remote, _ = home_copies(jnp.int32(chunk), col)
            pl.when(jnp.logical_not(here))(remote.wait_send)
    for slot in range(4):
        for part in range(per_tile):
            landed = out_ref.at[slot, pl.ds(part * CHUNK_ROWS, CHUNK_ROWS)]
            pltpu.make_async_copy(landed, landed, tile_rsem.at[slot, part]).wait()


def attention_kernel(norm_idx, count, logit_scale, a_hbm, stat_in, scale_ref, shift_ref, w_hbm, wo_hbm,
                     out_ref, stat_ref, a_ref, n_ref, q_ref, k_ref, v_ref, s_even, s_odd, peak_ref, o_ref,
                     wq_ref, wk_ref, wv_ref, wo_ref, acc_ref,
                     st_send, st_recv, load_sem, head_sem, st_ssem, st_rsem, kv_ssem, kv_rsem):
    tokens, channels = a_ref.shape
    heads, head_dim, _ = v_ref.shape
    loads = [pltpu.make_async_copy(src, dst, load_sem.at[i])
             for i, (src, dst) in enumerate(((a_hbm, a_ref), (w_hbm.at[2], wv_ref), (w_hbm.at[0], wq_ref), (wo_hbm, wo_ref)))]
    head_loads = [pltpu.make_async_copy(w_hbm.at[1, pl.ds(head * head_dim, head_dim)],
                                        wk_ref.at[pl.ds(head * LANES, head_dim)], head_sem.at[head])
                  for head in range(heads)]
    for load in loads[:2] + head_loads + loads[2:]:
        load.start()
    for head in range(heads):
        wk_ref[head * LANES + head_dim:(head + 1) * LANES] = jnp.zeros((LANES - head_dim, channels), BF16)
        q_ref[head, head_dim:] = jnp.zeros((LANES - head_dim, tokens), BF16)
    st_send[0] = stat_in[...]
    barrier_pair()
    sums = exchange(0, st_send, st_recv, st_ssem, st_rsem)
    mean, inv_std = norm_params(sums, count)
    gain = inv_std * scale_ref[norm_idx:norm_idx + 1].astype(F32)
    shift = shift_ref[norm_idx:norm_idx + 1].astype(F32)
    loads[0].wait()
    loads[1].wait()
    for load in head_loads:
        load.wait()

    step = TOKEN_BLOCK
    chunks = tokens // step
    transposed = (((1,), (1,)), ((), ()))

    def kv_copy(which, chunk):
        if which:
            ref, axis_index = v_ref, (slice(None), slice(None))
        else:
            ref, axis_index = k_ref, (slice(None),)
        return pltpu.make_async_remote_copy(
            src_ref=ref.at[axis_index + (pl.ds(pl.multiple_of(chunk * step, step), step),)],
            dst_ref=ref.at[axis_index + (pl.ds(pl.multiple_of(tokens + chunk * step, step), step),)],
            send_sem=kv_ssem.at[which, chunk],
            recv_sem=kv_rsem.at[which, chunk],
            device_id=partner_id(),
            device_id_type=MESH,
        )

    def key_values(i, carry):
        here = pl.ds(pl.multiple_of(i * step, step), step)
        normed = ((a_ref[here].astype(F32) - mean) * gain + shift).astype(BF16)
        n_ref[here] = normed
        part = lax.dot_general(normed, wk_ref[...], transposed, preferred_element_type=F32).astype(BF16)
        for head in range(heads):
            k_ref[head, here] = part[:, head * LANES:(head + 1) * LANES]
        part = lax.dot_general(wv_ref[...], normed, transposed, preferred_element_type=F32).astype(BF16)
        for head in range(heads):
            v_ref[head, :, here] = part[head * head_dim:(head + 1) * head_dim]

        @pl.when(i > 0)
        def _():
            kv_copy(0, i - 1).start()
            kv_copy(1, i - 1).start()
        return carry

    lax.fori_loop(0, chunks, key_values, 0)
    loads[2].wait()

    def queries(i, carry):
        here = pl.ds(pl.multiple_of(i * step, step), step)
        part = lax.dot_general(wq_ref[...], n_ref[here], transposed, preferred_element_type=F32).astype(BF16)
        for head in range(heads):
            q_ref[head, 0:head_dim, here] = part[head * head_dim:(head + 1) * head_dim]

        @pl.when(i == 0)
        def _():
            kv_copy(0, chunks - 1).start()
            kv_copy(1, chunks - 1).start()
        return carry

    lax.fori_loop(0, chunks, queries, 0)

    def arrived(i, carry):
        kv_copy(0, i).wait()
        kv_copy(1, i).wait()
        return carry

    lax.fori_loop(0, chunks, arrived, 0)

    blocks = tokens // QUERY_BLOCK
    key_blocks = 2 * tokens // KEY_BLOCK

    def fold(value, combine):
        return combine(value.reshape(KEY_BLOCK // 8, 8, QUERY_BLOCK), axis=0)

    def interleaved(i, s_ref, s_next, slot):
        if i is not None:
            head = lax.div(i, blocks)
            here = pl.ds(pl.multiple_of(lax.rem(i, blocks) * QUERY_BLOCK, QUERY_BLOCK), QUERY_BLOCK)
            peak = jnp.max(peak_ref[slot], axis=0, keepdims=True)
            after = jnp.minimum(i + 1, heads * blocks - 1)
        else:
            after = 0
        next_head = lax.div(after, blocks)
        next_here = pl.ds(pl.multiple_of(lax.rem(after, blocks) * QUERY_BLOCK, QUERY_BLOCK), QUERY_BLOCK)
        query = q_ref[next_head, :, next_here]
        next_peak, total, attended = None, None, None
        for j in range(key_blocks):
            keys = slice(j * KEY_BLOCK, (j + 1) * KEY_BLOCK)
            scores = jnp.dot(k_ref[next_head, keys], query, preferred_element_type=F32)
            s_next[keys] = scores
            piece = fold(scores, jnp.max)
            next_peak = piece if next_peak is None else jnp.maximum(next_peak, piece)
            if i is not None:
                weights = jnp.exp2((s_ref[keys] - peak) * logit_scale)
                piece = fold(weights, jnp.sum)
                total = piece if total is None else total + piece
                term = jnp.dot(v_ref[head, :, keys], weights.astype(BF16), preferred_element_type=F32)
                attended = term if attended is None else attended + term
        peak_ref[1 - slot] = next_peak
        if i is not None:
            total = jnp.sum(total, axis=0, keepdims=True)
            rows = pl.ds(pl.multiple_of(head * head_dim, 16), head_dim)
            o_ref[rows, here] = (attended / total).astype(BF16)

    interleaved(None, None, s_even, 1)

    def attend(i, carry):
        interleaved(2 * i, s_even, s_odd, 0)
        interleaved(2 * i + 1, s_odd, s_even, 1)
        return carry

    lax.fori_loop(0, heads * blocks // 2, attend, 0)
    loads[3].wait()
    acc_ref[...] = jnp.zeros_like(acc_ref)

    def project(i, carry):
        here = pl.ds(pl.multiple_of(i * step, step), step)
        added = lax.dot_general(o_ref[:, here], wo_ref[...], (((0,), (0,)), ((), ())), preferred_element_type=F32)
        new = (a_ref[here].astype(F32) + added).astype(BF16)
        out_ref[here] = new
        add_moments(acc_ref, new.astype(F32))
        return carry

    lax.fori_loop(0, chunks, project, 0)
    stat_ref[...] = moment_rows(acc_ref)


VMEM_SPEC = pl.BlockSpec(memory_space=pltpu.VMEM)
ANY_SPEC = pl.BlockSpec(memory_space=pl.ANY)


def params(collective_id):
    return pltpu.CompilerParams(collective_id=collective_id, has_side_effects=True, vmem_limit_bytes=60 * 2**20)


def conv_scratch(rows, cols, channels):
    return [
        pltpu.VMEM((rows + 2, cols, channels), BF16),
        pltpu.VMEM((rows + 2, cols, channels), BF16),
        pltpu.VMEM((CHUNK_ROWS + 2, cols, 3 * channels), BF16),
        pltpu.VMEM((CHUNK_ROWS + 2, cols, 3 * channels), BF16),
        pltpu.VMEM((2, 9 * channels, channels), BF16),
    ]


def first_call(count, rows, cols, x, time_emb, scale, shift, w, time_w):
    channels = x.shape[3]
    dma = pltpu.SemaphoreType.DMA
    return pl.pallas_call(
        functools.partial(first_kernel, count),
        out_shape=[
            jax.ShapeDtypeStruct((rows, cols, channels), BF16),
            jax.ShapeDtypeStruct((8, channels), F32),
            jax.ShapeDtypeStruct((8, channels), F32),
        ],
        in_specs=[ANY_SPEC, VMEM_SPEC, VMEM_SPEC, VMEM_SPEC, ANY_SPEC, ANY_SPEC],
        out_specs=[VMEM_SPEC, VMEM_SPEC, VMEM_SPEC],
        scratch_shapes=[pltpu.VMEM(x.shape, BF16)] + conv_scratch(rows, cols, channels) + [
            pltpu.VMEM(time_w.shape, BF16),
            pltpu.VMEM((2, 8, channels), F32),
            pltpu.VMEM((2, 8, channels), F32),
            pltpu.VMEM((8, 8, LANES), F32),
            pltpu.VMEM((8, LANES), F32),
            pltpu.VMEM((1, 8, channels), F32),
            pltpu.VMEM((1, 8, channels), F32),
            dma((4,)), dma((7,)), dma((8,)), dma((1,)), dma((1,)), dma, dma,
            dma((4, len(PIECES))), dma((len(PIECES), 4)), dma((4,)), dma((2,)),
        ],
        compiler_params=params(0),
        name="res_first",
    )(x, time_emb, scale, shift, w, time_w)


def second_call(count, tile_shape, a, stats, time_vec, scale, shift, w):
    rows, cols, channels = a.shape
    dma = pltpu.SemaphoreType.DMA
    return pl.pallas_call(
        functools.partial(second_kernel, count),
        out_shape=jax.ShapeDtypeStruct(tile_shape, BF16),
        in_specs=[ANY_SPEC, VMEM_SPEC, VMEM_SPEC, VMEM_SPEC, VMEM_SPEC, ANY_SPEC],
        out_specs=ANY_SPEC,
        scratch_shapes=conv_scratch(rows, cols, channels) + [
            pltpu.VMEM((2, 8, channels), F32),
            pltpu.VMEM((rows, cols, channels), BF16),
            pltpu.VMEM((2, 8, channels), F32),
            pltpu.VMEM((2, 8, channels), F32),
            dma((3,)), dma((2,)), dma((2,)), dma((2,)), dma((2,)), dma((CHUNKS, 2)), dma((4, CHUNKS // 2)),
        ],
        compiler_params=params(2),
        name="res_second",
    )(a, stats, time_vec, scale, shift, w)


def attention_call(norm_idx, count, heads, a, stats, scale, shift, w, wo):
    tokens, channels = a.shape
    head_dim = channels // heads
    logit_scale = head_dim ** -0.5 * 1.4426950408889634
    return pl.pallas_call(
        functools.partial(attention_kernel, norm_idx, count, logit_scale),
        out_shape=[jax.ShapeDtypeStruct((tokens, channels), BF16), jax.ShapeDtypeStruct((8, channels), F32)],
        in_specs=[ANY_SPEC, VMEM_SPEC, VMEM_SPEC, VMEM_SPEC, ANY_SPEC, ANY_SPEC],
        out_specs=[VMEM_SPEC, VMEM_SPEC],
        scratch_shapes=[
            pltpu.VMEM((tokens, channels), BF16),
            pltpu.VMEM((tokens, channels), BF16),
            pltpu.VMEM((heads, LANES, tokens), BF16),
            pltpu.VMEM((heads, 2 * tokens, LANES), BF16),
            pltpu.VMEM((heads, head_dim, 2 * tokens), BF16),
            pltpu.VMEM((2 * tokens, QUERY_BLOCK), F32),
            pltpu.VMEM((2 * tokens, QUERY_BLOCK), F32),
            pltpu.VMEM((2, 8, QUERY_BLOCK), F32),
            pltpu.VMEM((channels, tokens), BF16),
            pltpu.VMEM((channels, channels), BF16),
            pltpu.VMEM((heads * LANES, channels), BF16),
            pltpu.VMEM((channels, channels), BF16),
            pltpu.VMEM((channels, channels), BF16),
            pltpu.VMEM((2, 8, channels), F32),
            pltpu.VMEM((1, 8, channels), F32),
            pltpu.VMEM((1, 8, channels), F32),
            pltpu.SemaphoreType.DMA((4,)),
            pltpu.SemaphoreType.DMA((heads,)),
            pltpu.SemaphoreType.DMA((1,)),
            pltpu.SemaphoreType.DMA((1,)),
            pltpu.SemaphoreType.DMA((2, tokens // TOKEN_BLOCK)),
            pltpu.SemaphoreType.DMA((2, tokens // TOKEN_BLOCK)),
        ],
        compiler_params=params(1),
        name="attention",
    )(a, stats, scale, shift, w, wo)


def solution(mesh):
    lat_spec = P("dp", "sp", "sp2", None)

    def local(x, time_emb, gn_scale, gn_shift, conv_w, time_w, w_qkv, w_out):
        images, tile_rows, tile_cols, channels = x.shape
        rows, cols = 2 * tile_rows, 2 * tile_cols
        count = 2 * rows * cols * (channels // GROUPS)
        heads = w_out.shape[0]
        w = conv_w.reshape(4, 9 * channels, channels)
        qkv = jnp.transpose(w_qkv, (0, 2, 3, 1)).reshape(3, channels, channels)
        wo = w_out.reshape(channels, channels)
        first, stats, time_vec = first_call(count, rows, cols, x, time_emb, gn_scale, gn_shift, w, time_w)
        middle, stats = attention_call(2, count, heads, first.reshape(rows * cols, channels), stats, gn_scale, gn_shift, qkv, wo)
        return second_call(count, x.shape, middle.reshape(rows, cols, channels), stats, time_vec, gn_scale, gn_shift, w)

    return jax.shard_map(local, mesh=mesh, in_specs=(lat_spec, P("dp", None), P(), P(), P(), P(), P(), P()), out_specs=lat_spec, check_vma=False)
```

```python
import functools

import jax
import jax.numpy as jnp
from jax import lax
from jax.experimental import pallas as pl
from jax.experimental.pallas import tpu as pltpu
from jax.sharding import PartitionSpec as P

GROUPS = 32
NORM_EPS = 1e-5
LANES = 128
CHUNK_ROWS = 4
CHUNKS = 8
PIECES = ((0, 5), (5, 4), (9, 4), (13, 3))
QUERY_BLOCK = 512
KEY_BLOCK = 512
TOKEN_BLOCK = 512
MESH = pl.DeviceIdType.MESH
F32 = jnp.float32
BF16 = jnp.bfloat16


def position():
    sp = lax.axis_index("sp")
    return lax.div(sp, 2), lax.rem(sp, 2), lax.axis_index("sp2")


def partner_id():
    chip_x, core, _ = position()
    return {"sp": 2 * chip_x + 1 - core}


def barrier_pair():
    sem = pltpu.get_barrier_semaphore()
    pl.semaphore_signal(sem, inc=1, device_id=partner_id(), device_id_type=MESH)
    pl.semaphore_wait(sem, 1)


def others():
    sp, col = lax.axis_index("sp"), lax.axis_index("sp2")
    return [(lax.rem(sp + i, 4), lax.rem(col + j, 2)) for i in range(4) for j in range(2) if i or j]


def signal_all():
    for sp, col in others():
        pl.semaphore_signal(pltpu.get_barrier_semaphore(), inc=1, device_id={"sp": sp, "sp2": col}, device_id_type=MESH)


def wait_all():
    pl.semaphore_wait(pltpu.get_barrier_semaphore(), 7)


def split3(value):
    high = value.astype(BF16).astype(F32)
    rest = value - high
    mid = rest.astype(BF16).astype(F32)
    low = rest - mid
    return jnp.concatenate([high, mid, low, jnp.zeros_like(value)], axis=0).astype(BF16)


def exact_dot(value, one_hot):
    out = jnp.dot(split3(value), one_hot, preferred_element_type=F32)
    return out[0:8] + out[8:16] + out[16:24]


def group_matrices(channels):
    width = channels // GROUPS
    chan = lax.broadcasted_iota(jnp.int32, (channels, LANES), 0)
    grp = lax.broadcasted_iota(jnp.int32, (channels, LANES), 1) * width
    gather = jnp.where((chan >= grp) & (chan < grp + width), 1.0, 0.0).astype(BF16)
    chan_t = lax.broadcasted_iota(jnp.int32, (LANES, channels), 1)
    grp_t = lax.broadcasted_iota(jnp.int32, (LANES, channels), 0) * width
    spread = jnp.where((chan_t >= grp_t) & (chan_t < grp_t + width), 1.0, 0.0).astype(BF16)
    return gather, spread


def spread_groups(group_sums, spread, count):
    mean = group_sums[0:1] / count
    inv_std = lax.rsqrt(group_sums[1:2] / count - mean * mean + NORM_EPS)
    stacked = jnp.concatenate([mean, inv_std, jnp.zeros((6, LANES), F32)], axis=0)
    per_channel = exact_dot(stacked, spread)
    return per_channel[0:1], per_channel[1:2]


def norm_params(sums, count):
    gather, spread = group_matrices(sums.shape[1])
    return spread_groups(exact_dot(sums, gather)[0:2], spread, count)


def fold_rows(value):
    rows, channels = value.shape
    return jnp.sum(value.reshape(rows // 8, 8, channels), axis=0)


def add_moments(acc_ref, value):
    acc_ref[0] += fold_rows(value)
    acc_ref[1] += fold_rows(value * value)


def moment_rows(acc_ref):
    total = jnp.sum(acc_ref[0], axis=0, keepdims=True)
    square = jnp.sum(acc_ref[1], axis=0, keepdims=True)
    return jnp.concatenate([total, square, jnp.zeros((6, total.shape[1]), F32)], axis=0)


def exchange(slot, send_ref, recv_ref, send_sem, recv_sem):
    copy = pltpu.make_async_remote_copy(
        src_ref=send_ref.at[slot],
        dst_ref=recv_ref.at[slot],
        send_sem=send_sem.at[slot],
        recv_sem=recv_sem.at[slot],
        device_id=partner_id(),
        device_id_type=MESH,
    )
    copy.start()
    copy.wait()
    return send_ref[slot] + recv_ref[slot]


def silu(value):
    half = 0.5 * value
    return half + half * jnp.tanh(half)


def fill_chunk(u_ref, src_ref, chunk, params, top_edge, bottom_edge):
    mean, gain, shift = params
    _, cols, channels = src_ref.shape
    place = lax.broadcasted_iota(jnp.int32, (cols, channels), 0)
    last = CHUNK_ROWS + 1
    for j in range(CHUNK_ROWS + 2):
        value = silu((src_ref[chunk * CHUNK_ROWS + j].astype(F32) - mean) * gain + shift)
        if j == 0:
            value = jnp.where(top_edge & (chunk == 0), 0.0, value)
        if j == last:
            value = jnp.where(bottom_edge & (chunk == CHUNKS - 1), 0.0, value)
        before = jnp.where(place == 0, 0.0, pltpu.roll(value, 1, 0))
        after = jnp.where(place == cols - 1, 0.0, pltpu.roll(value, cols - 1, 0))
        u_ref[j, :, 0:channels] = before.astype(BF16)
        u_ref[j, :, channels:2 * channels] = value.astype(BF16)
        u_ref[j, :, 2 * channels:3 * channels] = after.astype(BF16)


def conv_chunk(u_ref, w):
    _, cols, depth = u_ref.shape
    lhs = jnp.concatenate([u_ref[dy:dy + CHUNK_ROWS].reshape(CHUNK_ROWS * cols, depth) for dy in range(3)], axis=1)
    return jnp.dot(lhs, w[...], preferred_element_type=F32)


def conv_loop(order, ready, fill, finish, u_even, u_odd, w, arriving=False):
    def step(i, half, parity, u_now, u_next):
        after = jnp.minimum(i + 1, CHUNKS - 1)
        if arriving:
            finish(order(i), conv_chunk(u_now, w))
            ready(half, parity)
            fill(u_next, order(after))
        else:
            ready(half, parity)
            fill(u_next, order(after))
            finish(order(i), conv_chunk(u_now, w))

    def pair(half, carry):
        step(2 * half, half, 0, u_even, u_odd)
        step(2 * half + 1, half, 1, u_odd, u_even)
        return carry

    fill(u_even, order(jnp.int32(0)))
    lax.fori_loop(0, CHUNKS // 2, pair, 0)


def in_order(i):
    return i


def from_ends(i):
    return lax.rem(i + 1, 2) * lax.div(i, 2) + lax.rem(i, 2) * (CHUNKS - 1 - lax.div(i, 2))


def rows_of(ref, chunk, first=0):
    value = ref[pl.ds(chunk * CHUNK_ROWS + first, CHUNK_ROWS)]
    return value.reshape(value.shape[0] * value.shape[1], value.shape[2])


def send_edge_row(ref, send_sem, recv_sem, src_ref=None, src_row=None):
    rows = ref.shape[0] - 2
    core = position()[1]
    src = ref.at[rows - (rows - 1) * core] if src_ref is None else src_ref.at[src_row]
    return pltpu.make_async_remote_copy(
        src_ref=src, dst_ref=ref.at[(rows + 1) * core],
        send_sem=send_sem, recv_sem=recv_sem, device_id=partner_id(), device_id_type=MESH)


def first_kernel(count, x_ref, emb_ref, scale_ref, shift_ref, w_ref, tw_ref, out_ref, stat_ref, time_ref,
                 x_vmem, a_ref, h_ref, u_even, u_odd, w_vmem, tw_vmem, acc_ref, time_all, grp_recv, grp_total, st_send, st_recv,
                 load_sem, grp_ssem, grp_rsem, st_ssem, st_rsem, edge_ssem, edge_rsem, piece_ssem, piece_rsem, halo_ssem, halo_rsem):
    images, tile_rows, tile_cols, channels = x_ref.shape
    rows = 2 * tile_rows
    chip_x, core, chip_y = position()
    sp = lax.axis_index("sp")
    me = 2 * sp + chip_y
    image = 2 * chip_x + chip_y

    signal_all()
    x_load = pltpu.make_async_copy(x_ref, x_vmem, load_sem.at[0])
    x_load.start()
    weights = [pltpu.make_async_copy(w_ref.at[k], w_vmem.at[k], load_sem.at[1 + k]) for k in range(2)]
    tw_load = pltpu.make_async_copy(tw_ref, tw_vmem, load_sem.at[3])
    for copy in weights[:1] + [tw_load] + weights[1:]:
        copy.start()

    def piece(part, source_core):
        low, high = PIECES[part]
        start = (1 - source_core) * low + source_core * (tile_rows - low - high)
        return pl.ds(start, high), pl.ds(1 + source_core * tile_rows + start, high)

    def piece_copies(k, part):
        to_x, to_y = lax.rem(chip_x + k // 2, 2), lax.rem(chip_y + k % 2, 2)
        src_rows, dst_rows = piece(part, core)
        src = x_ref.at[2 * to_x + to_y, src_rows]
        dst = a_ref.at[dst_rows, pl.ds(chip_y * tile_cols, tile_cols)]
        landed = piece_rsem.at[part, 2 * chip_y + core]
        remote = pltpu.make_async_remote_copy(
            src_ref=src, dst_ref=dst, send_sem=piece_ssem.at[k, part], recv_sem=landed,
            device_id={"sp": 2 * to_x + chip_x, "sp2": to_y}, device_id_type=MESH)
        return remote, pltpu.make_async_copy(src, dst, landed)

    def halo_copies(k):
        to_x, to_y = lax.rem(chip_x + k // 2, 2), lax.rem(chip_y + k % 2, 2)
        src = x_ref.at[2 * to_x + to_y, (tile_rows - 1) * core]
        dst = a_ref.at[(rows + 1) * chip_x, pl.ds(chip_y * tile_cols, tile_cols)]
        remote = pltpu.make_async_remote_copy(
            src_ref=src, dst_ref=dst, send_sem=halo_ssem.at[k], recv_sem=halo_rsem.at[chip_y],
            device_id={"sp": 2 * to_x + 1 - chip_x, "sp2": to_y}, device_id_type=MESH)
        return remote, pltpu.make_async_copy(src, dst, halo_rsem.at[chip_y])

    at_home = core == chip_x
    far_first = (3, 2, 1, 0)

    def send_piece(part):
        for k in far_first:
            remote, local = piece_copies(k, part)
            if k:
                remote.start()
            else:
                pl.when(at_home)(local.start)
                pl.when(jnp.logical_not(at_home))(remote.start)

    wait_all()

    @pl.when(jnp.logical_not(at_home))
    def _():
        for k in far_first:
            halo_copies(k)[0 if k else 1].start()

    send_piece(0)

    gather, spread = group_matrices(channels)
    x_load.wait()
    moments = []
    for i in range(images):
        acc_ref[...] = jnp.zeros_like(acc_ref)

        def add_row(row, carry):
            add_moments(acc_ref, x_vmem[i, row].astype(F32))
            return carry

        lax.fori_loop(0, tile_rows, add_row, 0)
        moments += [jnp.sum(acc_ref[0], axis=0, keepdims=True), jnp.sum(acc_ref[1], axis=0, keepdims=True)]
    grp_recv[me] = exact_dot(jnp.concatenate(moments, axis=0), gather)
    group_copies = []
    for k, (to_sp, to_y) in enumerate(others()):
        copy = pltpu.make_async_remote_copy(
            src_ref=grp_recv.at[me], dst_ref=grp_recv.at[me], send_sem=grp_ssem.at[k], recv_sem=grp_rsem.at[me],
            device_id={"sp": to_sp, "sp2": to_y}, device_id_type=MESH)
        copy.start()
        group_copies.append((copy, 2 * to_sp + to_y))

    for part in range(1, len(PIECES)):
        send_piece(part)

    tw_load.wait()
    emb = silu(emb_ref[...].astype(F32)).astype(BF16)
    for k in range(2):
        time_all[k, 0:images] = jnp.dot(emb, tw_vmem[k], preferred_element_type=F32)
    time_ref[...] = jnp.broadcast_to(time_all[1, pl.ds(image, 1)], time_ref.shape)
    time_vec = time_all[0, pl.ds(image, 1)]

    total = jnp.zeros((8, LANES), F32)
    for copy, _ in group_copies:
        copy.wait_send()
    for copy, sender in group_copies:
        pltpu.make_async_copy(grp_recv.at[sender], grp_recv.at[sender], grp_rsem.at[sender]).wait()
    for slot in range(8):
        total = total + grp_recv[slot]
    grp_total[...] = total
    mean, inv_std = spread_groups(grp_total[pl.ds(2 * image, 2)], spread, count)

    def wait_piece(part, source_core):
        for col in range(2):
            landed = a_ref.at[piece(part, source_core)[1], pl.ds(col * tile_cols, tile_cols)]
            pltpu.make_async_copy(landed, landed, piece_rsem.at[part, 2 * col + source_core]).wait()

    def ready(half, parity):
        if parity == 0:
            for part in range(3):
                pl.when(half == part)(functools.partial(wait_piece, part, 1))
        else:
            for part in range(1, 4):
                pl.when(half + 1 == part)(functools.partial(wait_piece, part, 0))
            pl.when(half + 1 == 3)(functools.partial(wait_piece, 3, 1))

    top_edge, bottom_edge = core == 0, core == 1

    def norm(k, mean, inv_std):
        return mean, inv_std * scale_ref[k:k + 1].astype(F32), shift_ref[k:k + 1].astype(F32)

    params = norm(0, mean, inv_std)
    for col in range(2):
        landed = a_ref.at[(rows + 1) * (1 - core), pl.ds(col * tile_cols, tile_cols)]
        pltpu.make_async_copy(landed, landed, halo_rsem.at[col]).wait()
    wait_piece(0, 0)
    acc_ref[...] = jnp.zeros_like(acc_ref)
    weights[0].wait()

    def finish_first(chunk, total):
        hidden = (total + time_vec).astype(BF16)
        h_ref[pl.ds(chunk * CHUNK_ROWS + 1, CHUNK_ROWS)] = hidden.reshape(CHUNK_ROWS, 2 * tile_cols, channels)
        add_moments(acc_ref, hidden.astype(F32))

    conv_loop(from_ends, ready, lambda u_ref, chunk: fill_chunk(u_ref, a_ref, chunk, params, top_edge, bottom_edge),
              finish_first, u_even, u_odd, w_vmem.at[0], arriving=True)

    edge = send_edge_row(h_ref, edge_ssem, edge_rsem)
    edge.start()
    st_send[0] = moment_rows(acc_ref)
    acc_ref[...] = jnp.zeros_like(acc_ref)
    weights[1].wait()
    second = norm(1, *norm_params(exchange(0, st_send, st_recv, st_ssem, st_rsem), count))
    edge.wait()

    def finish_second(chunk, total):
        new = (rows_of(a_ref, chunk, 1).astype(F32) + total).astype(BF16)
        out_ref[pl.ds(chunk * CHUNK_ROWS, CHUNK_ROWS)] = new.reshape(CHUNK_ROWS, 2 * tile_cols, channels)
        add_moments(acc_ref, new.astype(F32))

    conv_loop(in_order, lambda half, parity: None,
              lambda u_ref, chunk: fill_chunk(u_ref, h_ref, chunk, second, top_edge, bottom_edge),
              finish_second, u_even, u_odd, w_vmem.at[1])
    stat_ref[...] = moment_rows(acc_ref)

    @pl.when(jnp.logical_not(at_home))
    def _():
        for k in (1, 2, 3):
            halo_copies(k)[0].wait_send()

    for part in range(len(PIECES)):
        for k in range(4):
            remote, _ = piece_copies(k, part)
            if k:
                remote.wait_send()
            else:
                pl.when(jnp.logical_not(at_home))(remote.wait_send)


def second_kernel(count, a_hbm, stat_in, time_ref, scale_ref, shift_ref, w_ref, out_ref,
                  a_ref, h_ref, u_even, u_odd, w_vmem, acc_ref, res_ref, st_send, st_recv,
                  load_sem, st_ssem, st_rsem, edge_ssem, edge_rsem, tile_ssem, tile_rsem):
    rows, cols, channels = res_ref.shape
    tile_rows, tile_cols = rows // 2, cols // 2
    chip_x, core, chip_y = position()
    sp = lax.axis_index("sp")
    image = 2 * chip_x + chip_y

    signal_all()
    a_load = pltpu.make_async_copy(a_hbm, a_ref.at[pl.ds(1, rows)], load_sem.at[0])
    a_load.start()
    weights = [pltpu.make_async_copy(w_ref.at[2 + k], w_vmem.at[k], load_sem.at[1 + k]) for k in range(2)]
    for copy in weights:
        copy.start()
    st_send[0] = stat_in[...]
    acc_ref[...] = jnp.zeros_like(acc_ref)
    wait_all()
    edge = send_edge_row(a_ref, edge_ssem.at[0], edge_rsem.at[0], a_hbm, (rows - 1) * (1 - core))
    edge.start()
    top_edge, bottom_edge = core == 0, core == 1

    def norm(k, sums):
        mean, inv_std = norm_params(sums, count)
        return mean, inv_std * scale_ref[3 + k:4 + k].astype(F32), shift_ref[3 + k:4 + k].astype(F32)

    params = norm(0, exchange(0, st_send, st_recv, st_ssem, st_rsem))
    a_load.wait()
    edge.wait()
    weights[0].wait()
    time_vec = time_ref[0:1]

    def finish_first(chunk, total):
        hidden = (total + time_vec).astype(BF16)
        h_ref[pl.ds(chunk * CHUNK_ROWS + 1, CHUNK_ROWS)] = hidden.reshape(CHUNK_ROWS, cols, channels)
        add_moments(acc_ref, hidden.astype(F32))

    conv_loop(in_order, lambda half, parity: None,
              lambda u_ref, chunk: fill_chunk(u_ref, a_ref, chunk, params, top_edge, bottom_edge),
              finish_first, u_even, u_odd, w_vmem.at[0])

    edge = send_edge_row(h_ref, edge_ssem.at[1], edge_rsem.at[1])
    edge.start()
    st_send[1] = moment_rows(acc_ref)
    weights[1].wait()
    second = norm(1, exchange(1, st_send, st_recv, st_ssem, st_rsem))
    edge.wait()

    per_tile = CHUNKS // 2

    def home_copies(chunk, col):
        to_sp = 2 * core + lax.div(chunk, per_tile)
        slot = lax.rem(chunk, per_tile)
        here = (to_sp == sp) & (chip_y == col)
        src = res_ref.at[pl.ds(chunk * CHUNK_ROWS, CHUNK_ROWS), pl.ds(col * tile_cols, tile_cols)]
        dst = out_ref.at[image, pl.ds(slot * CHUNK_ROWS, CHUNK_ROWS)]
        landed = tile_rsem.at[image, slot]
        remote = pltpu.make_async_remote_copy(
            src_ref=src, dst_ref=dst, send_sem=tile_ssem.at[chunk, col], recv_sem=landed,
            device_id={"sp": to_sp, "sp2": col}, device_id_type=MESH)
        return here, remote, pltpu.make_async_copy(src, dst, landed)

    def send_home(chunk):
        for col in range(2):
            here, remote, local = home_copies(chunk, col)
            pl.when(here)(local.start)
            pl.when(jnp.logical_not(here))(remote.start)

    def ready(half, parity):
        if parity:
            send_home(2 * half)
        else:
            pl.when(half > 0)(lambda: send_home(2 * half - 1))

    def finish_second(chunk, total):
        new = (rows_of(a_ref, chunk, 1).astype(F32) + total).astype(BF16)
        res_ref[pl.ds(chunk * CHUNK_ROWS, CHUNK_ROWS)] = new.reshape(CHUNK_ROWS, cols, channels)

    conv_loop(in_order, ready, lambda u_ref, chunk: fill_chunk(u_ref, h_ref, chunk, second, top_edge, bottom_edge),
              finish_second, u_even, u_odd, w_vmem.at[1])
    send_home(jnp.int32(CHUNKS - 1))
    for chunk in range(CHUNKS):
        for col in range(2):
            here, remote, _ = home_copies(jnp.int32(chunk), col)
            pl.when(jnp.logical_not(here))(remote.wait_send)
    for slot in range(4):
        for part in range(per_tile):
            landed = out_ref.at[slot, pl.ds(part * CHUNK_ROWS, CHUNK_ROWS)]
            pltpu.make_async_copy(landed, landed, tile_rsem.at[slot, part]).wait()


def attention_kernel(norm_idx, count, logit_scale, a_hbm, stat_in, scale_ref, shift_ref, w_hbm, wo_hbm,
                     out_ref, stat_ref, a_ref, n_ref, q_ref, k_ref, v_ref, s_even, s_odd, peak_ref, o_ref,
                     wq_ref, wk_ref, wv_ref, wo_ref, acc_ref,
                     st_send, st_recv, load_sem, head_sem, st_ssem, st_rsem, kv_ssem, kv_rsem):
    tokens, channels = a_ref.shape
    heads, head_dim, _ = v_ref.shape
    loads = [pltpu.make_async_copy(src, dst, load_sem.at[i])
             for i, (src, dst) in enumerate(((a_hbm, a_ref), (w_hbm.at[2], wv_ref), (w_hbm.at[0], wq_ref), (wo_hbm, wo_ref)))]
    head_loads = [pltpu.make_async_copy(w_hbm.at[1, pl.ds(head * head_dim, head_dim)],
                                        wk_ref.at[pl.ds(head * LANES, head_dim)], head_sem.at[head])
                  for head in range(heads)]
    for load in loads[:2] + head_loads + loads[2:]:
        load.start()
    for head in range(heads):
        wk_ref[head * LANES + head_dim:(head + 1) * LANES] = jnp.zeros((LANES - head_dim, channels), BF16)
        q_ref[head, head_dim:] = jnp.zeros((LANES - head_dim, tokens), BF16)
    st_send[0] = stat_in[...]
    barrier_pair()
    sums = exchange(0, st_send, st_recv, st_ssem, st_rsem)
    mean, inv_std = norm_params(sums, count)
    gain = inv_std * scale_ref[norm_idx:norm_idx + 1].astype(F32)
    shift = shift_ref[norm_idx:norm_idx + 1].astype(F32)
    loads[0].wait()
    loads[1].wait()
    for load in head_loads:
        load.wait()

    step = TOKEN_BLOCK
    chunks = tokens // step
    transposed = (((1,), (1,)), ((), ()))

    def head_copy(which, head, chunk=None):
        first, size = (0, tokens) if chunk is None else (pl.multiple_of(chunk * step, step), step)
        src, dst = pl.ds(first, size), pl.ds(tokens + first, size)
        if which:
            src_ref, dst_ref = v_ref.at[head, :, src], v_ref.at[head, :, dst]
        else:
            src_ref, dst_ref = k_ref.at[head, src], k_ref.at[head, dst]
        slot = head if chunk is None else heads + chunk
        return pltpu.make_async_remote_copy(
            src_ref=src_ref, dst_ref=dst_ref, send_sem=kv_ssem.at[which, slot], recv_sem=kv_rsem.at[which, slot],
            device_id=partner_id(), device_id_type=MESH)

    def both(act, head, chunk=None):
        for which in range(2):
            getattr(head_copy(which, head, chunk), act)()

    def key_values(i, carry):
        here = pl.ds(pl.multiple_of(i * step, step), step)
        normed = ((a_ref[here].astype(F32) - mean) * gain + shift).astype(BF16)
        n_ref[here] = normed
        part = lax.dot_general(normed, wk_ref[...], transposed, preferred_element_type=F32).astype(BF16)
        for head in range(heads):
            k_ref[head, here] = part[:, head * LANES:(head + 1) * LANES]
        part = lax.dot_general(wv_ref[...], normed, transposed, preferred_element_type=F32).astype(BF16)
        for head in range(heads):
            v_ref[head, :, here] = part[head * head_dim:(head + 1) * head_dim]

        @pl.when(i > 0)
        def _():
            both("start", 0, i - 1)
        return carry

    lax.fori_loop(0, chunks, key_values, 0)
    loads[2].wait()

    def queries(i, carry):
        here = pl.ds(pl.multiple_of(i * step, step), step)
        part = lax.dot_general(wq_ref[...], n_ref[here], transposed, preferred_element_type=F32).astype(BF16)
        for head in range(heads):
            q_ref[head, 0:head_dim, here] = part[head * head_dim:(head + 1) * head_dim]

        @pl.when(i == 0)
        def _():
            both("start", 0, chunks - 1)
            for head in range(1, heads):
                both("start", head)
        return carry

    lax.fori_loop(0, chunks, queries, 0)

    for i in range(chunks):
        both("wait_recv", 0, i)

    blocks = tokens // QUERY_BLOCK
    key_blocks = 2 * tokens // KEY_BLOCK

    def fold(value, combine):
        return combine(value.reshape(KEY_BLOCK // 8, 8, QUERY_BLOCK), axis=0)

    def interleaved(i, s_ref, s_next, slot):
        if i is not None:
            head = lax.div(i, blocks)
            here = pl.ds(pl.multiple_of(lax.rem(i, blocks) * QUERY_BLOCK, QUERY_BLOCK), QUERY_BLOCK)
            peak = jnp.max(peak_ref[slot], axis=0, keepdims=True)
            after = jnp.minimum(i + 1, heads * blocks - 1)
        else:
            after = 0
        next_head = lax.div(after, blocks)
        next_here = pl.ds(pl.multiple_of(lax.rem(after, blocks) * QUERY_BLOCK, QUERY_BLOCK), QUERY_BLOCK)
        query = q_ref[next_head, :, next_here]
        next_peak, total, attended = None, None, None
        for j in range(key_blocks):
            keys = slice(j * KEY_BLOCK, (j + 1) * KEY_BLOCK)
            scores = jnp.dot(k_ref[next_head, keys], query, preferred_element_type=F32)
            s_next[keys] = scores
            piece = fold(scores, jnp.max)
            next_peak = piece if next_peak is None else jnp.maximum(next_peak, piece)
            if i is not None:
                weights = jnp.exp2((s_ref[keys] - peak) * logit_scale)
                piece = fold(weights, jnp.sum)
                total = piece if total is None else total + piece
                term = jnp.dot(v_ref[head, :, keys], weights.astype(BF16), preferred_element_type=F32)
                attended = term if attended is None else attended + term
        peak_ref[1 - slot] = next_peak
        if i is not None:
            total = jnp.sum(total, axis=0, keepdims=True)
            rows = pl.ds(pl.multiple_of(head * head_dim, 16), head_dim)
            o_ref[rows, here] = (attended / total).astype(BF16)

    interleaved(None, None, s_even, 1)

    def attend(i, carry):
        head = lax.div(2 * i + 2, blocks)
        pl.when((lax.rem(2 * i + 2, blocks) == 0) & (head < heads))(lambda: both("wait_recv", head))
        interleaved(2 * i, s_even, s_odd, 0)
        interleaved(2 * i + 1, s_odd, s_even, 1)
        return carry

    lax.fori_loop(0, heads * blocks // 2, attend, 0)
    for i in range(chunks):
        both("wait_send", 0, i)
    for head in range(1, heads):
        both("wait_send", head)
    loads[3].wait()
    acc_ref[...] = jnp.zeros_like(acc_ref)

    def project(i, carry):
        here = pl.ds(pl.multiple_of(i * step, step), step)
        added = lax.dot_general(o_ref[:, here], wo_ref[...], (((0,), (0,)), ((), ())), preferred_element_type=F32)
        new = (a_ref[here].astype(F32) + added).astype(BF16)
        out_ref[here] = new
        add_moments(acc_ref, new.astype(F32))
        return carry

    lax.fori_loop(0, chunks, project, 0)
    stat_ref[...] = moment_rows(acc_ref)


VMEM_SPEC = pl.BlockSpec(memory_space=pltpu.VMEM)
ANY_SPEC = pl.BlockSpec(memory_space=pl.ANY)


def params(collective_id):
    return pltpu.CompilerParams(collective_id=collective_id, has_side_effects=True, vmem_limit_bytes=60 * 2**20)


def conv_scratch(rows, cols, channels):
    return [
        pltpu.VMEM((rows + 2, cols, channels), BF16),
        pltpu.VMEM((rows + 2, cols, channels), BF16),
        pltpu.VMEM((CHUNK_ROWS + 2, cols, 3 * channels), BF16),
        pltpu.VMEM((CHUNK_ROWS + 2, cols, 3 * channels), BF16),
        pltpu.VMEM((2, 9 * channels, channels), BF16),
    ]


def first_call(count, rows, cols, x, time_emb, scale, shift, w, time_w):
    channels = x.shape[3]
    dma = pltpu.SemaphoreType.DMA
    return pl.pallas_call(
        functools.partial(first_kernel, count),
        out_shape=[
            jax.ShapeDtypeStruct((rows, cols, channels), BF16),
            jax.ShapeDtypeStruct((8, channels), F32),
            jax.ShapeDtypeStruct((8, channels), F32),
        ],
        in_specs=[ANY_SPEC, VMEM_SPEC, VMEM_SPEC, VMEM_SPEC, ANY_SPEC, ANY_SPEC],
        out_specs=[VMEM_SPEC, VMEM_SPEC, VMEM_SPEC],
        scratch_shapes=[pltpu.VMEM(x.shape, BF16)] + conv_scratch(rows, cols, channels) + [
            pltpu.VMEM(time_w.shape, BF16),
            pltpu.VMEM((2, 8, channels), F32),
            pltpu.VMEM((2, 8, channels), F32),
            pltpu.VMEM((8, 8, LANES), F32),
            pltpu.VMEM((8, LANES), F32),
            pltpu.VMEM((1, 8, channels), F32),
            pltpu.VMEM((1, 8, channels), F32),
            dma((4,)), dma((7,)), dma((8,)), dma((1,)), dma((1,)), dma, dma,
            dma((4, len(PIECES))), dma((len(PIECES), 4)), dma((4,)), dma((2,)),
        ],
        compiler_params=params(0),
        name="res_first",
    )(x, time_emb, scale, shift, w, time_w)


def second_call(count, tile_shape, a, stats, time_vec, scale, shift, w):
    rows, cols, channels = a.shape
    dma = pltpu.SemaphoreType.DMA
    return pl.pallas_call(
        functools.partial(second_kernel, count),
        out_shape=jax.ShapeDtypeStruct(tile_shape, BF16),
        in_specs=[ANY_SPEC, VMEM_SPEC, VMEM_SPEC, VMEM_SPEC, VMEM_SPEC, ANY_SPEC],
        out_specs=ANY_SPEC,
        scratch_shapes=conv_scratch(rows, cols, channels) + [
            pltpu.VMEM((2, 8, channels), F32),
            pltpu.VMEM((rows, cols, channels), BF16),
            pltpu.VMEM((2, 8, channels), F32),
            pltpu.VMEM((2, 8, channels), F32),
            dma((3,)), dma((2,)), dma((2,)), dma((2,)), dma((2,)), dma((CHUNKS, 2)), dma((4, CHUNKS // 2)),
        ],
        compiler_params=params(2),
        name="res_second",
    )(a, stats, time_vec, scale, shift, w)


def attention_call(norm_idx, count, heads, a, stats, scale, shift, w, wo):
    tokens, channels = a.shape
    head_dim = channels // heads
    logit_scale = head_dim ** -0.5 * 1.4426950408889634
    return pl.pallas_call(
        functools.partial(attention_kernel, norm_idx, count, logit_scale),
        out_shape=[jax.ShapeDtypeStruct((tokens, channels), BF16), jax.ShapeDtypeStruct((8, channels), F32)],
        in_specs=[ANY_SPEC, VMEM_SPEC, VMEM_SPEC, VMEM_SPEC, ANY_SPEC, ANY_SPEC],
        out_specs=[VMEM_SPEC, VMEM_SPEC],
        scratch_shapes=[
            pltpu.VMEM((tokens, channels), BF16),
            pltpu.VMEM((tokens, channels), BF16),
            pltpu.VMEM((heads, LANES, tokens), BF16),
            pltpu.VMEM((heads, 2 * tokens, LANES), BF16),
            pltpu.VMEM((heads, head_dim, 2 * tokens), BF16),
            pltpu.VMEM((2 * tokens, QUERY_BLOCK), F32),
            pltpu.VMEM((2 * tokens, QUERY_BLOCK), F32),
            pltpu.VMEM((2, 8, QUERY_BLOCK), F32),
            pltpu.VMEM((channels, tokens), BF16),
            pltpu.VMEM((channels, channels), BF16),
            pltpu.VMEM((heads * LANES, channels), BF16),
            pltpu.VMEM((channels, channels), BF16),
            pltpu.VMEM((channels, channels), BF16),
            pltpu.VMEM((2, 8, channels), F32),
            pltpu.VMEM((1, 8, channels), F32),
            pltpu.VMEM((1, 8, channels), F32),
            pltpu.SemaphoreType.DMA((4,)),
            pltpu.SemaphoreType.DMA((heads,)),
            pltpu.SemaphoreType.DMA((1,)),
            pltpu.SemaphoreType.DMA((1,)),
            pltpu.SemaphoreType.DMA((2, heads + tokens // TOKEN_BLOCK)),
            pltpu.SemaphoreType.DMA((2, heads + tokens // TOKEN_BLOCK)),
        ],
        compiler_params=params(1),
        name="attention",
    )(a, stats, scale, shift, w, wo)


def solution(mesh):
    lat_spec = P("dp", "sp", "sp2", None)

    def local(x, time_emb, gn_scale, gn_shift, conv_w, time_w, w_qkv, w_out):
        images, tile_rows, tile_cols, channels = x.shape
        rows, cols = 2 * tile_rows, 2 * tile_cols
        count = 2 * rows * cols * (channels // GROUPS)
        heads = w_out.shape[0]
        w = conv_w.reshape(4, 9 * channels, channels)
        qkv = jnp.transpose(w_qkv, (0, 2, 3, 1)).reshape(3, channels, channels)
        wo = w_out.reshape(channels, channels)
        first, stats, time_vec = first_call(count, rows, cols, x, time_emb, gn_scale, gn_shift, w, time_w)
        middle, stats = attention_call(2, count, heads, first.reshape(rows * cols, channels), stats, gn_scale, gn_shift, qkv, wo)
        return second_call(count, x.shape, middle.reshape(rows, cols, channels), stats, time_vec, gn_scale, gn_shift, w)

    return jax.shard_map(local, mesh=mesh, in_specs=(lat_spec, P("dp", None), P(), P(), P(), P(), P(), P()), out_specs=lat_spec, check_vma=False)
```

```python
import functools

import jax
import jax.numpy as jnp
from jax import lax
from jax.experimental import pallas as pl
from jax.experimental.pallas import tpu as pltpu
from jax.sharding import PartitionSpec as P

GROUPS = 32
NORM_EPS = 1e-5
LANES = 128
CHUNK_ROWS = 4
CHUNKS = 8
PIECES = ((0, 5), (5, 4), (9, 4), (13, 3))
QUERY_BLOCK = 512
KEY_BLOCK = 512
TOKEN_BLOCK = 512
MESH = pl.DeviceIdType.MESH
F32 = jnp.float32
BF16 = jnp.bfloat16


def position():
    sp = lax.axis_index("sp")
    return lax.div(sp, 2), lax.rem(sp, 2), lax.axis_index("sp2")


def partner_id():
    chip_x, core, _ = position()
    return {"sp": 2 * chip_x + 1 - core}


def barrier_pair():
    sem = pltpu.get_barrier_semaphore()
    pl.semaphore_signal(sem, inc=1, device_id=partner_id(), device_id_type=MESH)
    pl.semaphore_wait(sem, 1)


def others():
    sp, col = lax.axis_index("sp"), lax.axis_index("sp2")
    return [(lax.rem(sp + i, 4), lax.rem(col + j, 2)) for i in range(4) for j in range(2) if i or j]


def signal_all():
    for sp, col in others():
        pl.semaphore_signal(pltpu.get_barrier_semaphore(), inc=1, device_id={"sp": sp, "sp2": col}, device_id_type=MESH)


def wait_all():
    pl.semaphore_wait(pltpu.get_barrier_semaphore(), 7)


def split3(value):
    high = value.astype(BF16).astype(F32)
    rest = value - high
    mid = rest.astype(BF16).astype(F32)
    low = rest - mid
    return jnp.concatenate([high, mid, low, jnp.zeros_like(value)], axis=0).astype(BF16)


def exact_dot(value, one_hot):
    out = jnp.dot(split3(value), one_hot, preferred_element_type=F32)
    return out[0:8] + out[8:16] + out[16:24]


def group_matrices(channels):
    width = channels // GROUPS
    chan = lax.broadcasted_iota(jnp.int32, (channels, LANES), 0)
    grp = lax.broadcasted_iota(jnp.int32, (channels, LANES), 1) * width
    gather = jnp.where((chan >= grp) & (chan < grp + width), 1.0, 0.0).astype(BF16)
    chan_t = lax.broadcasted_iota(jnp.int32, (LANES, channels), 1)
    grp_t = lax.broadcasted_iota(jnp.int32, (LANES, channels), 0) * width
    spread = jnp.where((chan_t >= grp_t) & (chan_t < grp_t + width), 1.0, 0.0).astype(BF16)
    return gather, spread


def spread_groups(group_sums, spread, count):
    mean = group_sums[0:1] / count
    inv_std = lax.rsqrt(group_sums[1:2] / count - mean * mean + NORM_EPS)
    stacked = jnp.concatenate([mean, inv_std, jnp.zeros((6, LANES), F32)], axis=0)
    per_channel = exact_dot(stacked, spread)
    return per_channel[0:1], per_channel[1:2]


def norm_params(sums, count):
    gather, spread = group_matrices(sums.shape[1])
    return spread_groups(exact_dot(sums, gather)[0:2], spread, count)


def fold_rows(value):
    rows, channels = value.shape
    return jnp.sum(value.reshape(rows // 8, 8, channels), axis=0)


def add_moments(acc_ref, value):
    acc_ref[0] += fold_rows(value)
    acc_ref[1] += fold_rows(value * value)


def moment_rows(acc_ref):
    total = jnp.sum(acc_ref[0], axis=0, keepdims=True)
    square = jnp.sum(acc_ref[1], axis=0, keepdims=True)
    return jnp.concatenate([total, square, jnp.zeros((6, total.shape[1]), F32)], axis=0)


def exchange(slot, send_ref, recv_ref, send_sem, recv_sem):
    copy = pltpu.make_async_remote_copy(
        src_ref=send_ref.at[slot],
        dst_ref=recv_ref.at[slot],
        send_sem=send_sem.at[slot],
        recv_sem=recv_sem.at[slot],
        device_id=partner_id(),
        device_id_type=MESH,
    )
    copy.start()
    copy.wait()
    return send_ref[slot] + recv_ref[slot]


def silu(value):
    half = 0.5 * value
    return half + half * jnp.tanh(half)


def fill_chunk(u_ref, src_ref, chunk, params, top_edge, bottom_edge):
    mean, gain, shift = params
    _, cols, channels = src_ref.shape
    place = lax.broadcasted_iota(jnp.int32, (cols, channels), 0)
    last = CHUNK_ROWS + 1
    for j in range(CHUNK_ROWS + 2):
        value = silu((src_ref[chunk * CHUNK_ROWS + j].astype(F32) - mean) * gain + shift)
        if j == 0:
            value = jnp.where(top_edge & (chunk == 0), 0.0, value)
        if j == last:
            value = jnp.where(bottom_edge & (chunk == CHUNKS - 1), 0.0, value)
        before = jnp.where(place == 0, 0.0, pltpu.roll(value, 1, 0))
        after = jnp.where(place == cols - 1, 0.0, pltpu.roll(value, cols - 1, 0))
        u_ref[j, :, 0:channels] = before.astype(BF16)
        u_ref[j, :, channels:2 * channels] = value.astype(BF16)
        u_ref[j, :, 2 * channels:3 * channels] = after.astype(BF16)


def conv_chunk(u_ref, w):
    _, cols, depth = u_ref.shape
    rows, split = CHUNK_ROWS * cols, w.shape[1] - LANES
    taps = [u_ref[dy:dy + CHUNK_ROWS].reshape(rows, depth) for dy in range(3)]
    main = jnp.dot(jnp.concatenate(taps, axis=1), w[:, 0:split], preferred_element_type=F32)
    both = jnp.concatenate([w[0:depth, split:], w[depth:2 * depth, split:]], axis=1)
    pair = jnp.dot(u_ref[0:CHUNK_ROWS + 1].reshape(rows + cols, depth), both, preferred_element_type=F32)
    third = jnp.dot(taps[2], w[2 * depth:, split:], preferred_element_type=F32)
    rest = pair[0:rows, 0:LANES] + pair[cols:, LANES:] + third
    return jnp.concatenate([main, rest], axis=1)


def conv_loop(order, ready, fill, finish, u_even, u_odd, w, arriving=False):
    def step(i, half, parity, u_now, u_next):
        after = jnp.minimum(i + 1, CHUNKS - 1)
        if arriving:
            finish(order(i), conv_chunk(u_now, w))
            ready(half, parity)
            fill(u_next, order(after))
        else:
            ready(half, parity)
            fill(u_next, order(after))
            finish(order(i), conv_chunk(u_now, w))

    def pair(half, carry):
        step(2 * half, half, 0, u_even, u_odd)
        step(2 * half + 1, half, 1, u_odd, u_even)
        return carry

    fill(u_even, order(jnp.int32(0)))
    lax.fori_loop(0, CHUNKS // 2, pair, 0)


def in_order(i):
    return i


def from_ends(i):
    return lax.rem(i + 1, 2) * lax.div(i, 2) + lax.rem(i, 2) * (CHUNKS - 1 - lax.div(i, 2))


def rows_of(ref, chunk, first=0):
    value = ref[pl.ds(chunk * CHUNK_ROWS + first, CHUNK_ROWS)]
    return value.reshape(value.shape[0] * value.shape[1], value.shape[2])


def send_edge_row(ref, send_sem, recv_sem, src_ref=None, src_row=None):
    rows = ref.shape[0] - 2
    core = position()[1]
    src = ref.at[rows - (rows - 1) * core] if src_ref is None else src_ref.at[src_row]
    return pltpu.make_async_remote_copy(
        src_ref=src, dst_ref=ref.at[(rows + 1) * core],
        send_sem=send_sem, recv_sem=recv_sem, device_id=partner_id(), device_id_type=MESH)


def first_kernel(count, x_ref, emb_ref, scale_ref, shift_ref, w_ref, tw_ref, out_ref, stat_ref, time_ref,
                 x_vmem, a_ref, h_ref, u_even, u_odd, w_vmem, tw_vmem, acc_ref, time_all, grp_recv, grp_total, st_send, st_recv,
                 load_sem, grp_ssem, grp_rsem, st_ssem, st_rsem, edge_ssem, edge_rsem, piece_ssem, piece_rsem, halo_ssem, halo_rsem):
    images, tile_rows, tile_cols, channels = x_ref.shape
    rows = 2 * tile_rows
    chip_x, core, chip_y = position()
    sp = lax.axis_index("sp")
    me = 2 * sp + chip_y
    image = 2 * chip_x + chip_y

    signal_all()
    x_load = pltpu.make_async_copy(x_ref, x_vmem, load_sem.at[0])
    x_load.start()
    weights = [pltpu.make_async_copy(w_ref.at[k], w_vmem.at[k], load_sem.at[1 + k]) for k in range(2)]
    tw_load = pltpu.make_async_copy(tw_ref, tw_vmem, load_sem.at[3])
    tw_load.start()

    def piece(part, source_core):
        low, high = PIECES[part]
        start = (1 - source_core) * low + source_core * (tile_rows - low - high)
        return pl.ds(start, high), pl.ds(1 + source_core * tile_rows + start, high)

    def piece_copies(k, part):
        to_x, to_y = lax.rem(chip_x + k // 2, 2), lax.rem(chip_y + k % 2, 2)
        src_rows, dst_rows = piece(part, core)
        src = x_ref.at[2 * to_x + to_y, src_rows]
        dst = a_ref.at[dst_rows, pl.ds(chip_y * tile_cols, tile_cols)]
        landed = piece_rsem.at[part, 2 * chip_y + core]
        remote = pltpu.make_async_remote_copy(
            src_ref=src, dst_ref=dst, send_sem=piece_ssem.at[k, part], recv_sem=landed,
            device_id={"sp": 2 * to_x + chip_x, "sp2": to_y}, device_id_type=MESH)
        return remote, pltpu.make_async_copy(src, dst, landed)

    def halo_copies(k):
        to_x, to_y = lax.rem(chip_x + k // 2, 2), lax.rem(chip_y + k % 2, 2)
        src = x_ref.at[2 * to_x + to_y, (tile_rows - 1) * core]
        dst = a_ref.at[(rows + 1) * chip_x, pl.ds(chip_y * tile_cols, tile_cols)]
        remote = pltpu.make_async_remote_copy(
            src_ref=src, dst_ref=dst, send_sem=halo_ssem.at[k], recv_sem=halo_rsem.at[chip_y],
            device_id={"sp": 2 * to_x + 1 - chip_x, "sp2": to_y}, device_id_type=MESH)
        return remote, pltpu.make_async_copy(src, dst, halo_rsem.at[chip_y])

    at_home = core == chip_x
    far_first = (3, 2, 1, 0)

    def send_piece(part):
        for k in far_first:
            remote, local = piece_copies(k, part)
            if k:
                remote.start()
            else:
                pl.when(at_home)(local.start)
                pl.when(jnp.logical_not(at_home))(remote.start)

    wait_all()

    @pl.when(jnp.logical_not(at_home))
    def _():
        for k in far_first:
            halo_copies(k)[0 if k else 1].start()

    send_piece(0)
    for copy in weights:
        copy.start()

    gather, spread = group_matrices(channels)
    x_load.wait()
    moments = []
    for i in range(images):
        acc_ref[...] = jnp.zeros_like(acc_ref)

        def add_row(row, carry):
            add_moments(acc_ref, x_vmem[i, row].astype(F32))
            return carry

        lax.fori_loop(0, tile_rows, add_row, 0)
        moments += [jnp.sum(acc_ref[0], axis=0, keepdims=True), jnp.sum(acc_ref[1], axis=0, keepdims=True)]
    grp_recv[me] = exact_dot(jnp.concatenate(moments, axis=0), gather)
    group_copies = []
    for k, (to_sp, to_y) in enumerate(others()):
        copy = pltpu.make_async_remote_copy(
            src_ref=grp_recv.at[me], dst_ref=grp_recv.at[me], send_sem=grp_ssem.at[k], recv_sem=grp_rsem.at[me],
            device_id={"sp": to_sp, "sp2": to_y}, device_id_type=MESH)
        copy.start()
        group_copies.append((copy, 2 * to_sp + to_y))

    for part in range(1, len(PIECES)):
        send_piece(part)

    tw_load.wait()
    emb = silu(emb_ref[...].astype(F32)).astype(BF16)
    for k in range(2):
        time_all[k, 0:images] = jnp.dot(emb, tw_vmem[k], preferred_element_type=F32)
    time_ref[...] = jnp.broadcast_to(time_all[1, pl.ds(image, 1)], time_ref.shape)
    time_vec = time_all[0, pl.ds(image, 1)]

    total = jnp.zeros((8, LANES), F32)
    for copy, _ in group_copies:
        copy.wait_send()
    for copy, sender in group_copies:
        pltpu.make_async_copy(grp_recv.at[sender], grp_recv.at[sender], grp_rsem.at[sender]).wait()
    for slot in range(8):
        total = total + grp_recv[slot]
    grp_total[...] = total
    mean, inv_std = spread_groups(grp_total[pl.ds(2 * image, 2)], spread, count)

    def wait_piece(part, source_core):
        for col in range(2):
            landed = a_ref.at[piece(part, source_core)[1], pl.ds(col * tile_cols, tile_cols)]
            pltpu.make_async_copy(landed, landed, piece_rsem.at[part, 2 * col + source_core]).wait()

    def ready(half, parity):
        if parity == 0:
            for part in range(3):
                pl.when(half == part)(functools.partial(wait_piece, part, 1))
        else:
            for part in range(1, 4):
                pl.when(half + 1 == part)(functools.partial(wait_piece, part, 0))
            pl.when(half + 1 == 3)(functools.partial(wait_piece, 3, 1))

    top_edge, bottom_edge = core == 0, core == 1

    def norm(k, mean, inv_std):
        return mean, inv_std * scale_ref[k:k + 1].astype(F32), shift_ref[k:k + 1].astype(F32)

    params = norm(0, mean, inv_std)
    for col in range(2):
        landed = a_ref.at[(rows + 1) * (1 - core), pl.ds(col * tile_cols, tile_cols)]
        pltpu.make_async_copy(landed, landed, halo_rsem.at[col]).wait()
    wait_piece(0, 0)
    acc_ref[...] = jnp.zeros_like(acc_ref)
    weights[0].wait()

    def finish_first(chunk, total):
        hidden = (total + time_vec).astype(BF16)
        h_ref[pl.ds(chunk * CHUNK_ROWS + 1, CHUNK_ROWS)] = hidden.reshape(CHUNK_ROWS, 2 * tile_cols, channels)
        add_moments(acc_ref, hidden.astype(F32))

    conv_loop(from_ends, ready, lambda u_ref, chunk: fill_chunk(u_ref, a_ref, chunk, params, top_edge, bottom_edge),
              finish_first, u_even, u_odd, w_vmem.at[0], arriving=True)

    edge = send_edge_row(h_ref, edge_ssem, edge_rsem)
    edge.start()
    st_send[0] = moment_rows(acc_ref)
    acc_ref[...] = jnp.zeros_like(acc_ref)
    weights[1].wait()
    second = norm(1, *norm_params(exchange(0, st_send, st_recv, st_ssem, st_rsem), count))
    edge.wait()

    def finish_second(chunk, total):
        new = (rows_of(a_ref, chunk, 1).astype(F32) + total).astype(BF16)
        out_ref[pl.ds(chunk * CHUNK_ROWS, CHUNK_ROWS)] = new.reshape(CHUNK_ROWS, 2 * tile_cols, channels)
        add_moments(acc_ref, new.astype(F32))

    conv_loop(in_order, lambda half, parity: None,
              lambda u_ref, chunk: fill_chunk(u_ref, h_ref, chunk, second, top_edge, bottom_edge),
              finish_second, u_even, u_odd, w_vmem.at[1])
    stat_ref[...] = moment_rows(acc_ref)

    @pl.when(jnp.logical_not(at_home))
    def _():
        for k in (1, 2, 3):
            halo_copies(k)[0].wait_send()

    for part in range(len(PIECES)):
        for k in range(4):
            remote, _ = piece_copies(k, part)
            if k:
                remote.wait_send()
            else:
                pl.when(jnp.logical_not(at_home))(remote.wait_send)


def second_kernel(count, a_hbm, stat_in, time_ref, scale_ref, shift_ref, w_ref, out_ref,
                  a_ref, h_ref, u_even, u_odd, w_vmem, acc_ref, res_ref, st_send, st_recv,
                  load_sem, st_ssem, st_rsem, edge_ssem, edge_rsem, tile_ssem, tile_rsem):
    rows, cols, channels = res_ref.shape
    tile_rows, tile_cols = rows // 2, cols // 2
    chip_x, core, chip_y = position()
    sp = lax.axis_index("sp")
    image = 2 * chip_x + chip_y

    signal_all()
    a_load = pltpu.make_async_copy(a_hbm, a_ref.at[pl.ds(1, rows)], load_sem.at[0])
    a_load.start()
    weights = [pltpu.make_async_copy(w_ref.at[2 + k], w_vmem.at[k], load_sem.at[1 + k]) for k in range(2)]
    for copy in weights:
        copy.start()
    st_send[0] = stat_in[...]
    acc_ref[...] = jnp.zeros_like(acc_ref)
    wait_all()
    edge = send_edge_row(a_ref, edge_ssem.at[0], edge_rsem.at[0], a_hbm, (rows - 1) * (1 - core))
    edge.start()
    top_edge, bottom_edge = core == 0, core == 1

    def norm(k, sums):
        mean, inv_std = norm_params(sums, count)
        return mean, inv_std * scale_ref[3 + k:4 + k].astype(F32), shift_ref[3 + k:4 + k].astype(F32)

    params = norm(0, exchange(0, st_send, st_recv, st_ssem, st_rsem))
    a_load.wait()
    edge.wait()
    weights[0].wait()
    time_vec = time_ref[0:1]

    def finish_first(chunk, total):
        hidden = (total + time_vec).astype(BF16)
        h_ref[pl.ds(chunk * CHUNK_ROWS + 1, CHUNK_ROWS)] = hidden.reshape(CHUNK_ROWS, cols, channels)
        add_moments(acc_ref, hidden.astype(F32))

    conv_loop(in_order, lambda half, parity: None,
              lambda u_ref, chunk: fill_chunk(u_ref, a_ref, chunk, params, top_edge, bottom_edge),
              finish_first, u_even, u_odd, w_vmem.at[0])

    edge = send_edge_row(h_ref, edge_ssem.at[1], edge_rsem.at[1])
    edge.start()
    st_send[1] = moment_rows(acc_ref)
    weights[1].wait()
    second = norm(1, exchange(1, st_send, st_recv, st_ssem, st_rsem))
    edge.wait()

    per_tile = CHUNKS // 2

    def home_copies(chunk, col):
        to_sp = 2 * core + lax.div(chunk, per_tile)
        slot = lax.rem(chunk, per_tile)
        here = (to_sp == sp) & (chip_y == col)
        src = res_ref.at[pl.ds(chunk * CHUNK_ROWS, CHUNK_ROWS), pl.ds(col * tile_cols, tile_cols)]
        dst = out_ref.at[image, pl.ds(slot * CHUNK_ROWS, CHUNK_ROWS)]
        landed = tile_rsem.at[image, slot]
        remote = pltpu.make_async_remote_copy(
            src_ref=src, dst_ref=dst, send_sem=tile_ssem.at[chunk, col], recv_sem=landed,
            device_id={"sp": to_sp, "sp2": col}, device_id_type=MESH)
        return here, remote, pltpu.make_async_copy(src, dst, landed)

    def send_home(chunk):
        for col in range(2):
            here, remote, local = home_copies(chunk, col)
            pl.when(here)(local.start)
            pl.when(jnp.logical_not(here))(remote.start)

    def ready(half, parity):
        if parity:
            send_home(2 * half)
        else:
            pl.when(half > 0)(lambda: send_home(2 * half - 1))

    def finish_second(chunk, total):
        new = (rows_of(a_ref, chunk, 1).astype(F32) + total).astype(BF16)
        res_ref[pl.ds(chunk * CHUNK_ROWS, CHUNK_ROWS)] = new.reshape(CHUNK_ROWS, cols, channels)

    conv_loop(in_order, ready, lambda u_ref, chunk: fill_chunk(u_ref, h_ref, chunk, second, top_edge, bottom_edge),
              finish_second, u_even, u_odd, w_vmem.at[1])
    send_home(jnp.int32(CHUNKS - 1))
    for chunk in range(CHUNKS):
        for col in range(2):
            here, remote, _ = home_copies(jnp.int32(chunk), col)
            pl.when(jnp.logical_not(here))(remote.wait_send)
    for slot in range(4):
        for part in range(per_tile):
            landed = out_ref.at[slot, pl.ds(part * CHUNK_ROWS, CHUNK_ROWS)]
            pltpu.make_async_copy(landed, landed, tile_rsem.at[slot, part]).wait()


def attention_kernel(norm_idx, count, logit_scale, a_hbm, stat_in, scale_ref, shift_ref, w_hbm, wo_hbm,
                     out_ref, stat_ref, a_ref, n_ref, q_ref, k_ref, v_ref, s_even, s_odd, peak_ref, total_ref, part_ref, o_ref,
                     wq_ref, wk_ref, wv_ref, wo_ref, acc_ref,
                     st_send, st_recv, load_sem, head_sem, st_ssem, st_rsem, kv_ssem, kv_rsem):
    tokens, channels = a_ref.shape
    heads, head_dim, _ = v_ref.shape
    loads = [pltpu.make_async_copy(src, dst, load_sem.at[i])
             for i, (src, dst) in enumerate(((a_hbm, a_ref), (w_hbm.at[2], wv_ref), (w_hbm.at[0], wq_ref), (wo_hbm, wo_ref)))]
    head_loads = [pltpu.make_async_copy(w_hbm.at[1, pl.ds(head * head_dim, head_dim)],
                                        wk_ref.at[pl.ds(head * LANES, head_dim)], head_sem.at[head])
                  for head in range(heads)]
    for load in loads[:2] + head_loads + loads[2:]:
        load.start()
    for head in range(heads):
        wk_ref[head * LANES + head_dim:(head + 1) * LANES] = jnp.zeros((LANES - head_dim, channels), BF16)
        q_ref[head, head_dim:] = jnp.zeros((LANES - head_dim, tokens), BF16)
    st_send[0] = stat_in[...]
    barrier_pair()
    sums = exchange(0, st_send, st_recv, st_ssem, st_rsem)
    mean, inv_std = norm_params(sums, count)
    gain = inv_std * scale_ref[norm_idx:norm_idx + 1].astype(F32)
    shift = shift_ref[norm_idx:norm_idx + 1].astype(F32)
    loads[0].wait()
    loads[1].wait()
    for load in head_loads:
        load.wait()

    step = TOKEN_BLOCK
    chunks = tokens // step
    transposed = (((1,), (1,)), ((), ()))

    def head_copy(which, head, chunk=None):
        first, size = (0, tokens) if chunk is None else (pl.multiple_of(chunk * step, step), step)
        src, dst = pl.ds(first, size), pl.ds(tokens + first, size)
        if which:
            src_ref, dst_ref = v_ref.at[head, :, src], v_ref.at[head, :, dst]
        else:
            src_ref, dst_ref = k_ref.at[head, src], k_ref.at[head, dst]
        slot = head if chunk is None else heads + chunk
        return pltpu.make_async_remote_copy(
            src_ref=src_ref, dst_ref=dst_ref, send_sem=kv_ssem.at[which, slot], recv_sem=kv_rsem.at[which, slot],
            device_id=partner_id(), device_id_type=MESH)

    def both(act, head, chunk=None):
        for which in range(2):
            getattr(head_copy(which, head, chunk), act)()

    def key_values(i, carry):
        here = pl.ds(pl.multiple_of(i * step, step), step)
        normed = ((a_ref[here].astype(F32) - mean) * gain + shift).astype(BF16)
        n_ref[here] = normed
        part = lax.dot_general(normed, wk_ref[...], transposed, preferred_element_type=F32).astype(BF16)
        for head in range(heads):
            k_ref[head, here] = part[:, head * LANES:(head + 1) * LANES]
        part = lax.dot_general(wv_ref[...], normed, transposed, preferred_element_type=F32).astype(BF16)
        for head in range(heads):
            v_ref[head, :, here] = part[head * head_dim:(head + 1) * head_dim]

        @pl.when(i > 0)
        def _():
            both("start", 0, i - 1)
        return carry

    lax.fori_loop(0, chunks, key_values, 0)
    loads[2].wait()

    def query_chunk(i):
        here = pl.ds(pl.multiple_of(i * step, step), step)
        part = lax.dot_general(wq_ref[...], n_ref[here], transposed, preferred_element_type=F32).astype(BF16)
        for head in range(heads):
            q_ref[head, 0:head_dim, here] = part[head * head_dim:(head + 1) * head_dim]

    def queries(i, carry):
        query_chunk(2 * i)
        query_chunk(2 * i + 1)

        @pl.when(i == 0)
        def _():
            both("start", 0, chunks - 1)
            for head in range(1, heads):
                both("start", head)
        return carry

    lax.fori_loop(0, chunks // 2, queries, 0)

    for i in range(chunks):
        both("wait_recv", 0, i)

    blocks = tokens // QUERY_BLOCK
    key_blocks = 2 * tokens // KEY_BLOCK

    def fold(value, combine):
        return combine(value.reshape(KEY_BLOCK // 8, 8, QUERY_BLOCK), axis=0)

    def place_of(block):
        first = pl.multiple_of(lax.rem(block, blocks) * QUERY_BLOCK, QUERY_BLOCK)
        return lax.div(block, blocks), pl.ds(first, QUERY_BLOCK)

    def keys_of(j):
        return slice(j * KEY_BLOCK, (j + 1) * KEY_BLOCK)

    def score(j, head, query, s_ref, peak):
        scores = jnp.dot(k_ref[head, keys_of(j)], query, preferred_element_type=F32)
        s_ref[keys_of(j)] = scores
        piece = fold(scores, jnp.max)
        return piece if peak is None else jnp.maximum(peak, piece)

    def absorb(j, head, peak, s_ref, state):
        weights = jnp.exp2((s_ref[keys_of(j)] - peak) * logit_scale)
        total = fold(weights, jnp.sum)
        attended = jnp.dot(v_ref[head, :, keys_of(j)], weights.astype(BF16), preferred_element_type=F32)
        return (total, attended) if state is None else (state[0] + total, state[1] + attended)

    def finish_block(block, peak, s_ref, state):
        head, here = place_of(block)
        total, attended = absorb(key_blocks - 1, head, peak, s_ref, state)
        total = jnp.sum(total, axis=0, keepdims=True)
        o_ref[pl.ds(pl.multiple_of(head * head_dim, 16), head_dim), here] = (attended / total).astype(BF16)

    def peak_of(slot):
        return jnp.max(peak_ref[slot], axis=0, keepdims=True)

    def advance(i, s_ref, s_next, slot, state):
        head, _ = place_of(i)
        next_head, next_here = place_of(jnp.minimum(i + 1, heads * blocks - 1))
        query = q_ref[next_head, :, next_here]
        peak, next_peak, new_state = peak_of(slot), None, None
        for j in range(key_blocks):
            next_peak = score(j, next_head, query, s_next, next_peak)
            if j == 1:
                finish_block(jnp.maximum(i - 1, 0), peak_of(1 - slot), s_next, state)
            if j:
                new_state = absorb(j - 1, head, peak, s_ref, new_state)
        peak_ref[1 - slot] = next_peak
        return new_state

    s_odd[keys_of(key_blocks - 1)] = jnp.zeros((KEY_BLOCK, QUERY_BLOCK), F32)
    peak_ref[1] = jnp.zeros((8, QUERY_BLOCK), F32)
    total_ref[...] = jnp.zeros_like(total_ref)
    part_ref[...] = jnp.zeros_like(part_ref)
    query = q_ref[0, :, 0:QUERY_BLOCK]
    first_peak = None
    for j in range(key_blocks):
        first_peak = score(j, 0, query, s_even, first_peak)
    peak_ref[0] = first_peak

    def attend(i, carry):
        head = lax.div(2 * i + 2, blocks)
        pl.when((lax.rem(2 * i + 2, blocks) == 0) & (head < heads))(lambda: both("wait_recv", head))
        state = advance(2 * i, s_even, s_odd, 0, (total_ref[...], part_ref[...]))
        state = advance(2 * i + 1, s_odd, s_even, 1, state)
        total_ref[...], part_ref[...] = state
        return carry

    lax.fori_loop(0, heads * blocks // 2, attend, 0)
    finish_block(jnp.int32(heads * blocks - 1), peak_of(1), s_odd, (total_ref[...], part_ref[...]))
    for i in range(chunks):
        both("wait_send", 0, i)
    for head in range(1, heads):
        both("wait_send", head)
    loads[3].wait()
    acc_ref[...] = jnp.zeros_like(acc_ref)

    def project_chunk(i):
        here = pl.ds(pl.multiple_of(i * step, step), step)
        added = lax.dot_general(o_ref[:, here], wo_ref[...], (((0,), (0,)), ((), ())), preferred_element_type=F32)
        new = (a_ref[here].astype(F32) + added).astype(BF16)
        a_ref[here] = new
        add_moments(acc_ref, new.astype(F32))

    def leave(i):
        here = pl.ds(pl.multiple_of(i * 2 * step, 2 * step), 2 * step)
        return pltpu.make_async_copy(a_ref.at[here], out_ref.at[here], load_sem.at[i])

    def project(i, carry):
        pl.when(i > 0)(lambda: leave(i - 1).start())
        project_chunk(2 * i)
        project_chunk(2 * i + 1)
        return carry

    lax.fori_loop(0, chunks // 2, project, 0)
    stat_ref[...] = moment_rows(acc_ref)
    leave(chunks // 2 - 1).start()
    for i in range(chunks // 2):
        leave(i).wait()


VMEM_SPEC = pl.BlockSpec(memory_space=pltpu.VMEM)
ANY_SPEC = pl.BlockSpec(memory_space=pl.ANY)


def params(collective_id):
    return pltpu.CompilerParams(collective_id=collective_id, has_side_effects=True, vmem_limit_bytes=60 * 2**20)


def conv_scratch(rows, cols, channels):
    return [
        pltpu.VMEM((rows + 2, cols, channels), BF16),
        pltpu.VMEM((rows + 2, cols, channels), BF16),
        pltpu.VMEM((CHUNK_ROWS + 2, cols, 3 * channels), BF16),
        pltpu.VMEM((CHUNK_ROWS + 2, cols, 3 * channels), BF16),
        pltpu.VMEM((2, 9 * channels, channels), BF16),
    ]


def first_call(count, rows, cols, x, time_emb, scale, shift, w, time_w):
    channels = x.shape[3]
    dma = pltpu.SemaphoreType.DMA
    return pl.pallas_call(
        functools.partial(first_kernel, count),
        out_shape=[
            jax.ShapeDtypeStruct((rows, cols, channels), BF16),
            jax.ShapeDtypeStruct((8, channels), F32),
            jax.ShapeDtypeStruct((8, channels), F32),
        ],
        in_specs=[ANY_SPEC, VMEM_SPEC, VMEM_SPEC, VMEM_SPEC, ANY_SPEC, ANY_SPEC],
        out_specs=[VMEM_SPEC, VMEM_SPEC, VMEM_SPEC],
        scratch_shapes=[pltpu.VMEM(x.shape, BF16)] + conv_scratch(rows, cols, channels) + [
            pltpu.VMEM(time_w.shape, BF16),
            pltpu.VMEM((2, 8, channels), F32),
            pltpu.VMEM((2, 8, channels), F32),
            pltpu.VMEM((8, 8, LANES), F32),
            pltpu.VMEM((8, LANES), F32),
            pltpu.VMEM((1, 8, channels), F32),
            pltpu.VMEM((1, 8, channels), F32),
            dma((4,)), dma((7,)), dma((8,)), dma((1,)), dma((1,)), dma, dma,
            dma((4, len(PIECES))), dma((len(PIECES), 4)), dma((4,)), dma((2,)),
        ],
        compiler_params=params(0),
        name="res_first",
    )(x, time_emb, scale, shift, w, time_w)


def second_call(count, tile_shape, a, stats, time_vec, scale, shift, w):
    rows, cols, channels = a.shape
    dma = pltpu.SemaphoreType.DMA
    return pl.pallas_call(
        functools.partial(second_kernel, count),
        out_shape=jax.ShapeDtypeStruct(tile_shape, BF16),
        in_specs=[ANY_SPEC, VMEM_SPEC, VMEM_SPEC, VMEM_SPEC, VMEM_SPEC, ANY_SPEC],
        out_specs=ANY_SPEC,
        scratch_shapes=conv_scratch(rows, cols, channels) + [
            pltpu.VMEM((2, 8, channels), F32),
            pltpu.VMEM((rows, cols, channels), BF16),
            pltpu.VMEM((2, 8, channels), F32),
            pltpu.VMEM((2, 8, channels), F32),
            dma((3,)), dma((2,)), dma((2,)), dma((2,)), dma((2,)), dma((CHUNKS, 2)), dma((4, CHUNKS // 2)),
        ],
        compiler_params=params(2),
        name="res_second",
    )(a, stats, time_vec, scale, shift, w)


def attention_call(norm_idx, count, heads, a, stats, scale, shift, w, wo):
    tokens, channels = a.shape
    head_dim = channels // heads
    logit_scale = head_dim ** -0.5 * 1.4426950408889634
    return pl.pallas_call(
        functools.partial(attention_kernel, norm_idx, count, logit_scale),
        out_shape=[jax.ShapeDtypeStruct((tokens, channels), BF16), jax.ShapeDtypeStruct((8, channels), F32)],
        in_specs=[ANY_SPEC, VMEM_SPEC, VMEM_SPEC, VMEM_SPEC, ANY_SPEC, ANY_SPEC],
        out_specs=[ANY_SPEC, VMEM_SPEC],
        scratch_shapes=[
            pltpu.VMEM((tokens, channels), BF16),
            pltpu.VMEM((tokens, channels), BF16),
            pltpu.VMEM((heads, LANES, tokens), BF16),
            pltpu.VMEM((heads, 2 * tokens, LANES), BF16),
            pltpu.VMEM((heads, head_dim, 2 * tokens), BF16),
            pltpu.VMEM((2 * tokens, QUERY_BLOCK), F32),
            pltpu.VMEM((2 * tokens, QUERY_BLOCK), F32),
            pltpu.VMEM((2, 8, QUERY_BLOCK), F32),
            pltpu.VMEM((8, QUERY_BLOCK), F32),
            pltpu.VMEM((head_dim, QUERY_BLOCK), F32),
            pltpu.VMEM((channels, tokens), BF16),
            pltpu.VMEM((channels, channels), BF16),
            pltpu.VMEM((heads * LANES, channels), BF16),
            pltpu.VMEM((channels, channels), BF16),
            pltpu.VMEM((channels, channels), BF16),
            pltpu.VMEM((2, 8, channels), F32),
            pltpu.VMEM((1, 8, channels), F32),
            pltpu.VMEM((1, 8, channels), F32),
            pltpu.SemaphoreType.DMA((4,)),
            pltpu.SemaphoreType.DMA((heads,)),
            pltpu.SemaphoreType.DMA((1,)),
            pltpu.SemaphoreType.DMA((1,)),
            pltpu.SemaphoreType.DMA((2, heads + tokens // TOKEN_BLOCK)),
            pltpu.SemaphoreType.DMA((2, heads + tokens // TOKEN_BLOCK)),
        ],
        compiler_params=params(1),
        name="attention",
    )(a, stats, scale, shift, w, wo)


def solution(mesh):
    lat_spec = P("dp", "sp", "sp2", None)

    def local(x, time_emb, gn_scale, gn_shift, conv_w, time_w, w_qkv, w_out):
        images, tile_rows, tile_cols, channels = x.shape
        rows, cols = 2 * tile_rows, 2 * tile_cols
        count = 2 * rows * cols * (channels // GROUPS)
        heads = w_out.shape[0]
        w = conv_w.reshape(4, 9 * channels, channels)
        qkv = jnp.transpose(w_qkv, (0, 2, 3, 1)).reshape(3, channels, channels)
        wo = w_out.reshape(channels, channels)
        first, stats, time_vec = first_call(count, rows, cols, x, time_emb, gn_scale, gn_shift, w, time_w)
        middle, stats = attention_call(2, count, heads, first.reshape(rows * cols, channels), stats, gn_scale, gn_shift, qkv, wo)
        return second_call(count, x.shape, middle.reshape(rows, cols, channels), stats, time_vec, gn_scale, gn_shift, w)

    return jax.shard_map(local, mesh=mesh, in_specs=(lat_spec, P("dp", None), P(), P(), P(), P(), P(), P()), out_specs=lat_spec, check_vma=False)
```

```python
import functools

import jax
import jax.numpy as jnp
from jax import lax
from jax.experimental import pallas as pl
from jax.experimental.pallas import tpu as pltpu
from jax.sharding import PartitionSpec as P

GROUPS = 32
NORM_EPS = 1e-5
LANES = 128
CHUNK_ROWS = 4
CHUNKS = 8
PIECES = ((0, 5), (5, 4), (9, 4), (13, 3))
QUERY_BLOCK = 512
KEY_BLOCK = 512
TOKEN_BLOCK = 512
MESH = pl.DeviceIdType.MESH
F32 = jnp.float32
BF16 = jnp.bfloat16


def position():
    sp = lax.axis_index("sp")
    return lax.div(sp, 2), lax.rem(sp, 2), lax.axis_index("sp2")


def partner_id():
    chip_x, core, _ = position()
    return {"sp": 2 * chip_x + 1 - core}


def barrier_pair():
    sem = pltpu.get_barrier_semaphore()
    pl.semaphore_signal(sem, inc=1, device_id=partner_id(), device_id_type=MESH)
    pl.semaphore_wait(sem, 1)


def others():
    sp, col = lax.axis_index("sp"), lax.axis_index("sp2")
    return [(lax.rem(sp + i, 4), lax.rem(col + j, 2)) for i in range(4) for j in range(2) if i or j]


def signal_all():
    for sp, col in others():
        pl.semaphore_signal(pltpu.get_barrier_semaphore(), inc=1, device_id={"sp": sp, "sp2": col}, device_id_type=MESH)


def wait_all():
    pl.semaphore_wait(pltpu.get_barrier_semaphore(), 7)


def split3(value):
    high = value.astype(BF16).astype(F32)
    rest = value - high
    mid = rest.astype(BF16).astype(F32)
    low = rest - mid
    return jnp.concatenate([high, mid, low, jnp.zeros_like(value)], axis=0).astype(BF16)


def exact_dot(value, one_hot):
    out = jnp.dot(split3(value), one_hot, preferred_element_type=F32)
    return out[0:8] + out[8:16] + out[16:24]


def group_matrices(channels):
    width = channels // GROUPS
    chan = lax.broadcasted_iota(jnp.int32, (channels, LANES), 0)
    grp = lax.broadcasted_iota(jnp.int32, (channels, LANES), 1) * width
    gather = jnp.where((chan >= grp) & (chan < grp + width), 1.0, 0.0).astype(BF16)
    chan_t = lax.broadcasted_iota(jnp.int32, (LANES, channels), 1)
    grp_t = lax.broadcasted_iota(jnp.int32, (LANES, channels), 0) * width
    spread = jnp.where((chan_t >= grp_t) & (chan_t < grp_t + width), 1.0, 0.0).astype(BF16)
    return gather, spread


def spread_groups(group_sums, spread, count):
    mean = group_sums[0:1] / count
    inv_std = lax.rsqrt(group_sums[1:2] / count - mean * mean + NORM_EPS)
    stacked = jnp.concatenate([mean, inv_std, jnp.zeros((6, LANES), F32)], axis=0)
    per_channel = exact_dot(stacked, spread)
    return per_channel[0:1], per_channel[1:2]


def norm_params(sums, count):
    gather, spread = group_matrices(sums.shape[1])
    return spread_groups(exact_dot(sums, gather)[0:2], spread, count)


def fold_rows(value):
    rows, channels = value.shape
    return jnp.sum(value.reshape(rows // 8, 8, channels), axis=0)


def add_moments(acc_ref, value):
    acc_ref[0] += fold_rows(value)
    acc_ref[1] += fold_rows(value * value)


def moment_rows(acc_ref):
    total = jnp.sum(acc_ref[0], axis=0, keepdims=True)
    square = jnp.sum(acc_ref[1], axis=0, keepdims=True)
    return jnp.concatenate([total, square, jnp.zeros((6, total.shape[1]), F32)], axis=0)


def exchange(slot, send_ref, recv_ref, send_sem, recv_sem):
    copy = pltpu.make_async_remote_copy(
        src_ref=send_ref.at[slot],
        dst_ref=recv_ref.at[slot],
        send_sem=send_sem.at[slot],
        recv_sem=recv_sem.at[slot],
        device_id=partner_id(),
        device_id_type=MESH,
    )
    copy.start()
    copy.wait()
    return send_ref[slot] + recv_ref[slot]


def silu(value):
    half = 0.5 * value
    return half + half * jnp.tanh(half)


def fill_chunk(u_ref, src_ref, chunk, params, top_edge, bottom_edge):
    mean, gain, shift = params
    _, cols, channels = src_ref.shape
    place = lax.broadcasted_iota(jnp.int32, (cols, channels), 0)
    last = CHUNK_ROWS + 1
    for j in range(CHUNK_ROWS + 2):
        value = silu((src_ref[chunk * CHUNK_ROWS + j].astype(F32) - mean) * gain + shift)
        if j == 0:
            value = jnp.where(top_edge & (chunk == 0), 0.0, value)
        if j == last:
            value = jnp.where(bottom_edge & (chunk == CHUNKS - 1), 0.0, value)
        before = jnp.where(place == 0, 0.0, pltpu.roll(value, 1, 0))
        after = jnp.where(place == cols - 1, 0.0, pltpu.roll(value, cols - 1, 0))
        u_ref[j, :, 0:channels] = before.astype(BF16)
        u_ref[j, :, channels:2 * channels] = value.astype(BF16)
        u_ref[j, :, 2 * channels:3 * channels] = after.astype(BF16)


def conv_chunk(u_ref, w):
    _, cols, depth = u_ref.shape
    rows, split = CHUNK_ROWS * cols, w.shape[1] - LANES
    taps = [u_ref[dy:dy + CHUNK_ROWS].reshape(rows, depth) for dy in range(3)]
    main = jnp.dot(jnp.concatenate(taps, axis=1), w[:, 0:split], preferred_element_type=F32)
    both = jnp.concatenate([w[0:depth, split:], w[depth:2 * depth, split:]], axis=1)
    pair = jnp.dot(u_ref[0:CHUNK_ROWS + 1].reshape(rows + cols, depth), both, preferred_element_type=F32)
    third = jnp.dot(taps[2], w[2 * depth:, split:], preferred_element_type=F32)
    rest = pair[0:rows, 0:LANES] + pair[cols:, LANES:] + third
    return jnp.concatenate([main, rest], axis=1)


def conv_loop(order, ready, fill, finish, u_even, u_odd, w, arriving=False):
    def step(i, half, parity, u_now, u_next):
        after = jnp.minimum(i + 1, CHUNKS - 1)
        if arriving:
            finish(order(i), conv_chunk(u_now, w))
            ready(half, parity)
            fill(u_next, order(after))
        else:
            ready(half, parity)
            fill(u_next, order(after))
            finish(order(i), conv_chunk(u_now, w))

    def pair(half, carry):
        step(2 * half, half, 0, u_even, u_odd)
        step(2 * half + 1, half, 1, u_odd, u_even)
        return carry

    fill(u_even, order(jnp.int32(0)))
    lax.fori_loop(0, CHUNKS // 2, pair, 0)


def in_order(i):
    return i


def from_ends(i):
    return lax.rem(i + 1, 2) * lax.div(i, 2) + lax.rem(i, 2) * (CHUNKS - 1 - lax.div(i, 2))


def rows_of(ref, chunk, first=0):
    value = ref[pl.ds(chunk * CHUNK_ROWS + first, CHUNK_ROWS)]
    return value.reshape(value.shape[0] * value.shape[1], value.shape[2])


def send_edge_row(ref, send_sem, recv_sem, src_ref=None, src_row=None):
    rows = ref.shape[0] - 2
    core = position()[1]
    src = ref.at[rows - (rows - 1) * core] if src_ref is None else src_ref.at[src_row]
    return pltpu.make_async_remote_copy(
        src_ref=src, dst_ref=ref.at[(rows + 1) * core],
        send_sem=send_sem, recv_sem=recv_sem, device_id=partner_id(), device_id_type=MESH)


def first_kernel(count, x_ref, emb_ref, scale_ref, shift_ref, w_ref, tw_ref, out_ref, stat_ref, time_ref,
                 x_vmem, a_ref, h_ref, u_even, u_odd, w_vmem, tw_vmem, acc_ref, time_all, grp_recv, grp_total, st_send, st_recv,
                 load_sem, grp_ssem, grp_rsem, st_ssem, st_rsem, edge_ssem, edge_rsem, piece_ssem, piece_rsem, halo_ssem, halo_rsem):
    images, tile_rows, tile_cols, channels = x_ref.shape
    rows = 2 * tile_rows
    chip_x, core, chip_y = position()
    sp = lax.axis_index("sp")
    me = 2 * sp + chip_y
    image = 2 * chip_x + chip_y

    signal_all()
    x_load = pltpu.make_async_copy(x_ref, x_vmem, load_sem.at[0])
    x_load.start()
    weights = [pltpu.make_async_copy(w_ref.at[k], w_vmem.at[k], load_sem.at[1 + k]) for k in range(2)]
    tw_load = pltpu.make_async_copy(tw_ref, tw_vmem, load_sem.at[3])
    tw_load.start()

    def piece(part, source_core):
        low, high = PIECES[part]
        start = (1 - source_core) * low + source_core * (tile_rows - low - high)
        return pl.ds(start, high), pl.ds(1 + source_core * tile_rows + start, high)

    def piece_copies(k, part):
        to_x, to_y = lax.rem(chip_x + k // 2, 2), lax.rem(chip_y + k % 2, 2)
        src_rows, dst_rows = piece(part, core)
        src = x_ref.at[2 * to_x + to_y, src_rows]
        dst = a_ref.at[dst_rows, pl.ds(chip_y * tile_cols, tile_cols)]
        landed = piece_rsem.at[part, 2 * chip_y + core]
        remote = pltpu.make_async_remote_copy(
            src_ref=src, dst_ref=dst, send_sem=piece_ssem.at[k, part], recv_sem=landed,
            device_id={"sp": 2 * to_x + chip_x, "sp2": to_y}, device_id_type=MESH)
        return remote, pltpu.make_async_copy(src, dst, landed)

    def halo_copies(k):
        to_x, to_y = lax.rem(chip_x + k // 2, 2), lax.rem(chip_y + k % 2, 2)
        src = x_ref.at[2 * to_x + to_y, (tile_rows - 1) * core]
        dst = a_ref.at[(rows + 1) * chip_x, pl.ds(chip_y * tile_cols, tile_cols)]
        remote = pltpu.make_async_remote_copy(
            src_ref=src, dst_ref=dst, send_sem=halo_ssem.at[k], recv_sem=halo_rsem.at[chip_y],
            device_id={"sp": 2 * to_x + 1 - chip_x, "sp2": to_y}, device_id_type=MESH)
        return remote, pltpu.make_async_copy(src, dst, halo_rsem.at[chip_y])

    at_home = core == chip_x
    far_first = (3, 2, 1, 0)

    def send_piece(part):
        for k in far_first:
            remote, local = piece_copies(k, part)
            if k:
                remote.start()
            else:
                pl.when(at_home)(local.start)
                pl.when(jnp.logical_not(at_home))(remote.start)

    wait_all()

    @pl.when(jnp.logical_not(at_home))
    def _():
        for k in far_first:
            halo_copies(k)[0 if k else 1].start()

    send_piece(0)
    for copy in weights:
        copy.start()

    gather, spread = group_matrices(channels)
    x_load.wait()
    moments = []
    for i in range(images):
        acc_ref[...] = jnp.zeros_like(acc_ref)

        def add_row(row, carry):
            add_moments(acc_ref, x_vmem[i, row].astype(F32))
            return carry

        lax.fori_loop(0, tile_rows, add_row, 0)
        moments += [jnp.sum(acc_ref[0], axis=0, keepdims=True), jnp.sum(acc_ref[1], axis=0, keepdims=True)]
    grp_recv[me] = exact_dot(jnp.concatenate(moments, axis=0), gather)
    group_copies = []
    for k, (to_sp, to_y) in enumerate(others()):
        copy = pltpu.make_async_remote_copy(
            src_ref=grp_recv.at[me], dst_ref=grp_recv.at[me], send_sem=grp_ssem.at[k], recv_sem=grp_rsem.at[me],
            device_id={"sp": to_sp, "sp2": to_y}, device_id_type=MESH)
        copy.start()
        group_copies.append((copy, 2 * to_sp + to_y))

    for part in range(1, len(PIECES)):
        send_piece(part)

    tw_load.wait()
    emb = silu(emb_ref[...].astype(F32)).astype(BF16)
    for k in range(2):
        time_all[k, 0:images] = jnp.dot(emb, tw_vmem[k], preferred_element_type=F32)
    time_ref[...] = jnp.broadcast_to(time_all[1, pl.ds(image, 1)], time_ref.shape)
    time_vec = time_all[0, pl.ds(image, 1)]

    total = jnp.zeros((8, LANES), F32)
    for copy, _ in group_copies:
        copy.wait_send()
    for copy, sender in group_copies:
        pltpu.make_async_copy(grp_recv.at[sender], grp_recv.at[sender], grp_rsem.at[sender]).wait()
    for slot in range(8):
        total = total + grp_recv[slot]
    grp_total[...] = total
    mean, inv_std = spread_groups(grp_total[pl.ds(2 * image, 2)], spread, count)

    def wait_piece(part, source_core):
        for col in range(2):
            landed = a_ref.at[piece(part, source_core)[1], pl.ds(col * tile_cols, tile_cols)]
            pltpu.make_async_copy(landed, landed, piece_rsem.at[part, 2 * col + source_core]).wait()

    def ready(half, parity):
        if parity == 0:
            for part in range(3):
                pl.when(half == part)(functools.partial(wait_piece, part, 1))
        else:
            for part in range(1, 4):
                pl.when(half + 1 == part)(functools.partial(wait_piece, part, 0))
            pl.when(half + 1 == 3)(functools.partial(wait_piece, 3, 1))

    top_edge, bottom_edge = core == 0, core == 1

    def norm(k, mean, inv_std):
        return mean, inv_std * scale_ref[k:k + 1].astype(F32), shift_ref[k:k + 1].astype(F32)

    params = norm(0, mean, inv_std)
    for col in range(2):
        landed = a_ref.at[(rows + 1) * (1 - core), pl.ds(col * tile_cols, tile_cols)]
        pltpu.make_async_copy(landed, landed, halo_rsem.at[col]).wait()
    wait_piece(0, 0)
    acc_ref[...] = jnp.zeros_like(acc_ref)
    weights[0].wait()

    def finish_first(chunk, total):
        hidden = (total + time_vec).astype(BF16)
        h_ref[pl.ds(chunk * CHUNK_ROWS + 1, CHUNK_ROWS)] = hidden.reshape(CHUNK_ROWS, 2 * tile_cols, channels)
        add_moments(acc_ref, hidden.astype(F32))

    conv_loop(from_ends, ready, lambda u_ref, chunk: fill_chunk(u_ref, a_ref, chunk, params, top_edge, bottom_edge),
              finish_first, u_even, u_odd, w_vmem.at[0], arriving=True)

    edge = send_edge_row(h_ref, edge_ssem, edge_rsem)
    edge.start()
    st_send[0] = moment_rows(acc_ref)
    acc_ref[...] = jnp.zeros_like(acc_ref)
    weights[1].wait()
    second = norm(1, *norm_params(exchange(0, st_send, st_recv, st_ssem, st_rsem), count))
    edge.wait()

    def finish_second(chunk, total):
        new = (rows_of(a_ref, chunk, 1).astype(F32) + total).astype(BF16)
        out_ref[pl.ds(chunk * CHUNK_ROWS, CHUNK_ROWS)] = new.reshape(CHUNK_ROWS, 2 * tile_cols, channels)
        add_moments(acc_ref, new.astype(F32))

    conv_loop(in_order, lambda half, parity: None,
              lambda u_ref, chunk: fill_chunk(u_ref, h_ref, chunk, second, top_edge, bottom_edge),
              finish_second, u_even, u_odd, w_vmem.at[1])
    stat_ref[...] = moment_rows(acc_ref)

    @pl.when(jnp.logical_not(at_home))
    def _():
        for k in (1, 2, 3):
            halo_copies(k)[0].wait_send()

    for part in range(len(PIECES)):
        for k in range(4):
            remote, _ = piece_copies(k, part)
            if k:
                remote.wait_send()
            else:
                pl.when(jnp.logical_not(at_home))(remote.wait_send)


def second_kernel(count, a_hbm, stat_in, time_ref, scale_ref, shift_ref, w_ref, out_ref,
                  a_ref, h_ref, u_even, u_odd, w_vmem, acc_ref, res_ref, st_send, st_recv,
                  load_sem, st_ssem, st_rsem, edge_ssem, edge_rsem, tile_ssem, tile_rsem):
    rows, cols, channels = res_ref.shape
    tile_rows, tile_cols = rows // 2, cols // 2
    chip_x, core, chip_y = position()
    sp = lax.axis_index("sp")
    image = 2 * chip_x + chip_y

    signal_all()
    a_load = pltpu.make_async_copy(a_hbm, a_ref.at[pl.ds(1, rows)], load_sem.at[0])
    a_load.start()
    weights = [pltpu.make_async_copy(w_ref.at[2 + k], w_vmem.at[k], load_sem.at[1 + k]) for k in range(2)]
    for copy in weights:
        copy.start()
    st_send[0] = stat_in[...]
    acc_ref[...] = jnp.zeros_like(acc_ref)
    wait_all()
    edge = send_edge_row(a_ref, edge_ssem.at[0], edge_rsem.at[0], a_hbm, (rows - 1) * (1 - core))
    edge.start()
    top_edge, bottom_edge = core == 0, core == 1

    def norm(k, sums):
        mean, inv_std = norm_params(sums, count)
        return mean, inv_std * scale_ref[3 + k:4 + k].astype(F32), shift_ref[3 + k:4 + k].astype(F32)

    params = norm(0, exchange(0, st_send, st_recv, st_ssem, st_rsem))
    a_load.wait()
    edge.wait()
    weights[0].wait()
    time_vec = time_ref[0:1]

    def finish_first(chunk, total):
        hidden = (total + time_vec).astype(BF16)
        h_ref[pl.ds(chunk * CHUNK_ROWS + 1, CHUNK_ROWS)] = hidden.reshape(CHUNK_ROWS, cols, channels)
        add_moments(acc_ref, hidden.astype(F32))

    conv_loop(in_order, lambda half, parity: None,
              lambda u_ref, chunk: fill_chunk(u_ref, a_ref, chunk, params, top_edge, bottom_edge),
              finish_first, u_even, u_odd, w_vmem.at[0])

    edge = send_edge_row(h_ref, edge_ssem.at[1], edge_rsem.at[1])
    edge.start()
    st_send[1] = moment_rows(acc_ref)
    weights[1].wait()
    second = norm(1, exchange(1, st_send, st_recv, st_ssem, st_rsem))
    edge.wait()

    per_tile = CHUNKS // 2

    def home_copies(chunk, col):
        to_sp = 2 * core + lax.div(chunk, per_tile)
        slot = lax.rem(chunk, per_tile)
        here = (to_sp == sp) & (chip_y == col)
        src = res_ref.at[pl.ds(chunk * CHUNK_ROWS, CHUNK_ROWS), pl.ds(col * tile_cols, tile_cols)]
        dst = out_ref.at[image, pl.ds(slot * CHUNK_ROWS, CHUNK_ROWS)]
        landed = tile_rsem.at[image, slot]
        remote = pltpu.make_async_remote_copy(
            src_ref=src, dst_ref=dst, send_sem=tile_ssem.at[chunk, col], recv_sem=landed,
            device_id={"sp": to_sp, "sp2": col}, device_id_type=MESH)
        return here, remote, pltpu.make_async_copy(src, dst, landed)

    def send_home(chunk):
        for col in range(2):
            here, remote, local = home_copies(chunk, col)
            pl.when(here)(local.start)
            pl.when(jnp.logical_not(here))(remote.start)

    def ready(half, parity):
        if parity:
            send_home(2 * half)
        else:
            pl.when(half > 0)(lambda: send_home(2 * half - 1))

    def finish_second(chunk, total):
        new = (rows_of(a_ref, chunk, 1).astype(F32) + total).astype(BF16)
        res_ref[pl.ds(chunk * CHUNK_ROWS, CHUNK_ROWS)] = new.reshape(CHUNK_ROWS, cols, channels)

    conv_loop(in_order, ready, lambda u_ref, chunk: fill_chunk(u_ref, h_ref, chunk, second, top_edge, bottom_edge),
              finish_second, u_even, u_odd, w_vmem.at[1])
    send_home(jnp.int32(CHUNKS - 1))
    for chunk in range(CHUNKS):
        for col in range(2):
            here, remote, _ = home_copies(jnp.int32(chunk), col)
            pl.when(jnp.logical_not(here))(remote.wait_send)
    for slot in range(4):
        for part in range(per_tile):
            landed = out_ref.at[slot, pl.ds(part * CHUNK_ROWS, CHUNK_ROWS)]
            pltpu.make_async_copy(landed, landed, tile_rsem.at[slot, part]).wait()


def attention_kernel(norm_idx, count, logit_scale, a_hbm, stat_in, scale_ref, shift_ref, w_hbm, wo_hbm,
                     out_ref, stat_ref, a_ref, n_ref, q_ref, k_ref, v_ref, s_even, s_odd, peak_ref, total_ref, part_ref, o_ref,
                     wq_ref, wk_ref, wv_ref, wo_ref, acc_ref,
                     st_send, st_recv, load_sem, st_ssem, st_rsem, kv_ssem, kv_rsem):
    tokens, channels = a_ref.shape
    heads, head_dim, _ = v_ref.shape
    pairs = ((a_hbm, a_ref), (w_hbm.at[1], wk_ref), (w_hbm.at[2], wv_ref), (w_hbm.at[0], wq_ref), (wo_hbm, wo_ref))
    loads = [pltpu.make_async_copy(src, dst, load_sem.at[i]) for i, (src, dst) in enumerate(pairs)]
    for load in loads:
        load.start()
    for head in range(heads):
        k_ref[head, 0:tokens, head_dim:] = jnp.zeros((tokens, LANES - head_dim), BF16)
        q_ref[head, head_dim:] = jnp.zeros((LANES - head_dim, tokens), BF16)
    st_send[0] = stat_in[...]
    barrier_pair()
    sums = exchange(0, st_send, st_recv, st_ssem, st_rsem)
    mean, inv_std = norm_params(sums, count)
    gain = inv_std * scale_ref[norm_idx:norm_idx + 1].astype(F32)
    shift = shift_ref[norm_idx:norm_idx + 1].astype(F32)
    for load in loads[:3]:
        load.wait()

    step = TOKEN_BLOCK
    chunks = tokens // step
    transposed = (((1,), (1,)), ((), ()))

    def head_copy(which, head, chunk=None):
        first, size = (0, tokens) if chunk is None else (pl.multiple_of(chunk * step, step), step)
        src, dst = pl.ds(first, size), pl.ds(tokens + first, size)
        if which:
            src_ref, dst_ref = v_ref.at[head, :, src], v_ref.at[head, :, dst]
        else:
            src_ref, dst_ref = k_ref.at[head, src], k_ref.at[head, dst]
        slot = head if chunk is None else heads + chunk
        return pltpu.make_async_remote_copy(
            src_ref=src_ref, dst_ref=dst_ref, send_sem=kv_ssem.at[which, slot], recv_sem=kv_rsem.at[which, slot],
            device_id=partner_id(), device_id_type=MESH)

    def both(act, head, chunk=None):
        for which in range(2):
            getattr(head_copy(which, head, chunk), act)()

    def key_values(i, carry):
        here = pl.ds(pl.multiple_of(i * step, step), step)
        normed = ((a_ref[here].astype(F32) - mean) * gain + shift).astype(BF16)
        n_ref[here] = normed
        part = lax.dot_general(normed, wk_ref[...], transposed, preferred_element_type=F32).astype(BF16)
        for head in range(heads):
            k_ref[head, here, 0:head_dim] = part[:, head * head_dim:(head + 1) * head_dim]
        part = lax.dot_general(wv_ref[...], normed, transposed, preferred_element_type=F32).astype(BF16)
        for head in range(heads):
            v_ref[head, :, here] = part[head * head_dim:(head + 1) * head_dim]

        @pl.when(i > 0)
        def _():
            both("start", 0, i - 1)
        return carry

    lax.fori_loop(0, chunks, key_values, 0)
    loads[3].wait()

    def query_chunk(i):
        here = pl.ds(pl.multiple_of(i * step, step), step)
        part = lax.dot_general(wq_ref[...], n_ref[here], transposed, preferred_element_type=F32).astype(BF16)
        for head in range(heads):
            q_ref[head, 0:head_dim, here] = part[head * head_dim:(head + 1) * head_dim]

    def queries(i, carry):
        query_chunk(2 * i)
        query_chunk(2 * i + 1)

        @pl.when(i == 0)
        def _():
            both("start", 0, chunks - 1)
            for head in range(1, heads):
                both("start", head)
        return carry

    lax.fori_loop(0, chunks // 2, queries, 0)

    for i in range(chunks):
        both("wait_recv", 0, i)

    blocks = tokens // QUERY_BLOCK
    key_blocks = 2 * tokens // KEY_BLOCK

    def fold(value, combine):
        return combine(value.reshape(KEY_BLOCK // 8, 8, QUERY_BLOCK), axis=0)

    def place_of(block):
        first = pl.multiple_of(lax.rem(block, blocks) * QUERY_BLOCK, QUERY_BLOCK)
        return lax.div(block, blocks), pl.ds(first, QUERY_BLOCK)

    def keys_of(j):
        return slice(j * KEY_BLOCK, (j + 1) * KEY_BLOCK)

    def score(j, head, query, s_ref, peak):
        scores = jnp.dot(k_ref[head, keys_of(j)], query, preferred_element_type=F32)
        s_ref[keys_of(j)] = scores
        piece = fold(scores, jnp.max)
        return piece if peak is None else jnp.maximum(peak, piece)

    def absorb(j, head, peak, s_ref, state):
        weights = jnp.exp2((s_ref[keys_of(j)] - peak) * logit_scale)
        total = fold(weights, jnp.sum)
        attended = jnp.dot(v_ref[head, :, keys_of(j)], weights.astype(BF16), preferred_element_type=F32)
        return (total, attended) if state is None else (state[0] + total, state[1] + attended)

    def finish_block(block, peak, s_ref, state):
        head, here = place_of(block)
        total, attended = absorb(key_blocks - 1, head, peak, s_ref, state)
        total = jnp.sum(total, axis=0, keepdims=True)
        o_ref[pl.ds(pl.multiple_of(head * head_dim, 16), head_dim), here] = (attended / total).astype(BF16)

    def peak_of(slot):
        return jnp.max(peak_ref[slot], axis=0, keepdims=True)

    def advance(i, s_ref, s_next, slot, state):
        head, _ = place_of(i)
        next_head, next_here = place_of(jnp.minimum(i + 1, heads * blocks - 1))
        query = q_ref[next_head, :, next_here]
        peak, next_peak, new_state = peak_of(slot), None, None
        for j in range(key_blocks):
            next_peak = score(j, next_head, query, s_next, next_peak)
            if j == 1:
                finish_block(jnp.maximum(i - 1, 0), peak_of(1 - slot), s_next, state)
            if j:
                new_state = absorb(j - 1, head, peak, s_ref, new_state)
        peak_ref[1 - slot] = next_peak
        return new_state

    s_odd[keys_of(key_blocks - 1)] = jnp.zeros((KEY_BLOCK, QUERY_BLOCK), F32)
    peak_ref[1] = jnp.zeros((8, QUERY_BLOCK), F32)
    total_ref[...] = jnp.zeros_like(total_ref)
    part_ref[...] = jnp.zeros_like(part_ref)
    query = q_ref[0, :, 0:QUERY_BLOCK]
    first_peak = None
    for j in range(key_blocks):
        first_peak = score(j, 0, query, s_even, first_peak)
    peak_ref[0] = first_peak

    def attend(head, carry):
        pl.when(head + 1 < heads)(lambda: both("wait_recv", head + 1))
        state = (total_ref[...], part_ref[...])
        for j in range(0, blocks, 2):
            state = advance(blocks * head + j, s_even, s_odd, 0, state)
            state = advance(blocks * head + j + 1, s_odd, s_even, 1, state)
        total_ref[...], part_ref[...] = state
        return carry

    lax.fori_loop(0, heads, attend, 0)
    finish_block(jnp.int32(heads * blocks - 1), peak_of(1), s_odd, (total_ref[...], part_ref[...]))
    for i in range(chunks):
        both("wait_send", 0, i)
    for head in range(1, heads):
        both("wait_send", head)
    loads[4].wait()
    acc_ref[...] = jnp.zeros_like(acc_ref)

    def project_chunk(i):
        here = pl.ds(pl.multiple_of(i * step, step), step)
        added = lax.dot_general(o_ref[:, here], wo_ref[...], (((0,), (0,)), ((), ())), preferred_element_type=F32)
        new = (a_ref[here].astype(F32) + added).astype(BF16)
        a_ref[here] = new
        add_moments(acc_ref, new.astype(F32))

    def leave(i):
        here = pl.ds(pl.multiple_of(i * 2 * step, 2 * step), 2 * step)
        return pltpu.make_async_copy(a_ref.at[here], out_ref.at[here], load_sem.at[i])

    def project(i, carry):
        pl.when(i > 0)(lambda: leave(i - 1).start())
        project_chunk(2 * i)
        project_chunk(2 * i + 1)
        return carry

    lax.fori_loop(0, chunks // 2, project, 0)
    stat_ref[...] = moment_rows(acc_ref)
    leave(chunks // 2 - 1).start()
    for i in range(chunks // 2):
        leave(i).wait()


VMEM_SPEC = pl.BlockSpec(memory_space=pltpu.VMEM)
ANY_SPEC = pl.BlockSpec(memory_space=pl.ANY)


def params(collective_id):
    return pltpu.CompilerParams(collective_id=collective_id, has_side_effects=True, vmem_limit_bytes=60 * 2**20)


def conv_scratch(rows, cols, channels):
    return [
        pltpu.VMEM((rows + 2, cols, channels), BF16),
        pltpu.VMEM((rows + 2, cols, channels), BF16),
        pltpu.VMEM((CHUNK_ROWS + 2, cols, 3 * channels), BF16),
        pltpu.VMEM((CHUNK_ROWS + 2, cols, 3 * channels), BF16),
        pltpu.VMEM((2, 9 * channels, channels), BF16),
    ]


def first_call(count, rows, cols, x, time_emb, scale, shift, w, time_w):
    channels = x.shape[3]
    dma = pltpu.SemaphoreType.DMA
    return pl.pallas_call(
        functools.partial(first_kernel, count),
        out_shape=[
            jax.ShapeDtypeStruct((rows, cols, channels), BF16),
            jax.ShapeDtypeStruct((8, channels), F32),
            jax.ShapeDtypeStruct((8, channels), F32),
        ],
        in_specs=[ANY_SPEC, VMEM_SPEC, VMEM_SPEC, VMEM_SPEC, ANY_SPEC, ANY_SPEC],
        out_specs=[VMEM_SPEC, VMEM_SPEC, VMEM_SPEC],
        scratch_shapes=[pltpu.VMEM(x.shape, BF16)] + conv_scratch(rows, cols, channels) + [
            pltpu.VMEM(time_w.shape, BF16),
            pltpu.VMEM((2, 8, channels), F32),
            pltpu.VMEM((2, 8, channels), F32),
            pltpu.VMEM((8, 8, LANES), F32),
            pltpu.VMEM((8, LANES), F32),
            pltpu.VMEM((1, 8, channels), F32),
            pltpu.VMEM((1, 8, channels), F32),
            dma((4,)), dma((7,)), dma((8,)), dma((1,)), dma((1,)), dma, dma,
            dma((4, len(PIECES))), dma((len(PIECES), 4)), dma((4,)), dma((2,)),
        ],
        compiler_params=params(0),
        name="res_first",
    )(x, time_emb, scale, shift, w, time_w)


def second_call(count, tile_shape, a, stats, time_vec, scale, shift, w):
    rows, cols, channels = a.shape
    dma = pltpu.SemaphoreType.DMA
    return pl.pallas_call(
        functools.partial(second_kernel, count),
        out_shape=jax.ShapeDtypeStruct(tile_shape, BF16),
        in_specs=[ANY_SPEC, VMEM_SPEC, VMEM_SPEC, VMEM_SPEC, VMEM_SPEC, ANY_SPEC],
        out_specs=ANY_SPEC,
        scratch_shapes=conv_scratch(rows, cols, channels) + [
            pltpu.VMEM((2, 8, channels), F32),
            pltpu.VMEM((rows, cols, channels), BF16),
            pltpu.VMEM((2, 8, channels), F32),
            pltpu.VMEM((2, 8, channels), F32),
            dma((3,)), dma((2,)), dma((2,)), dma((2,)), dma((2,)), dma((CHUNKS, 2)), dma((4, CHUNKS // 2)),
        ],
        compiler_params=params(2),
        name="res_second",
    )(a, stats, time_vec, scale, shift, w)


def copy_kernel(src_ref, out_ref, buf_ref, in_sem, out_sem):
    parts = [(i, slice(j * 8, (j + 1) * 8)) for i in range(src_ref.shape[0]) for j in range(src_ref.shape[1] // 8)]
    reads = [pltpu.make_async_copy(src_ref.at[i, rows], buf_ref.at[i, rows], in_sem.at[n]) for n, (i, rows) in enumerate(parts)]
    writes = [pltpu.make_async_copy(buf_ref.at[i, rows], out_ref.at[i, rows], out_sem.at[n]) for n, (i, rows) in enumerate(parts)]
    for read in reads:
        read.start()
    for read, write in zip(reads, writes):
        read.wait()
        write.start()
    for write in writes:
        write.wait()


def copy_call(src):
    parts = src.shape[0] * (src.shape[1] // 8)
    return pl.pallas_call(
        copy_kernel,
        out_shape=jax.ShapeDtypeStruct(src.shape, src.dtype),
        in_specs=[ANY_SPEC],
        out_specs=ANY_SPEC,
        scratch_shapes=[pltpu.VMEM(src.shape, src.dtype), pltpu.SemaphoreType.DMA((parts,)), pltpu.SemaphoreType.DMA((parts,))],
        name="copy_out",
    )(src)


def attention_call(norm_idx, count, heads, a, stats, scale, shift, w, wo):
    tokens, channels = a.shape
    head_dim = channels // heads
    logit_scale = head_dim ** -0.5 * 1.4426950408889634
    return pl.pallas_call(
        functools.partial(attention_kernel, norm_idx, count, logit_scale),
        out_shape=[jax.ShapeDtypeStruct((tokens, channels), BF16), jax.ShapeDtypeStruct((8, channels), F32)],
        in_specs=[ANY_SPEC, VMEM_SPEC, VMEM_SPEC, VMEM_SPEC, ANY_SPEC, ANY_SPEC],
        out_specs=[ANY_SPEC, VMEM_SPEC],
        scratch_shapes=[
            pltpu.VMEM((tokens, channels), BF16),
            pltpu.VMEM((tokens, channels), BF16),
            pltpu.VMEM((heads, LANES, tokens), BF16),
            pltpu.VMEM((heads, 2 * tokens, LANES), BF16),
            pltpu.VMEM((heads, head_dim, 2 * tokens), BF16),
            pltpu.VMEM((2 * tokens, QUERY_BLOCK), F32),
            pltpu.VMEM((2 * tokens, QUERY_BLOCK), F32),
            pltpu.VMEM((2, 8, QUERY_BLOCK), F32),
            pltpu.VMEM((8, QUERY_BLOCK), F32),
            pltpu.VMEM((head_dim, QUERY_BLOCK), F32),
            pltpu.VMEM((channels, tokens), BF16),
            pltpu.VMEM((channels, channels), BF16),
            pltpu.VMEM((channels, channels), BF16),
            pltpu.VMEM((channels, channels), BF16),
            pltpu.VMEM((channels, channels), BF16),
            pltpu.VMEM((2, 8, channels), F32),
            pltpu.VMEM((1, 8, channels), F32),
            pltpu.VMEM((1, 8, channels), F32),
            pltpu.SemaphoreType.DMA((5,)),
            pltpu.SemaphoreType.DMA((1,)),
            pltpu.SemaphoreType.DMA((1,)),
            pltpu.SemaphoreType.DMA((2, heads + tokens // TOKEN_BLOCK)),
            pltpu.SemaphoreType.DMA((2, heads + tokens // TOKEN_BLOCK)),
        ],
        compiler_params=params(1),
        name="attention",
    )(a, stats, scale, shift, w, wo)


def solution(mesh):
    lat_spec = P("dp", "sp", "sp2", None)

    def local(x, time_emb, gn_scale, gn_shift, conv_w, time_w, w_qkv, w_out):
        images, tile_rows, tile_cols, channels = x.shape
        rows, cols = 2 * tile_rows, 2 * tile_cols
        count = 2 * rows * cols * (channels // GROUPS)
        heads = w_out.shape[0]
        w = conv_w.reshape(4, 9 * channels, channels)
        qkv = jnp.transpose(w_qkv, (0, 2, 3, 1)).reshape(3, channels, channels)
        wo = w_out.reshape(channels, channels)
        first, stats, time_vec = first_call(count, rows, cols, x, time_emb, gn_scale, gn_shift, w, time_w)
        middle, stats = attention_call(2, count, heads, first.reshape(rows * cols, channels), stats, gn_scale, gn_shift, qkv, wo)
        return copy_call(second_call(count, x.shape, middle.reshape(rows, cols, channels), stats, time_vec, gn_scale, gn_shift, w))

    return jax.shard_map(local, mesh=mesh, in_specs=(lat_spec, P("dp", None), P(), P(), P(), P(), P(), P()), out_specs=lat_spec, check_vma=False)
```

```python
import functools

import jax
import jax.numpy as jnp
from jax import lax
from jax.experimental import pallas as pl
from jax.experimental.pallas import tpu as pltpu
from jax.sharding import PartitionSpec as P

GROUPS = 32
NORM_EPS = 1e-5
LANES = 128
CHUNK_ROWS = 4
CHUNKS = 8
PIECES = ((0, 5), (5, 4), (9, 4), (13, 3))
QUERY_BLOCK = 512
KEY_BLOCK = 512
TOKEN_BLOCK = 512
MESH = pl.DeviceIdType.MESH
F32 = jnp.float32
BF16 = jnp.bfloat16


def position():
    sp = lax.axis_index("sp")
    return lax.div(sp, 2), lax.rem(sp, 2), lax.axis_index("sp2")


def partner_id():
    chip_x, core, _ = position()
    return {"sp": 2 * chip_x + 1 - core}


def barrier_pair():
    sem = pltpu.get_barrier_semaphore()
    pl.semaphore_signal(sem, inc=1, device_id=partner_id(), device_id_type=MESH)
    pl.semaphore_wait(sem, 1)


def others():
    sp, col = lax.axis_index("sp"), lax.axis_index("sp2")
    return [(lax.rem(sp + i, 4), lax.rem(col + j, 2)) for i in range(4) for j in range(2) if i or j]


def signal_all():
    for sp, col in others():
        pl.semaphore_signal(pltpu.get_barrier_semaphore(), inc=1, device_id={"sp": sp, "sp2": col}, device_id_type=MESH)


def wait_all():
    pl.semaphore_wait(pltpu.get_barrier_semaphore(), 7)


def split3(value):
    high = value.astype(BF16).astype(F32)
    rest = value - high
    mid = rest.astype(BF16).astype(F32)
    low = rest - mid
    return jnp.concatenate([high, mid, low, jnp.zeros_like(value)], axis=0).astype(BF16)


def exact_dot(value, one_hot):
    out = jnp.dot(split3(value), one_hot, preferred_element_type=F32)
    return out[0:8] + out[8:16] + out[16:24]


def group_matrices(channels):
    width = channels // GROUPS
    chan = lax.broadcasted_iota(jnp.int32, (channels, LANES), 0)
    grp = lax.broadcasted_iota(jnp.int32, (channels, LANES), 1) * width
    gather = jnp.where((chan >= grp) & (chan < grp + width), 1.0, 0.0).astype(BF16)
    chan_t = lax.broadcasted_iota(jnp.int32, (LANES, channels), 1)
    grp_t = lax.broadcasted_iota(jnp.int32, (LANES, channels), 0) * width
    spread = jnp.where((chan_t >= grp_t) & (chan_t < grp_t + width), 1.0, 0.0).astype(BF16)
    return gather, spread


def spread_groups(group_sums, spread, count):
    mean = group_sums[0:1] / count
    inv_std = lax.rsqrt(group_sums[1:2] / count - mean * mean + NORM_EPS)
    stacked = jnp.concatenate([mean, inv_std, jnp.zeros((6, LANES), F32)], axis=0)
    per_channel = exact_dot(stacked, spread)
    return per_channel[0:1], per_channel[1:2]


def norm_params(sums, count):
    gather, spread = group_matrices(sums.shape[1])
    return spread_groups(exact_dot(sums, gather)[0:2], spread, count)


def fold_rows(value):
    rows, channels = value.shape
    return jnp.sum(value.reshape(rows // 8, 8, channels), axis=0)


def add_moments(acc_ref, value):
    acc_ref[0] += fold_rows(value)
    acc_ref[1] += fold_rows(value * value)


def moment_rows(acc_ref):
    total = jnp.sum(acc_ref[0], axis=0, keepdims=True)
    square = jnp.sum(acc_ref[1], axis=0, keepdims=True)
    return jnp.concatenate([total, square, jnp.zeros((6, total.shape[1]), F32)], axis=0)


def exchange(slot, send_ref, recv_ref, send_sem, recv_sem, meanwhile=None):
    copy = pltpu.make_async_remote_copy(
        src_ref=send_ref.at[slot],
        dst_ref=recv_ref.at[slot],
        send_sem=send_sem.at[slot],
        recv_sem=recv_sem.at[slot],
        device_id=partner_id(),
        device_id_type=MESH,
    )
    copy.start()
    if meanwhile is not None:
        meanwhile()
    copy.wait()
    return send_ref[slot] + recv_ref[slot]


def silu(value):
    half = 0.5 * value
    return half + half * jnp.tanh(half)


def fill_chunk(u_ref, src_ref, chunk, params, top_edge, bottom_edge):
    mean, gain, shift = params
    _, cols, channels = src_ref.shape
    place = lax.broadcasted_iota(jnp.int32, (cols, channels), 0)
    last = CHUNK_ROWS + 1
    for j in range(CHUNK_ROWS + 2):
        value = silu((src_ref[chunk * CHUNK_ROWS + j].astype(F32) - mean) * gain + shift)
        if j == 0:
            value = jnp.where(top_edge & (chunk == 0), 0.0, value)
        if j == last:
            value = jnp.where(bottom_edge & (chunk == CHUNKS - 1), 0.0, value)
        before = jnp.where(place == 0, 0.0, pltpu.roll(value, 1, 0))
        after = jnp.where(place == cols - 1, 0.0, pltpu.roll(value, cols - 1, 0))
        u_ref[j, :, 0:channels] = before.astype(BF16)
        u_ref[j, :, channels:2 * channels] = value.astype(BF16)
        u_ref[j, :, 2 * channels:3 * channels] = after.astype(BF16)


def conv_chunk(u_ref, w):
    _, cols, depth = u_ref.shape
    rows, split = CHUNK_ROWS * cols, w.shape[1] - LANES
    taps = [u_ref[dy:dy + CHUNK_ROWS].reshape(rows, depth) for dy in range(3)]
    main = jnp.dot(jnp.concatenate(taps, axis=1), w[:, 0:split], preferred_element_type=F32)
    both = jnp.concatenate([w[0:depth, split:], w[depth:2 * depth, split:]], axis=1)
    pair = jnp.dot(u_ref[0:CHUNK_ROWS + 1].reshape(rows + cols, depth), both, preferred_element_type=F32)
    third = jnp.dot(taps[2], w[2 * depth:, split:], preferred_element_type=F32)
    rest = pair[0:rows, 0:LANES] + pair[cols:, LANES:] + third
    return jnp.concatenate([main, rest], axis=1)


def conv_loop(order, ready, fill, finish, u_even, u_odd, w, arriving=False):
    def step(i, half, parity, u_now, u_next):
        after = jnp.minimum(i + 1, CHUNKS - 1)
        if arriving:
            finish(order(i), conv_chunk(u_now, w))
            ready(half, parity)
            fill(u_next, order(after))
        else:
            ready(half, parity)
            fill(u_next, order(after))
            finish(order(i), conv_chunk(u_now, w))

    def pair(half, carry):
        step(2 * half, half, 0, u_even, u_odd)
        step(2 * half + 1, half, 1, u_odd, u_even)
        return carry

    fill(u_even, order(jnp.int32(0)))
    lax.fori_loop(0, CHUNKS // 2, pair, 0)


def in_order(i):
    return i


def from_ends(i):
    return lax.rem(i + 1, 2) * lax.div(i, 2) + lax.rem(i, 2) * (CHUNKS - 1 - lax.div(i, 2))


def rows_of(ref, chunk, first=0):
    value = ref[pl.ds(chunk * CHUNK_ROWS + first, CHUNK_ROWS)]
    return value.reshape(value.shape[0] * value.shape[1], value.shape[2])


def send_edge_row(ref, send_sem, recv_sem, src_ref=None, src_row=None):
    rows = ref.shape[0] - 2
    core = position()[1]
    src = ref.at[rows - (rows - 1) * core] if src_ref is None else src_ref.at[src_row]
    return pltpu.make_async_remote_copy(
        src_ref=src, dst_ref=ref.at[(rows + 1) * core],
        send_sem=send_sem, recv_sem=recv_sem, device_id=partner_id(), device_id_type=MESH)


def first_kernel(count, x_ref, emb_ref, scale_ref, shift_ref, w_ref, tw_ref, out_ref, stat_ref, time_ref,
                 x_vmem, a_ref, h_ref, u_even, u_odd, w_vmem, tw_vmem, acc_ref, time_all, grp_recv, grp_total, st_send, st_recv,
                 load_sem, grp_ssem, grp_rsem, st_ssem, st_rsem, edge_ssem, edge_rsem, piece_ssem, piece_rsem, halo_ssem, halo_rsem):
    images, tile_rows, tile_cols, channels = x_ref.shape
    rows = 2 * tile_rows
    chip_x, core, chip_y = position()
    sp = lax.axis_index("sp")
    me = 2 * sp + chip_y
    image = 2 * chip_x + chip_y

    signal_all()
    x_load = pltpu.make_async_copy(x_ref, x_vmem, load_sem.at[0])
    x_load.start()
    weights = [pltpu.make_async_copy(w_ref.at[k], w_vmem.at[k], load_sem.at[1 + k]) for k in range(2)]
    tw_load = pltpu.make_async_copy(tw_ref, tw_vmem, load_sem.at[3])
    tw_load.start()

    def piece(part, source_core):
        low, high = PIECES[part]
        start = (1 - source_core) * low + source_core * (tile_rows - low - high)
        return pl.ds(start, high), pl.ds(1 + source_core * tile_rows + start, high)

    def piece_copies(k, part):
        to_x, to_y = lax.rem(chip_x + k // 2, 2), lax.rem(chip_y + k % 2, 2)
        src_rows, dst_rows = piece(part, core)
        src = x_ref.at[2 * to_x + to_y, src_rows]
        dst = a_ref.at[dst_rows, pl.ds(chip_y * tile_cols, tile_cols)]
        landed = piece_rsem.at[part, 2 * chip_y + core]
        remote = pltpu.make_async_remote_copy(
            src_ref=src, dst_ref=dst, send_sem=piece_ssem.at[k, part], recv_sem=landed,
            device_id={"sp": 2 * to_x + chip_x, "sp2": to_y}, device_id_type=MESH)
        return remote, pltpu.make_async_copy(src, dst, landed)

    def halo_copies(k):
        to_x, to_y = lax.rem(chip_x + k // 2, 2), lax.rem(chip_y + k % 2, 2)
        src = x_ref.at[2 * to_x + to_y, (tile_rows - 1) * core]
        dst = a_ref.at[(rows + 1) * chip_x, pl.ds(chip_y * tile_cols, tile_cols)]
        remote = pltpu.make_async_remote_copy(
            src_ref=src, dst_ref=dst, send_sem=halo_ssem.at[k], recv_sem=halo_rsem.at[chip_y],
            device_id={"sp": 2 * to_x + 1 - chip_x, "sp2": to_y}, device_id_type=MESH)
        return remote, pltpu.make_async_copy(src, dst, halo_rsem.at[chip_y])

    at_home = core == chip_x
    far_first = (3, 2, 1, 0)

    def send_piece(part):
        for k in far_first:
            remote, local = piece_copies(k, part)
            if k:
                remote.start()
            else:
                pl.when(at_home)(local.start)
                pl.when(jnp.logical_not(at_home))(remote.start)

    wait_all()

    @pl.when(jnp.logical_not(at_home))
    def _():
        for k in far_first:
            halo_copies(k)[0 if k else 1].start()

    send_piece(0)
    for copy in weights:
        copy.start()

    gather, spread = group_matrices(channels)
    x_load.wait()
    moments = []
    for i in range(images):
        acc_ref[...] = jnp.zeros_like(acc_ref)

        def add_row(row, carry):
            add_moments(acc_ref, x_vmem[i, row].astype(F32))
            return carry

        lax.fori_loop(0, tile_rows, add_row, 0)
        moments += [jnp.sum(acc_ref[0], axis=0, keepdims=True), jnp.sum(acc_ref[1], axis=0, keepdims=True)]
    grp_recv[me] = exact_dot(jnp.concatenate(moments, axis=0), gather)
    group_copies = []
    for k, (to_sp, to_y) in enumerate(others()):
        copy = pltpu.make_async_remote_copy(
            src_ref=grp_recv.at[me], dst_ref=grp_recv.at[me], send_sem=grp_ssem.at[k], recv_sem=grp_rsem.at[me],
            device_id={"sp": to_sp, "sp2": to_y}, device_id_type=MESH)
        copy.start()
        group_copies.append((copy, 2 * to_sp + to_y))

    for part in range(1, len(PIECES)):
        send_piece(part)

    tw_load.wait()
    emb = silu(emb_ref[...].astype(F32)).astype(BF16)
    for k in range(2):
        time_all[k, 0:images] = jnp.dot(emb, tw_vmem[k], preferred_element_type=F32)
    time_ref[...] = jnp.broadcast_to(time_all[1, pl.ds(image, 1)], time_ref.shape)
    time_vec = time_all[0, pl.ds(image, 1)]

    total = jnp.zeros((8, LANES), F32)
    for copy, _ in group_copies:
        copy.wait_send()
    for copy, sender in group_copies:
        pltpu.make_async_copy(grp_recv.at[sender], grp_recv.at[sender], grp_rsem.at[sender]).wait()
    for slot in range(8):
        total = total + grp_recv[slot]
    grp_total[...] = total
    mean, inv_std = spread_groups(grp_total[pl.ds(2 * image, 2)], spread, count)

    def wait_piece(part, source_core):
        for col in range(2):
            landed = a_ref.at[piece(part, source_core)[1], pl.ds(col * tile_cols, tile_cols)]
            pltpu.make_async_copy(landed, landed, piece_rsem.at[part, 2 * col + source_core]).wait()

    def ready(half, parity):
        if parity:
            for part in range(1, len(PIECES)):
                @pl.when(half + 1 == part)
                def _():
                    wait_piece(part, 0)
                    wait_piece(part, 1)

    top_edge, bottom_edge = core == 0, core == 1

    def norm(k, mean, inv_std):
        return mean, inv_std * scale_ref[k:k + 1].astype(F32), shift_ref[k:k + 1].astype(F32)

    params = norm(0, mean, inv_std)
    for col in range(2):
        landed = a_ref.at[(rows + 1) * (1 - core), pl.ds(col * tile_cols, tile_cols)]
        pltpu.make_async_copy(landed, landed, halo_rsem.at[col]).wait()
    wait_piece(0, 0)
    wait_piece(0, 1)
    acc_ref[...] = jnp.zeros_like(acc_ref)
    weights[0].wait()

    def finish_first(chunk, total):
        hidden = (total + time_vec).astype(BF16)
        h_ref[pl.ds(chunk * CHUNK_ROWS + 1, CHUNK_ROWS)] = hidden.reshape(CHUNK_ROWS, 2 * tile_cols, channels)
        add_moments(acc_ref, hidden.astype(F32))

    conv_loop(from_ends, ready, lambda u_ref, chunk: fill_chunk(u_ref, a_ref, chunk, params, top_edge, bottom_edge),
              finish_first, u_even, u_odd, w_vmem.at[0], arriving=True)

    edge = send_edge_row(h_ref, edge_ssem, edge_rsem)
    edge.start()
    st_send[0] = moment_rows(acc_ref)
    acc_ref[...] = jnp.zeros_like(acc_ref)
    weights[1].wait()
    second = norm(1, *norm_params(exchange(0, st_send, st_recv, st_ssem, st_rsem), count))
    edge.wait()

    def finish_second(chunk, total):
        new = (rows_of(a_ref, chunk, 1).astype(F32) + total).astype(BF16)
        out_ref[pl.ds(chunk * CHUNK_ROWS, CHUNK_ROWS)] = new.reshape(CHUNK_ROWS, 2 * tile_cols, channels)
        add_moments(acc_ref, new.astype(F32))

    conv_loop(in_order, lambda half, parity: None,
              lambda u_ref, chunk: fill_chunk(u_ref, h_ref, chunk, second, top_edge, bottom_edge),
              finish_second, u_even, u_odd, w_vmem.at[1])
    stat_ref[...] = moment_rows(acc_ref)

    @pl.when(jnp.logical_not(at_home))
    def _():
        for k in (1, 2, 3):
            halo_copies(k)[0].wait_send()

    for part in range(len(PIECES)):
        for k in range(4):
            remote, _ = piece_copies(k, part)
            if k:
                remote.wait_send()
            else:
                pl.when(jnp.logical_not(at_home))(remote.wait_send)


def second_kernel(count, a_hbm, stat_in, time_ref, scale_ref, shift_ref, w_ref, out_ref,
                  a_ref, h_ref, u_even, u_odd, w_vmem, acc_ref, res_ref, st_send, st_recv,
                  load_sem, st_ssem, st_rsem, edge_ssem, edge_rsem, tile_ssem, tile_rsem):
    rows, cols, channels = res_ref.shape
    tile_rows, tile_cols = rows // 2, cols // 2
    chip_x, core, chip_y = position()
    sp = lax.axis_index("sp")
    image = 2 * chip_x + chip_y

    signal_all()
    a_load = pltpu.make_async_copy(a_hbm, a_ref.at[pl.ds(1, rows)], load_sem.at[0])
    a_load.start()
    weights = [pltpu.make_async_copy(w_ref.at[2 + k], w_vmem.at[k], load_sem.at[1 + k]) for k in range(2)]
    for copy in weights:
        copy.start()
    st_send[0] = stat_in[...]
    acc_ref[...] = jnp.zeros_like(acc_ref)
    wait_all()
    edge = send_edge_row(a_ref, edge_ssem.at[0], edge_rsem.at[0], a_hbm, (rows - 1) * (1 - core))
    edge.start()
    top_edge, bottom_edge = core == 0, core == 1

    def norm(k, sums):
        mean, inv_std = norm_params(sums, count)
        return mean, inv_std * scale_ref[3 + k:4 + k].astype(F32), shift_ref[3 + k:4 + k].astype(F32)

    params = norm(0, exchange(0, st_send, st_recv, st_ssem, st_rsem))
    a_load.wait()
    edge.wait()
    weights[0].wait()
    time_vec = time_ref[0:1]

    def finish_first(chunk, total):
        hidden = (total + time_vec).astype(BF16)
        h_ref[pl.ds(chunk * CHUNK_ROWS + 1, CHUNK_ROWS)] = hidden.reshape(CHUNK_ROWS, cols, channels)
        add_moments(acc_ref, hidden.astype(F32))

    conv_loop(in_order, lambda half, parity: None,
              lambda u_ref, chunk: fill_chunk(u_ref, a_ref, chunk, params, top_edge, bottom_edge),
              finish_first, u_even, u_odd, w_vmem.at[0])

    edge = send_edge_row(h_ref, edge_ssem.at[1], edge_rsem.at[1])
    edge.start()
    st_send[1] = moment_rows(acc_ref)
    weights[1].wait()
    second = norm(1, exchange(1, st_send, st_recv, st_ssem, st_rsem))
    edge.wait()

    per_tile = CHUNKS // 2

    def home_copies(chunk, col):
        to_sp = 2 * core + lax.div(chunk, per_tile)
        slot = lax.rem(chunk, per_tile)
        here = (to_sp == sp) & (chip_y == col)
        src = res_ref.at[pl.ds(chunk * CHUNK_ROWS, CHUNK_ROWS), pl.ds(col * tile_cols, tile_cols)]
        dst = out_ref.at[image, pl.ds(slot * CHUNK_ROWS, CHUNK_ROWS)]
        landed = tile_rsem.at[image, slot]
        remote = pltpu.make_async_remote_copy(
            src_ref=src, dst_ref=dst, send_sem=tile_ssem.at[chunk, col], recv_sem=landed,
            device_id={"sp": to_sp, "sp2": col}, device_id_type=MESH)
        return here, remote, pltpu.make_async_copy(src, dst, landed)

    def send_home(chunk):
        for col in range(2):
            here, remote, local = home_copies(chunk, col)
            pl.when(here)(local.start)
            pl.when(jnp.logical_not(here))(remote.start)

    def ready(half, parity):
        if parity:
            send_home(2 * half)
        else:
            pl.when(half > 0)(lambda: send_home(2 * half - 1))

    def finish_second(chunk, total):
        new = (rows_of(a_ref, chunk, 1).astype(F32) + total).astype(BF16)
        res_ref[pl.ds(chunk * CHUNK_ROWS, CHUNK_ROWS)] = new.reshape(CHUNK_ROWS, cols, channels)

    conv_loop(in_order, ready, lambda u_ref, chunk: fill_chunk(u_ref, h_ref, chunk, second, top_edge, bottom_edge),
              finish_second, u_even, u_odd, w_vmem.at[1])
    send_home(jnp.int32(CHUNKS - 1))
    for chunk in range(CHUNKS):
        for col in range(2):
            here, remote, _ = home_copies(jnp.int32(chunk), col)
            pl.when(jnp.logical_not(here))(remote.wait_send)
    for slot in range(4):
        for part in range(per_tile):
            landed = out_ref.at[slot, pl.ds(part * CHUNK_ROWS, CHUNK_ROWS)]
            pltpu.make_async_copy(landed, landed, tile_rsem.at[slot, part]).wait()


def attention_kernel(norm_idx, count, logit_scale, a_hbm, stat_in, scale_ref, shift_ref, w_hbm, wo_hbm,
                     out_ref, stat_ref, a_ref, n_ref, q_ref, k_ref, v_ref, s_even, s_odd, peak_ref, total_ref, part_ref, o_ref,
                     wq_ref, wk_ref, wv_ref, wo_ref, acc_ref,
                     st_send, st_recv, load_sem, st_ssem, st_rsem, kv_ssem, kv_rsem):
    tokens, channels = a_ref.shape
    heads, head_dim, _ = v_ref.shape
    pairs = ((a_hbm, a_ref), (w_hbm.at[1], wk_ref), (w_hbm.at[2], wv_ref), (w_hbm.at[0], wq_ref), (wo_hbm, wo_ref))
    loads = [pltpu.make_async_copy(src, dst, load_sem.at[i]) for i, (src, dst) in enumerate(pairs)]
    for load in loads:
        load.start()

    def clear_padding():
        for head in range(heads):
            k_ref[head, 0:tokens, head_dim:] = jnp.zeros((tokens, LANES - head_dim), BF16)
            q_ref[head, head_dim:] = jnp.zeros((LANES - head_dim, tokens), BF16)

    st_send[0] = stat_in[...]
    barrier_pair()
    sums = exchange(0, st_send, st_recv, st_ssem, st_rsem, clear_padding)
    mean, inv_std = norm_params(sums, count)
    gain = inv_std * scale_ref[norm_idx:norm_idx + 1].astype(F32)
    shift = shift_ref[norm_idx:norm_idx + 1].astype(F32)
    for load in loads[:3]:
        load.wait()

    step = TOKEN_BLOCK
    chunks = tokens // step
    transposed = (((1,), (1,)), ((), ()))

    def head_copy(which, head, chunk=None):
        first, size = (0, tokens) if chunk is None else (pl.multiple_of(chunk * step, step), step)
        src, dst = pl.ds(first, size), pl.ds(tokens + first, size)
        if which:
            src_ref, dst_ref = v_ref.at[head, :, src], v_ref.at[head, :, dst]
        else:
            src_ref, dst_ref = k_ref.at[head, src], k_ref.at[head, dst]
        slot = head if chunk is None else heads + chunk
        return pltpu.make_async_remote_copy(
            src_ref=src_ref, dst_ref=dst_ref, send_sem=kv_ssem.at[which, slot], recv_sem=kv_rsem.at[which, slot],
            device_id=partner_id(), device_id_type=MESH)

    def both(act, head, chunk=None):
        for which in range(2):
            getattr(head_copy(which, head, chunk), act)()

    def key_values(i, carry):
        here = pl.ds(pl.multiple_of(i * step, step), step)
        normed = ((a_ref[here].astype(F32) - mean) * gain + shift).astype(BF16)
        n_ref[here] = normed
        part = lax.dot_general(normed, wk_ref[...], transposed, preferred_element_type=F32).astype(BF16)
        for head in range(heads):
            k_ref[head, here, 0:head_dim] = part[:, head * head_dim:(head + 1) * head_dim]
        part = lax.dot_general(wv_ref[...], normed, transposed, preferred_element_type=F32).astype(BF16)
        for head in range(heads):
            v_ref[head, :, here] = part[head * head_dim:(head + 1) * head_dim]

        @pl.when(i > 0)
        def _():
            both("start", 0, i - 1)
        return carry

    lax.fori_loop(0, chunks, key_values, 0)
    loads[3].wait()

    def query_chunk(i):
        here = pl.ds(pl.multiple_of(i * step, step), step)
        part = lax.dot_general(wq_ref[...], n_ref[here], transposed, preferred_element_type=F32).astype(BF16)
        for head in range(heads):
            q_ref[head, 0:head_dim, here] = part[head * head_dim:(head + 1) * head_dim]

    def queries(i, carry):
        query_chunk(2 * i)
        query_chunk(2 * i + 1)

        @pl.when(i == 0)
        def _():
            both("start", 0, chunks - 1)
            for head in range(1, heads):
                both("start", head)
        return carry

    lax.fori_loop(0, chunks // 2, queries, 0)

    for i in range(chunks):
        both("wait_recv", 0, i)

    blocks = tokens // QUERY_BLOCK
    key_blocks = 2 * tokens // KEY_BLOCK

    def fold(value, combine):
        return combine(value.reshape(KEY_BLOCK // 8, 8, QUERY_BLOCK), axis=0)

    def place_of(block):
        first = pl.multiple_of(lax.rem(block, blocks) * QUERY_BLOCK, QUERY_BLOCK)
        return lax.div(block, blocks), pl.ds(first, QUERY_BLOCK)

    def keys_of(j):
        return slice(j * KEY_BLOCK, (j + 1) * KEY_BLOCK)

    def score(j, head, query, s_ref, peak):
        scores = jnp.dot(k_ref[head, keys_of(j)], query, preferred_element_type=F32)
        s_ref[keys_of(j)] = scores
        piece = fold(scores, jnp.max)
        return piece if peak is None else jnp.maximum(peak, piece)

    def absorb(j, head, peak, s_ref, state):
        weights = jnp.exp2((s_ref[keys_of(j)] - peak) * logit_scale)
        total = fold(weights, jnp.sum)
        attended = jnp.dot(v_ref[head, :, keys_of(j)], weights.astype(BF16), preferred_element_type=F32)
        return (total, attended) if state is None else (state[0] + total, state[1] + attended)

    def finish_block(block, peak, s_ref, state):
        head, here = place_of(block)
        total, attended = absorb(key_blocks - 1, head, peak, s_ref, state)
        total = jnp.sum(total, axis=0, keepdims=True)
        o_ref[pl.ds(pl.multiple_of(head * head_dim, 16), head_dim), here] = (attended / total).astype(BF16)

    def peak_of(slot):
        return jnp.max(peak_ref[slot], axis=0, keepdims=True)

    def advance(i, s_ref, s_next, slot, state):
        head, _ = place_of(i)
        next_head, next_here = place_of(jnp.minimum(i + 1, heads * blocks - 1))
        query = q_ref[next_head, :, next_here]
        peak, next_peak, new_state = peak_of(slot), None, None
        for j in range(key_blocks):
            next_peak = score(j, next_head, query, s_next, next_peak)
            if j == 0:
                finish_block(jnp.maximum(i - 1, 0), peak_of(1 - slot), s_next, state)
            if j:
                new_state = absorb(j - 1, head, peak, s_ref, new_state)
        peak_ref[1 - slot] = next_peak
        return new_state

    s_odd[keys_of(key_blocks - 1)] = jnp.zeros((KEY_BLOCK, QUERY_BLOCK), F32)
    peak_ref[1] = jnp.zeros((8, QUERY_BLOCK), F32)
    total_ref[...] = jnp.zeros_like(total_ref)
    part_ref[...] = jnp.zeros_like(part_ref)
    query = q_ref[0, :, 0:QUERY_BLOCK]
    first_peak = None
    for j in range(key_blocks):
        first_peak = score(j, 0, query, s_even, first_peak)
    peak_ref[0] = first_peak

    def attend(head, carry):
        pl.when(head + 1 < heads)(lambda: both("wait_recv", head + 1))
        state = (total_ref[...], part_ref[...])
        for j in range(0, blocks, 2):
            state = advance(blocks * head + j, s_even, s_odd, 0, state)
            state = advance(blocks * head + j + 1, s_odd, s_even, 1, state)
        total_ref[...], part_ref[...] = state
        return carry

    lax.fori_loop(0, heads, attend, 0)
    finish_block(jnp.int32(heads * blocks - 1), peak_of(1), s_odd, (total_ref[...], part_ref[...]))
    for i in range(chunks):
        both("wait_send", 0, i)
    for head in range(1, heads):
        both("wait_send", head)
    loads[4].wait()
    acc_ref[...] = jnp.zeros_like(acc_ref)

    def project_chunk(i):
        here = pl.ds(pl.multiple_of(i * step, step), step)
        added = lax.dot_general(o_ref[:, here], wo_ref[...], (((0,), (0,)), ((), ())), preferred_element_type=F32)
        new = (a_ref[here].astype(F32) + added).astype(BF16)
        a_ref[here] = new
        add_moments(acc_ref, new.astype(F32))

    def leave(i):
        here = pl.ds(pl.multiple_of(i * 2 * step, 2 * step), 2 * step)
        return pltpu.make_async_copy(a_ref.at[here], out_ref.at[here], load_sem.at[i])

    def project(i, carry):
        pl.when(i > 0)(lambda: leave(i - 1).start())
        project_chunk(2 * i)
        project_chunk(2 * i + 1)
        return carry

    lax.fori_loop(0, chunks // 2, project, 0)
    stat_ref[...] = moment_rows(acc_ref)
    leave(chunks // 2 - 1).start()
    for i in range(chunks // 2):
        leave(i).wait()


VMEM_SPEC = pl.BlockSpec(memory_space=pltpu.VMEM)
ANY_SPEC = pl.BlockSpec(memory_space=pl.ANY)


def params(collective_id):
    return pltpu.CompilerParams(collective_id=collective_id, has_side_effects=True, vmem_limit_bytes=60 * 2**20)


def conv_scratch(rows, cols, channels):
    return [
        pltpu.VMEM((rows + 2, cols, channels), BF16),
        pltpu.VMEM((rows + 2, cols, channels), BF16),
        pltpu.VMEM((CHUNK_ROWS + 2, cols, 3 * channels), BF16),
        pltpu.VMEM((CHUNK_ROWS + 2, cols, 3 * channels), BF16),
        pltpu.VMEM((2, 9 * channels, channels), BF16),
    ]


def first_call(count, rows, cols, x, time_emb, scale, shift, w, time_w):
    channels = x.shape[3]
    dma = pltpu.SemaphoreType.DMA
    return pl.pallas_call(
        functools.partial(first_kernel, count),
        out_shape=[
            jax.ShapeDtypeStruct((rows, cols, channels), BF16),
            jax.ShapeDtypeStruct((8, channels), F32),
            jax.ShapeDtypeStruct((8, channels), F32),
        ],
        in_specs=[ANY_SPEC, VMEM_SPEC, VMEM_SPEC, VMEM_SPEC, ANY_SPEC, ANY_SPEC],
        out_specs=[VMEM_SPEC, VMEM_SPEC, VMEM_SPEC],
        scratch_shapes=[pltpu.VMEM(x.shape, BF16)] + conv_scratch(rows, cols, channels) + [
            pltpu.VMEM(time_w.shape, BF16),
            pltpu.VMEM((2, 8, channels), F32),
            pltpu.VMEM((2, 8, channels), F32),
            pltpu.VMEM((8, 8, LANES), F32),
            pltpu.VMEM((8, LANES), F32),
            pltpu.VMEM((1, 8, channels), F32),
            pltpu.VMEM((1, 8, channels), F32),
            dma((4,)), dma((7,)), dma((8,)), dma((1,)), dma((1,)), dma, dma,
            dma((4, len(PIECES))), dma((len(PIECES), 4)), dma((4,)), dma((2,)),
        ],
        compiler_params=params(0),
        name="res_first",
    )(x, time_emb, scale, shift, w, time_w)


def second_call(count, tile_shape, a, stats, time_vec, scale, shift, w):
    rows, cols, channels = a.shape
    dma = pltpu.SemaphoreType.DMA
    return pl.pallas_call(
        functools.partial(second_kernel, count),
        out_shape=jax.ShapeDtypeStruct(tile_shape, BF16),
        in_specs=[ANY_SPEC, VMEM_SPEC, VMEM_SPEC, VMEM_SPEC, VMEM_SPEC, ANY_SPEC],
        out_specs=ANY_SPEC,
        scratch_shapes=conv_scratch(rows, cols, channels) + [
            pltpu.VMEM((2, 8, channels), F32),
            pltpu.VMEM((rows, cols, channels), BF16),
            pltpu.VMEM((2, 8, channels), F32),
            pltpu.VMEM((2, 8, channels), F32),
            dma((3,)), dma((2,)), dma((2,)), dma((2,)), dma((2,)), dma((CHUNKS, 2)), dma((4, CHUNKS // 2)),
        ],
        compiler_params=params(2),
        name="res_second",
    )(a, stats, time_vec, scale, shift, w)


def copy_kernel(src_ref, out_ref, buf_ref, in_sem, out_sem):
    parts = [(i, slice(j * 8, (j + 1) * 8)) for i in range(src_ref.shape[0]) for j in range(src_ref.shape[1] // 8)]
    reads = [pltpu.make_async_copy(src_ref.at[i, rows], buf_ref.at[i, rows], in_sem.at[n]) for n, (i, rows) in enumerate(parts)]
    writes = [pltpu.make_async_copy(buf_ref.at[i, rows], out_ref.at[i, rows], out_sem.at[n]) for n, (i, rows) in enumerate(parts)]
    for read in reads:
        read.start()
    for read, write in zip(reads, writes):
        read.wait()
        write.start()
    for write in writes:
        write.wait()


def copy_call(src):
    parts = src.shape[0] * (src.shape[1] // 8)
    return pl.pallas_call(
        copy_kernel,
        out_shape=jax.ShapeDtypeStruct(src.shape, src.dtype),
        in_specs=[ANY_SPEC],
        out_specs=ANY_SPEC,
        scratch_shapes=[pltpu.VMEM(src.shape, src.dtype), pltpu.SemaphoreType.DMA((parts,)), pltpu.SemaphoreType.DMA((parts,))],
        name="copy_out",
    )(src)


def attention_call(norm_idx, count, heads, a, stats, scale, shift, w, wo):
    tokens, channels = a.shape
    head_dim = channels // heads
    logit_scale = head_dim ** -0.5 * 1.4426950408889634
    return pl.pallas_call(
        functools.partial(attention_kernel, norm_idx, count, logit_scale),
        out_shape=[jax.ShapeDtypeStruct((tokens, channels), BF16), jax.ShapeDtypeStruct((8, channels), F32)],
        in_specs=[ANY_SPEC, VMEM_SPEC, VMEM_SPEC, VMEM_SPEC, ANY_SPEC, ANY_SPEC],
        out_specs=[ANY_SPEC, VMEM_SPEC],
        scratch_shapes=[
            pltpu.VMEM((tokens, channels), BF16),
            pltpu.VMEM((tokens, channels), BF16),
            pltpu.VMEM((heads, LANES, tokens), BF16),
            pltpu.VMEM((heads, 2 * tokens, LANES), BF16),
            pltpu.VMEM((heads, head_dim, 2 * tokens), BF16),
            pltpu.VMEM((2 * tokens, QUERY_BLOCK), F32),
            pltpu.VMEM((2 * tokens, QUERY_BLOCK), F32),
            pltpu.VMEM((2, 8, QUERY_BLOCK), F32),
            pltpu.VMEM((8, QUERY_BLOCK), F32),
            pltpu.VMEM((head_dim, QUERY_BLOCK), F32),
            pltpu.VMEM((channels, tokens), BF16),
            pltpu.VMEM((channels, channels), BF16),
            pltpu.VMEM((channels, channels), BF16),
            pltpu.VMEM((channels, channels), BF16),
            pltpu.VMEM((channels, channels), BF16),
            pltpu.VMEM((2, 8, channels), F32),
            pltpu.VMEM((1, 8, channels), F32),
            pltpu.VMEM((1, 8, channels), F32),
            pltpu.SemaphoreType.DMA((5,)),
            pltpu.SemaphoreType.DMA((1,)),
            pltpu.SemaphoreType.DMA((1,)),
            pltpu.SemaphoreType.DMA((2, heads + tokens // TOKEN_BLOCK)),
            pltpu.SemaphoreType.DMA((2, heads + tokens // TOKEN_BLOCK)),
        ],
        compiler_params=params(1),
        name="attention",
    )(a, stats, scale, shift, w, wo)


def solution(mesh):
    lat_spec = P("dp", "sp", "sp2", None)

    def local(x, time_emb, gn_scale, gn_shift, conv_w, time_w, w_qkv, w_out):
        images, tile_rows, tile_cols, channels = x.shape
        rows, cols = 2 * tile_rows, 2 * tile_cols
        count = 2 * rows * cols * (channels // GROUPS)
        heads = w_out.shape[0]
        w = conv_w.reshape(4, 9 * channels, channels)
        qkv = jnp.transpose(w_qkv, (0, 2, 3, 1)).reshape(3, channels, channels)
        wo = w_out.reshape(channels, channels)
        first, stats, time_vec = first_call(count, rows, cols, x, time_emb, gn_scale, gn_shift, w, time_w)
        middle, stats = attention_call(2, count, heads, first.reshape(rows * cols, channels), stats, gn_scale, gn_shift, qkv, wo)
        return copy_call(second_call(count, x.shape, middle.reshape(rows, cols, channels), stats, time_vec, gn_scale, gn_shift, w))

    return jax.shard_map(local, mesh=mesh, in_specs=(lat_spec, P("dp", None), P(), P(), P(), P(), P(), P()), out_specs=lat_spec, check_vma=False)
```

```python
import functools

import jax
import jax.numpy as jnp
from jax import lax
from jax.experimental import pallas as pl
from jax.experimental.pallas import tpu as pltpu
from jax.sharding import PartitionSpec as P

GROUPS = 32
NORM_EPS = 1e-5
LANES = 128
CHUNK_ROWS = 4
CHUNKS = 8
PIECES = ((0, 5), (5, 4), (9, 4), (13, 3))
QUERY_BLOCK = 512
KEY_BLOCK = 512
TOKEN_BLOCK = 512
MESH = pl.DeviceIdType.MESH
F32 = jnp.float32
BF16 = jnp.bfloat16


def position():
    sp = lax.axis_index("sp")
    return lax.div(sp, 2), lax.rem(sp, 2), lax.axis_index("sp2")


def partner_id():
    chip_x, core, _ = position()
    return {"sp": 2 * chip_x + 1 - core}


def barrier_pair():
    sem = pltpu.get_barrier_semaphore()
    pl.semaphore_signal(sem, inc=1, device_id=partner_id(), device_id_type=MESH)
    pl.semaphore_wait(sem, 1)


def others():
    sp, col = lax.axis_index("sp"), lax.axis_index("sp2")
    return [(lax.rem(sp + i, 4), lax.rem(col + j, 2)) for i in range(4) for j in range(2) if i or j]


def signal_all():
    for sp, col in others():
        pl.semaphore_signal(pltpu.get_barrier_semaphore(), inc=1, device_id={"sp": sp, "sp2": col}, device_id_type=MESH)


def wait_all():
    pl.semaphore_wait(pltpu.get_barrier_semaphore(), 7)


def split3(value):
    high = value.astype(BF16).astype(F32)
    rest = value - high
    mid = rest.astype(BF16).astype(F32)
    low = rest - mid
    return jnp.concatenate([high, mid, low, jnp.zeros_like(value)], axis=0).astype(BF16)


def exact_dot(value, one_hot):
    out = jnp.dot(split3(value), one_hot, preferred_element_type=F32)
    return out[0:8] + out[8:16] + out[16:24]


def group_matrices(channels):
    width = channels // GROUPS
    chan = lax.broadcasted_iota(jnp.int32, (channels, LANES), 0)
    grp = lax.broadcasted_iota(jnp.int32, (channels, LANES), 1) * width
    gather = jnp.where((chan >= grp) & (chan < grp + width), 1.0, 0.0).astype(BF16)
    chan_t = lax.broadcasted_iota(jnp.int32, (LANES, channels), 1)
    grp_t = lax.broadcasted_iota(jnp.int32, (LANES, channels), 0) * width
    spread = jnp.where((chan_t >= grp_t) & (chan_t < grp_t + width), 1.0, 0.0).astype(BF16)
    return gather, spread


def spread_groups(group_sums, spread, count):
    mean = group_sums[0:1] / count
    inv_std = lax.rsqrt(group_sums[1:2] / count - mean * mean + NORM_EPS)
    stacked = jnp.concatenate([mean, inv_std, jnp.zeros((6, LANES), F32)], axis=0)
    per_channel = exact_dot(stacked, spread)
    return per_channel[0:1], per_channel[1:2]


def norm_params(sums, count):
    gather, spread = group_matrices(sums.shape[1])
    return spread_groups(exact_dot(sums, gather)[0:2], spread, count)


def fold_rows(value):
    rows, channels = value.shape
    return jnp.sum(value.reshape(rows // 8, 8, channels), axis=0)


def add_moments(acc_ref, value):
    acc_ref[0] += fold_rows(value)
    acc_ref[1] += fold_rows(value * value)


def moment_rows(acc_ref):
    total = jnp.sum(acc_ref[0], axis=0, keepdims=True)
    square = jnp.sum(acc_ref[1], axis=0, keepdims=True)
    return jnp.concatenate([total, square, jnp.zeros((6, total.shape[1]), F32)], axis=0)


def exchange(slot, send_ref, recv_ref, send_sem, recv_sem, meanwhile=None):
    copy = pltpu.make_async_remote_copy(
        src_ref=send_ref.at[slot],
        dst_ref=recv_ref.at[slot],
        send_sem=send_sem.at[slot],
        recv_sem=recv_sem.at[slot],
        device_id=partner_id(),
        device_id_type=MESH,
    )
    copy.start()
    if meanwhile is not None:
        meanwhile()
    copy.wait()
    return send_ref[slot] + recv_ref[slot]


def silu(value):
    half = 0.5 * value
    return half + half * jnp.tanh(half)


def fill_chunk(u_ref, src_ref, chunk, params, top_edge, bottom_edge):
    mean, gain, shift = params
    _, cols, channels = src_ref.shape
    place = lax.broadcasted_iota(jnp.int32, (cols, channels), 0)
    last = CHUNK_ROWS + 1
    for j in range(CHUNK_ROWS + 2):
        value = silu((src_ref[chunk * CHUNK_ROWS + j].astype(F32) - mean) * gain + shift)
        if j == 0:
            value = jnp.where(top_edge & (chunk == 0), 0.0, value)
        if j == last:
            value = jnp.where(bottom_edge & (chunk == CHUNKS - 1), 0.0, value)
        before = jnp.where(place == 0, 0.0, pltpu.roll(value, 1, 0))
        after = jnp.where(place == cols - 1, 0.0, pltpu.roll(value, cols - 1, 0))
        u_ref[j, :, 0:channels] = before.astype(BF16)
        u_ref[j, :, channels:2 * channels] = value.astype(BF16)
        u_ref[j, :, 2 * channels:3 * channels] = after.astype(BF16)


def conv_chunk(u_ref, w):
    _, cols, depth = u_ref.shape
    rows, split = CHUNK_ROWS * cols, w.shape[1] - LANES
    taps = [u_ref[dy:dy + CHUNK_ROWS].reshape(rows, depth) for dy in range(3)]
    main = jnp.dot(jnp.concatenate(taps, axis=1), w[:, 0:split], preferred_element_type=F32)
    both = jnp.concatenate([w[0:depth, split:], w[depth:2 * depth, split:]], axis=1)
    pair = jnp.dot(u_ref[0:CHUNK_ROWS + 1].reshape(rows + cols, depth), both, preferred_element_type=F32)
    third = jnp.dot(taps[2], w[2 * depth:, split:], preferred_element_type=F32)
    rest = pair[0:rows, 0:LANES] + pair[cols:, LANES:] + third
    return jnp.concatenate([main, rest], axis=1)


def conv_loop(order, ready, fill, finish, u_even, u_odd, w, arriving=False):
    def step(i, half, parity, u_now, u_next):
        after = jnp.minimum(i + 1, CHUNKS - 1)
        if arriving:
            finish(order(i), conv_chunk(u_now, w))
            ready(half, parity)
            fill(u_next, order(after))
        else:
            ready(half, parity)
            fill(u_next, order(after))
            finish(order(i), conv_chunk(u_now, w))

    def pair(half, carry):
        step(2 * half, half, 0, u_even, u_odd)
        step(2 * half + 1, half, 1, u_odd, u_even)
        return carry

    fill(u_even, order(jnp.int32(0)))
    lax.fori_loop(0, CHUNKS // 2, pair, 0)


def in_order(i):
    return i


def from_ends(i):
    return lax.rem(i + 1, 2) * lax.div(i, 2) + lax.rem(i, 2) * (CHUNKS - 1 - lax.div(i, 2))


def rows_of(ref, chunk, first=0):
    value = ref[pl.ds(chunk * CHUNK_ROWS + first, CHUNK_ROWS)]
    return value.reshape(value.shape[0] * value.shape[1], value.shape[2])


def send_edge_row(ref, send_sem, recv_sem, src_ref=None, src_row=None):
    rows = ref.shape[0] - 2
    core = position()[1]
    src = ref.at[rows - (rows - 1) * core] if src_ref is None else src_ref.at[src_row]
    return pltpu.make_async_remote_copy(
        src_ref=src, dst_ref=ref.at[(rows + 1) * core],
        send_sem=send_sem, recv_sem=recv_sem, device_id=partner_id(), device_id_type=MESH)


def first_kernel(count, x_ref, emb_ref, scale_ref, shift_ref, w_ref, tw_ref, out_ref, stat_ref, time_ref,
                 x_vmem, a_ref, h_ref, u_even, u_odd, w_vmem, tw_vmem, acc_ref, time_all, grp_recv, grp_total, st_send, st_recv,
                 load_sem, grp_ssem, grp_rsem, st_ssem, st_rsem, edge_ssem, edge_rsem, piece_ssem, piece_rsem, halo_ssem, halo_rsem):
    images, tile_rows, tile_cols, channels = x_ref.shape
    rows = 2 * tile_rows
    chip_x, core, chip_y = position()
    sp = lax.axis_index("sp")
    me = 2 * sp + chip_y
    image = 2 * chip_x + chip_y

    signal_all()
    x_load = pltpu.make_async_copy(x_ref, x_vmem, load_sem.at[0])
    x_load.start()
    weights = [pltpu.make_async_copy(w_ref.at[k], w_vmem.at[k], load_sem.at[1 + k]) for k in range(2)]
    tw_load = pltpu.make_async_copy(tw_ref, tw_vmem, load_sem.at[3])
    tw_load.start()

    def piece(part, source_core):
        low, high = PIECES[part]
        start = (1 - source_core) * low + source_core * (tile_rows - low - high)
        return pl.ds(start, high), pl.ds(1 + source_core * tile_rows + start, high)

    def piece_copies(k, part):
        to_x, to_y = lax.rem(chip_x + k // 2, 2), lax.rem(chip_y + k % 2, 2)
        src_rows, dst_rows = piece(part, core)
        src = x_ref.at[2 * to_x + to_y, src_rows]
        dst = a_ref.at[dst_rows, pl.ds(chip_y * tile_cols, tile_cols)]
        landed = piece_rsem.at[part, 2 * chip_y + core]
        remote = pltpu.make_async_remote_copy(
            src_ref=src, dst_ref=dst, send_sem=piece_ssem.at[k, part], recv_sem=landed,
            device_id={"sp": 2 * to_x + chip_x, "sp2": to_y}, device_id_type=MESH)
        return remote, pltpu.make_async_copy(src, dst, landed)

    def halo_copies(k):
        to_x, to_y = lax.rem(chip_x + k // 2, 2), lax.rem(chip_y + k % 2, 2)
        src = x_ref.at[2 * to_x + to_y, (tile_rows - 1) * core]
        dst = a_ref.at[(rows + 1) * chip_x, pl.ds(chip_y * tile_cols, tile_cols)]
        remote = pltpu.make_async_remote_copy(
            src_ref=src, dst_ref=dst, send_sem=halo_ssem.at[k], recv_sem=halo_rsem.at[chip_y],
            device_id={"sp": 2 * to_x + 1 - chip_x, "sp2": to_y}, device_id_type=MESH)
        return remote, pltpu.make_async_copy(src, dst, halo_rsem.at[chip_y])

    at_home = core == chip_x
    far_first = (3, 2, 1, 0)

    def send_piece(part):
        for k in far_first:
            remote, local = piece_copies(k, part)
            if k:
                remote.start()
            else:
                pl.when(at_home)(local.start)
                pl.when(jnp.logical_not(at_home))(remote.start)

    wait_all()

    @pl.when(jnp.logical_not(at_home))
    def _():
        for k in far_first:
            halo_copies(k)[0 if k else 1].start()

    send_piece(0)
    for copy in weights:
        copy.start()

    gather, spread = group_matrices(channels)
    x_load.wait()
    moments = []
    for i in range(images):
        acc_ref[...] = jnp.zeros_like(acc_ref)

        def add_row(row, carry):
            add_moments(acc_ref, x_vmem[i, row].astype(F32))
            return carry

        lax.fori_loop(0, tile_rows, add_row, 0)
        moments += [jnp.sum(acc_ref[0], axis=0, keepdims=True), jnp.sum(acc_ref[1], axis=0, keepdims=True)]
    grp_recv[me] = exact_dot(jnp.concatenate(moments, axis=0), gather)
    tw_load.wait()
    emb = silu(emb_ref[...].astype(F32)).astype(BF16)
    for k in range(2):
        time_all[k, 0:images] = jnp.dot(emb, tw_vmem[k], preferred_element_type=F32)
    time_ref[...] = jnp.broadcast_to(time_all[1, pl.ds(image, 1)], time_ref.shape)
    time_vec = time_all[0, pl.ds(image, 1)]

    group_copies = []
    for k, (to_sp, to_y) in enumerate(others()):
        copy = pltpu.make_async_remote_copy(
            src_ref=grp_recv.at[me], dst_ref=grp_recv.at[me], send_sem=grp_ssem.at[k], recv_sem=grp_rsem.at[me],
            device_id={"sp": to_sp, "sp2": to_y}, device_id_type=MESH)
        copy.start()
        group_copies.append((copy, 2 * to_sp + to_y))

    for part in range(1, len(PIECES)):
        send_piece(part)

    total = jnp.zeros((8, LANES), F32)
    for copy, _ in group_copies:
        copy.wait_send()
    for copy, sender in group_copies:
        pltpu.make_async_copy(grp_recv.at[sender], grp_recv.at[sender], grp_rsem.at[sender]).wait()
    for slot in range(8):
        total = total + grp_recv[slot]
    grp_total[...] = total
    mean, inv_std = spread_groups(grp_total[pl.ds(2 * image, 2)], spread, count)

    def wait_piece(part, source_core):
        for col in range(2):
            landed = a_ref.at[piece(part, source_core)[1], pl.ds(col * tile_cols, tile_cols)]
            pltpu.make_async_copy(landed, landed, piece_rsem.at[part, 2 * col + source_core]).wait()

    def ready(half, parity):
        if parity:
            for part in range(1, len(PIECES)):
                @pl.when(half + 1 == part)
                def _():
                    wait_piece(part, 0)
                    wait_piece(part, 1)

    top_edge, bottom_edge = core == 0, core == 1

    def norm(k, mean, inv_std):
        return mean, inv_std * scale_ref[k:k + 1].astype(F32), shift_ref[k:k + 1].astype(F32)

    params = norm(0, mean, inv_std)
    for col in range(2):
        landed = a_ref.at[(rows + 1) * (1 - core), pl.ds(col * tile_cols, tile_cols)]
        pltpu.make_async_copy(landed, landed, halo_rsem.at[col]).wait()
    wait_piece(0, 0)
    wait_piece(0, 1)
    acc_ref[...] = jnp.zeros_like(acc_ref)
    weights[0].wait()

    def finish_first(chunk, total):
        hidden = (total + time_vec).astype(BF16)
        h_ref[pl.ds(chunk * CHUNK_ROWS + 1, CHUNK_ROWS)] = hidden.reshape(CHUNK_ROWS, 2 * tile_cols, channels)
        add_moments(acc_ref, hidden.astype(F32))

    conv_loop(from_ends, ready, lambda u_ref, chunk: fill_chunk(u_ref, a_ref, chunk, params, top_edge, bottom_edge),
              finish_first, u_even, u_odd, w_vmem.at[0], arriving=True)

    edge = send_edge_row(h_ref, edge_ssem, edge_rsem)
    st_send[0] = moment_rows(acc_ref)
    edge.start()
    acc_ref[...] = jnp.zeros_like(acc_ref)
    weights[1].wait()
    second = norm(1, *norm_params(exchange(0, st_send, st_recv, st_ssem, st_rsem), count))
    edge.wait()

    def finish_second(chunk, total):
        new = (rows_of(a_ref, chunk, 1).astype(F32) + total).astype(BF16)
        out_ref[pl.ds(chunk * CHUNK_ROWS, CHUNK_ROWS)] = new.reshape(CHUNK_ROWS, 2 * tile_cols, channels)
        add_moments(acc_ref, new.astype(F32))

    conv_loop(in_order, lambda half, parity: None,
              lambda u_ref, chunk: fill_chunk(u_ref, h_ref, chunk, second, top_edge, bottom_edge),
              finish_second, u_even, u_odd, w_vmem.at[1])
    stat_ref[...] = moment_rows(acc_ref)

    @pl.when(jnp.logical_not(at_home))
    def _():
        for k in (1, 2, 3):
            halo_copies(k)[0].wait_send()

    for part in range(len(PIECES)):
        for k in range(4):
            remote, _ = piece_copies(k, part)
            if k:
                remote.wait_send()
            else:
                pl.when(jnp.logical_not(at_home))(remote.wait_send)


def second_kernel(count, a_hbm, stat_in, time_ref, scale_ref, shift_ref, w_ref, out_ref,
                  a_ref, h_ref, u_even, u_odd, w_vmem, acc_ref, res_ref, st_send, st_recv,
                  load_sem, st_ssem, st_rsem, edge_ssem, edge_rsem, tile_ssem, tile_rsem):
    rows, cols, channels = res_ref.shape
    tile_rows, tile_cols = rows // 2, cols // 2
    chip_x, core, chip_y = position()
    sp = lax.axis_index("sp")
    image = 2 * chip_x + chip_y

    signal_all()
    a_load = pltpu.make_async_copy(a_hbm, a_ref.at[pl.ds(1, rows)], load_sem.at[0])
    a_load.start()
    weights = [pltpu.make_async_copy(w_ref.at[2 + k], w_vmem.at[k], load_sem.at[1 + k]) for k in range(2)]
    for copy in weights:
        copy.start()
    st_send[0] = stat_in[...]
    acc_ref[...] = jnp.zeros_like(acc_ref)
    wait_all()
    edge = send_edge_row(a_ref, edge_ssem.at[0], edge_rsem.at[0], a_hbm, (rows - 1) * (1 - core))
    edge.start()
    top_edge, bottom_edge = core == 0, core == 1

    def norm(k, sums):
        mean, inv_std = norm_params(sums, count)
        return mean, inv_std * scale_ref[3 + k:4 + k].astype(F32), shift_ref[3 + k:4 + k].astype(F32)

    params = norm(0, exchange(0, st_send, st_recv, st_ssem, st_rsem))
    a_load.wait()
    edge.wait()
    weights[0].wait()
    time_vec = time_ref[0:1]

    def finish_first(chunk, total):
        hidden = (total + time_vec).astype(BF16)
        h_ref[pl.ds(chunk * CHUNK_ROWS + 1, CHUNK_ROWS)] = hidden.reshape(CHUNK_ROWS, cols, channels)
        add_moments(acc_ref, hidden.astype(F32))

    conv_loop(in_order, lambda half, parity: None,
              lambda u_ref, chunk: fill_chunk(u_ref, a_ref, chunk, params, top_edge, bottom_edge),
              finish_first, u_even, u_odd, w_vmem.at[0])

    edge = send_edge_row(h_ref, edge_ssem.at[1], edge_rsem.at[1])
    st_send[1] = moment_rows(acc_ref)
    edge.start()
    weights[1].wait()
    second = norm(1, exchange(1, st_send, st_recv, st_ssem, st_rsem))
    edge.wait()

    per_tile = CHUNKS // 2

    def home_copies(chunk, col):
        to_sp = 2 * core + lax.div(chunk, per_tile)
        slot = lax.rem(chunk, per_tile)
        here = (to_sp == sp) & (chip_y == col)
        src = res_ref.at[pl.ds(chunk * CHUNK_ROWS, CHUNK_ROWS), pl.ds(col * tile_cols, tile_cols)]
        dst = out_ref.at[image, pl.ds(slot * CHUNK_ROWS, CHUNK_ROWS)]
        landed = tile_rsem.at[image, slot]
        remote = pltpu.make_async_remote_copy(
            src_ref=src, dst_ref=dst, send_sem=tile_ssem.at[chunk, col], recv_sem=landed,
            device_id={"sp": to_sp, "sp2": col}, device_id_type=MESH)
        return here, remote, pltpu.make_async_copy(src, dst, landed)

    def send_home(chunk):
        for col in range(2):
            here, remote, local = home_copies(chunk, col)
            pl.when(here)(local.start)
            pl.when(jnp.logical_not(here))(remote.start)

    def ready(half, parity):
        if parity:
            send_home(2 * half)
        else:
            pl.when(half > 0)(lambda: send_home(2 * half - 1))

    def finish_second(chunk, total):
        new = (rows_of(a_ref, chunk, 1).astype(F32) + total).astype(BF16)
        res_ref[pl.ds(chunk * CHUNK_ROWS, CHUNK_ROWS)] = new.reshape(CHUNK_ROWS, cols, channels)

    conv_loop(in_order, ready, lambda u_ref, chunk: fill_chunk(u_ref, h_ref, chunk, second, top_edge, bottom_edge),
              finish_second, u_even, u_odd, w_vmem.at[1])
    send_home(jnp.int32(CHUNKS - 1))
    for chunk in range(CHUNKS):
        for col in range(2):
            here, remote, _ = home_copies(jnp.int32(chunk), col)
            pl.when(jnp.logical_not(here))(remote.wait_send)
    for slot in range(4):
        for part in range(per_tile):
            landed = out_ref.at[slot, pl.ds(part * CHUNK_ROWS, CHUNK_ROWS)]
            pltpu.make_async_copy(landed, landed, tile_rsem.at[slot, part]).wait()


def attention_kernel(norm_idx, count, logit_scale, a_hbm, stat_in, scale_ref, shift_ref, w_hbm, wo_hbm,
                     out_ref, stat_ref, a_ref, n_ref, q_ref, k_ref, v_ref, s_even, s_odd, peak_ref, total_ref, part_ref, o_ref,
                     wq_ref, wk_ref, wv_ref, wo_ref, acc_ref,
                     st_send, st_recv, load_sem, st_ssem, st_rsem, kv_ssem, kv_rsem):
    tokens, channels = a_ref.shape
    heads, head_dim, _ = v_ref.shape
    pairs = ((a_hbm, a_ref), (w_hbm.at[1], wk_ref), (w_hbm.at[2], wv_ref), (w_hbm.at[0], wq_ref), (wo_hbm, wo_ref))
    loads = [pltpu.make_async_copy(src, dst, load_sem.at[i]) for i, (src, dst) in enumerate(pairs)]
    for load in loads:
        load.start()

    def clear_padding():
        for head in range(heads):
            k_ref[head, 0:tokens, head_dim:] = jnp.zeros((tokens, LANES - head_dim), BF16)
            q_ref[head, head_dim:] = jnp.zeros((LANES - head_dim, tokens), BF16)

    st_send[0] = stat_in[...]
    barrier_pair()
    sums = exchange(0, st_send, st_recv, st_ssem, st_rsem, clear_padding)
    mean, inv_std = norm_params(sums, count)
    gain = inv_std * scale_ref[norm_idx:norm_idx + 1].astype(F32)
    shift = shift_ref[norm_idx:norm_idx + 1].astype(F32)
    for load in loads[:3]:
        load.wait()

    step = TOKEN_BLOCK
    chunks = tokens // step
    transposed = (((1,), (1,)), ((), ()))

    def head_copy(which, head, chunk=None):
        first, size = (0, tokens) if chunk is None else (pl.multiple_of(chunk * step, step), step)
        src, dst = pl.ds(first, size), pl.ds(tokens + first, size)
        if which:
            src_ref, dst_ref = v_ref.at[head, :, src], v_ref.at[head, :, dst]
        else:
            src_ref, dst_ref = k_ref.at[head, src], k_ref.at[head, dst]
        slot = head if chunk is None else heads + chunk
        return pltpu.make_async_remote_copy(
            src_ref=src_ref, dst_ref=dst_ref, send_sem=kv_ssem.at[which, slot], recv_sem=kv_rsem.at[which, slot],
            device_id=partner_id(), device_id_type=MESH)

    def both(act, head, chunk=None):
        for which in range(2):
            getattr(head_copy(which, head, chunk), act)()

    def key_values(i, carry):
        here = pl.ds(pl.multiple_of(i * step, step), step)
        normed = ((a_ref[here].astype(F32) - mean) * gain + shift).astype(BF16)
        n_ref[here] = normed
        part = lax.dot_general(normed, wk_ref[...], transposed, preferred_element_type=F32).astype(BF16)
        for head in range(heads):
            k_ref[head, here, 0:head_dim] = part[:, head * head_dim:(head + 1) * head_dim]
        part = lax.dot_general(wv_ref[...], normed, transposed, preferred_element_type=F32).astype(BF16)
        for head in range(heads):
            v_ref[head, :, here] = part[head * head_dim:(head + 1) * head_dim]

        @pl.when(i > 0)
        def _():
            both("start", 0, i - 1)
        return carry

    lax.fori_loop(0, chunks, key_values, 0)
    loads[3].wait()

    def query_chunk(i):
        here = pl.ds(pl.multiple_of(i * step, step), step)
        part = lax.dot_general(wq_ref[...], n_ref[here], transposed, preferred_element_type=F32).astype(BF16)
        for head in range(heads):
            q_ref[head, 0:head_dim, here] = part[head * head_dim:(head + 1) * head_dim]

    def queries(i, carry):
        query_chunk(2 * i)
        query_chunk(2 * i + 1)

        @pl.when(i == 0)
        def _():
            both("start", 0, chunks - 1)
            for head in range(1, heads):
                both("start", head)
        return carry

    lax.fori_loop(0, chunks // 2, queries, 0)

    for i in range(chunks):
        both("wait_recv", 0, i)

    blocks = tokens // QUERY_BLOCK
    key_blocks = 2 * tokens // KEY_BLOCK

    def fold(value, combine):
        return combine(value.reshape(KEY_BLOCK // 8, 8, QUERY_BLOCK), axis=0)

    def place_of(block):
        first = pl.multiple_of(lax.rem(block, blocks) * QUERY_BLOCK, QUERY_BLOCK)
        return lax.div(block, blocks), pl.ds(first, QUERY_BLOCK)

    def keys_of(j):
        return slice(j * KEY_BLOCK, (j + 1) * KEY_BLOCK)

    def score(j, head, query, s_ref, peak):
        scores = jnp.dot(k_ref[head, keys_of(j)], query, preferred_element_type=F32)
        s_ref[keys_of(j)] = scores
        piece = fold(scores, jnp.max)
        return piece if peak is None else jnp.maximum(peak, piece)

    def absorb(j, head, peak, s_ref, state):
        weights = jnp.exp2((s_ref[keys_of(j)] - peak) * logit_scale)
        total = fold(weights, jnp.sum)
        attended = jnp.dot(v_ref[head, :, keys_of(j)], weights.astype(BF16), preferred_element_type=F32)
        return (total, attended) if state is None else (state[0] + total, state[1] + attended)

    def finish_block(block, peak, s_ref, state):
        head, here = place_of(block)
        total, attended = absorb(key_blocks - 1, head, peak, s_ref, state)
        total = jnp.sum(total, axis=0, keepdims=True)
        o_ref[pl.ds(pl.multiple_of(head * head_dim, 16), head_dim), here] = (attended / total).astype(BF16)

    def peak_of(slot):
        return jnp.max(peak_ref[slot], axis=0, keepdims=True)

    def advance(i, s_ref, s_next, slot, state):
        head, _ = place_of(i)
        next_head, next_here = place_of(jnp.minimum(i + 1, heads * blocks - 1))
        query = q_ref[next_head, :, next_here]
        peak, next_peak, new_state = peak_of(slot), None, None
        for j in range(key_blocks):
            next_peak = score(j, next_head, query, s_next, next_peak)
            if j == 0:
                finish_block(jnp.maximum(i - 1, 0), peak_of(1 - slot), s_next, state)
            if j:
                new_state = absorb(j - 1, head, peak, s_ref, new_state)
        peak_ref[1 - slot] = next_peak
        return new_state

    s_odd[keys_of(key_blocks - 1)] = jnp.zeros((KEY_BLOCK, QUERY_BLOCK), F32)
    peak_ref[1] = jnp.zeros((8, QUERY_BLOCK), F32)
    total_ref[...] = jnp.zeros_like(total_ref)
    part_ref[...] = jnp.zeros_like(part_ref)
    query = q_ref[0, :, 0:QUERY_BLOCK]
    first_peak = None
    for j in range(key_blocks):
        first_peak = score(j, 0, query, s_even, first_peak)
    peak_ref[0] = first_peak

    def attend(head, carry):
        pl.when(head + 1 < heads)(lambda: both("wait_recv", head + 1))
        state = (total_ref[...], part_ref[...])
        for j in range(0, blocks, 2):
            state = advance(blocks * head + j, s_even, s_odd, 0, state)
            state = advance(blocks * head + j + 1, s_odd, s_even, 1, state)
        total_ref[...], part_ref[...] = state
        return carry

    lax.fori_loop(0, heads, attend, 0)
    finish_block(jnp.int32(heads * blocks - 1), peak_of(1), s_odd, (total_ref[...], part_ref[...]))
    for i in range(chunks):
        both("wait_send", 0, i)
    for head in range(1, heads):
        both("wait_send", head)
    loads[4].wait()
    acc_ref[...] = jnp.zeros_like(acc_ref)

    def project_chunk(i):
        here = pl.ds(pl.multiple_of(i * step, step), step)
        added = lax.dot_general(o_ref[:, here], wo_ref[...], (((0,), (0,)), ((), ())), preferred_element_type=F32)
        new = (a_ref[here].astype(F32) + added).astype(BF16)
        a_ref[here] = new
        add_moments(acc_ref, new.astype(F32))

    def leave(i):
        here = pl.ds(pl.multiple_of(i * 2 * step, 2 * step), 2 * step)
        return pltpu.make_async_copy(a_ref.at[here], out_ref.at[here], load_sem.at[i])

    def project(i, carry):
        pl.when(i > 0)(lambda: leave(i - 1).start())
        project_chunk(2 * i)
        project_chunk(2 * i + 1)
        return carry

    lax.fori_loop(0, chunks // 2, project, 0)
    stat_ref[...] = moment_rows(acc_ref)
    leave(chunks // 2 - 1).start()
    for i in range(chunks // 2):
        leave(i).wait()


VMEM_SPEC = pl.BlockSpec(memory_space=pltpu.VMEM)
ANY_SPEC = pl.BlockSpec(memory_space=pl.ANY)


def params(collective_id):
    return pltpu.CompilerParams(collective_id=collective_id, has_side_effects=True, vmem_limit_bytes=60 * 2**20)


def conv_scratch(rows, cols, channels):
    return [
        pltpu.VMEM((rows + 2, cols, channels), BF16),
        pltpu.VMEM((rows + 2, cols, channels), BF16),
        pltpu.VMEM((CHUNK_ROWS + 2, cols, 3 * channels), BF16),
        pltpu.VMEM((CHUNK_ROWS + 2, cols, 3 * channels), BF16),
        pltpu.VMEM((2, 9 * channels, channels), BF16),
    ]


def first_call(count, rows, cols, x, time_emb, scale, shift, w, time_w):
    channels = x.shape[3]
    dma = pltpu.SemaphoreType.DMA
    return pl.pallas_call(
        functools.partial(first_kernel, count),
        out_shape=[
            jax.ShapeDtypeStruct((rows, cols, channels), BF16),
            jax.ShapeDtypeStruct((8, channels), F32),
            jax.ShapeDtypeStruct((8, channels), F32),
        ],
        in_specs=[ANY_SPEC, VMEM_SPEC, VMEM_SPEC, VMEM_SPEC, ANY_SPEC, ANY_SPEC],
        out_specs=[VMEM_SPEC, VMEM_SPEC, VMEM_SPEC],
        scratch_shapes=[pltpu.VMEM(x.shape, BF16)] + conv_scratch(rows, cols, channels) + [
            pltpu.VMEM(time_w.shape, BF16),
            pltpu.VMEM((2, 8, channels), F32),
            pltpu.VMEM((2, 8, channels), F32),
            pltpu.VMEM((8, 8, LANES), F32),
            pltpu.VMEM((8, LANES), F32),
            pltpu.VMEM((1, 8, channels), F32),
            pltpu.VMEM((1, 8, channels), F32),
            dma((4,)), dma((7,)), dma((8,)), dma((1,)), dma((1,)), dma, dma,
            dma((4, len(PIECES))), dma((len(PIECES), 4)), dma((4,)), dma((2,)),
        ],
        compiler_params=params(0),
        name="res_first",
    )(x, time_emb, scale, shift, w, time_w)


def second_call(count, tile_shape, a, stats, time_vec, scale, shift, w):
    rows, cols, channels = a.shape
    dma = pltpu.SemaphoreType.DMA
    return pl.pallas_call(
        functools.partial(second_kernel, count),
        out_shape=jax.ShapeDtypeStruct(tile_shape, BF16),
        in_specs=[ANY_SPEC, VMEM_SPEC, VMEM_SPEC, VMEM_SPEC, VMEM_SPEC, ANY_SPEC],
        out_specs=ANY_SPEC,
        scratch_shapes=conv_scratch(rows, cols, channels) + [
            pltpu.VMEM((2, 8, channels), F32),
            pltpu.VMEM((rows, cols, channels), BF16),
            pltpu.VMEM((2, 8, channels), F32),
            pltpu.VMEM((2, 8, channels), F32),
            dma((3,)), dma((2,)), dma((2,)), dma((2,)), dma((2,)), dma((CHUNKS, 2)), dma((4, CHUNKS // 2)),
        ],
        compiler_params=params(2),
        name="res_second",
    )(a, stats, time_vec, scale, shift, w)


def copy_kernel(src_ref, out_ref, buf_ref, in_sem, out_sem):
    parts = [(i, slice(j * 8, (j + 1) * 8)) for i in range(src_ref.shape[0]) for j in range(src_ref.shape[1] // 8)]
    reads = [pltpu.make_async_copy(src_ref.at[i, rows], buf_ref.at[i, rows], in_sem.at[n]) for n, (i, rows) in enumerate(parts)]
    writes = [pltpu.make_async_copy(buf_ref.at[i, rows], out_ref.at[i, rows], out_sem.at[n]) for n, (i, rows) in enumerate(parts)]
    for read in reads:
        read.start()
    for read, write in zip(reads, writes):
        read.wait()
        write.start()
    for write in writes:
        write.wait()


def copy_call(src):
    parts = src.shape[0] * (src.shape[1] // 8)
    return pl.pallas_call(
        copy_kernel,
        out_shape=jax.ShapeDtypeStruct(src.shape, src.dtype),
        in_specs=[ANY_SPEC],
        out_specs=ANY_SPEC,
        scratch_shapes=[pltpu.VMEM(src.shape, src.dtype), pltpu.SemaphoreType.DMA((parts,)), pltpu.SemaphoreType.DMA((parts,))],
        name="copy_out",
    )(src)


def attention_call(norm_idx, count, heads, a, stats, scale, shift, w, wo):
    tokens, channels = a.shape
    head_dim = channels // heads
    logit_scale = head_dim ** -0.5 * 1.4426950408889634
    return pl.pallas_call(
        functools.partial(attention_kernel, norm_idx, count, logit_scale),
        out_shape=[jax.ShapeDtypeStruct((tokens, channels), BF16), jax.ShapeDtypeStruct((8, channels), F32)],
        in_specs=[ANY_SPEC, VMEM_SPEC, VMEM_SPEC, VMEM_SPEC, ANY_SPEC, ANY_SPEC],
        out_specs=[ANY_SPEC, VMEM_SPEC],
        scratch_shapes=[
            pltpu.VMEM((tokens, channels), BF16),
            pltpu.VMEM((tokens, channels), BF16),
            pltpu.VMEM((heads, LANES, tokens), BF16),
            pltpu.VMEM((heads, 2 * tokens, LANES), BF16),
            pltpu.VMEM((heads, head_dim, 2 * tokens), BF16),
            pltpu.VMEM((2 * tokens, QUERY_BLOCK), F32),
            pltpu.VMEM((2 * tokens, QUERY_BLOCK), F32),
            pltpu.VMEM((2, 8, QUERY_BLOCK), F32),
            pltpu.VMEM((8, QUERY_BLOCK), F32),
            pltpu.VMEM((head_dim, QUERY_BLOCK), F32),
            pltpu.VMEM((channels, tokens), BF16),
            pltpu.VMEM((channels, channels), BF16),
            pltpu.VMEM((channels, channels), BF16),
            pltpu.VMEM((channels, channels), BF16),
            pltpu.VMEM((channels, channels), BF16),
            pltpu.VMEM((2, 8, channels), F32),
            pltpu.VMEM((1, 8, channels), F32),
            pltpu.VMEM((1, 8, channels), F32),
            pltpu.SemaphoreType.DMA((5,)),
            pltpu.SemaphoreType.DMA((1,)),
            pltpu.SemaphoreType.DMA((1,)),
            pltpu.SemaphoreType.DMA((2, heads + tokens // TOKEN_BLOCK)),
            pltpu.SemaphoreType.DMA((2, heads + tokens // TOKEN_BLOCK)),
        ],
        compiler_params=params(1),
        name="attention",
    )(a, stats, scale, shift, w, wo)


def solution(mesh):
    lat_spec = P("dp", "sp", "sp2", None)

    def local(x, time_emb, gn_scale, gn_shift, conv_w, time_w, w_qkv, w_out):
        images, tile_rows, tile_cols, channels = x.shape
        rows, cols = 2 * tile_rows, 2 * tile_cols
        count = 2 * rows * cols * (channels // GROUPS)
        heads = w_out.shape[0]
        w = conv_w.reshape(4, 9 * channels, channels)
        qkv = jnp.transpose(w_qkv, (0, 2, 3, 1)).reshape(3, channels, channels)
        wo = w_out.reshape(channels, channels)
        first, stats, time_vec = first_call(count, rows, cols, x, time_emb, gn_scale, gn_shift, w, time_w)
        middle, stats = attention_call(2, count, heads, first.reshape(rows * cols, channels), stats, gn_scale, gn_shift, qkv, wo)
        return copy_call(second_call(count, x.shape, middle.reshape(rows, cols, channels), stats, time_vec, gn_scale, gn_shift, w))

    return jax.shard_map(local, mesh=mesh, in_specs=(lat_spec, P("dp", None), P(), P(), P(), P(), P(), P()), out_specs=lat_spec, check_vma=False)
```

```python
import functools

import jax
import jax.numpy as jnp
from jax import lax
from jax.experimental import pallas as pl
from jax.experimental.pallas import tpu as pltpu
from jax.sharding import PartitionSpec as P

GROUPS = 32
NORM_EPS = 1e-5
LANES = 128
CHUNK_ROWS = 4
CHUNKS = 8
PIECES = ((0, 5), (5, 4), (9, 4), (13, 3))
QUERY_BLOCK = 512
KEY_BLOCK = 512
TOKEN_BLOCK = 512
MESH = pl.DeviceIdType.MESH
F32 = jnp.float32
BF16 = jnp.bfloat16


def position():
    sp = lax.axis_index("sp")
    return lax.div(sp, 2), lax.rem(sp, 2), lax.axis_index("sp2")


def partner_id():
    chip_x, core, _ = position()
    return {"sp": 2 * chip_x + 1 - core}


def barrier_pair():
    sem = pltpu.get_barrier_semaphore()
    pl.semaphore_signal(sem, inc=1, device_id=partner_id(), device_id_type=MESH)
    pl.semaphore_wait(sem, 1)


def others():
    sp, col = lax.axis_index("sp"), lax.axis_index("sp2")
    return [(lax.rem(sp + i, 4), lax.rem(col + j, 2)) for i in range(4) for j in range(2) if i or j]


def signal_all():
    for sp, col in others():
        pl.semaphore_signal(pltpu.get_barrier_semaphore(), inc=1, device_id={"sp": sp, "sp2": col}, device_id_type=MESH)


def wait_all():
    pl.semaphore_wait(pltpu.get_barrier_semaphore(), 7)


def split3(value):
    high = value.astype(BF16).astype(F32)
    rest = value - high
    mid = rest.astype(BF16).astype(F32)
    low = rest - mid
    return jnp.concatenate([high, mid, low, jnp.zeros_like(value)], axis=0).astype(BF16)


def exact_dot(value, one_hot):
    out = jnp.dot(split3(value), one_hot, preferred_element_type=F32)
    return out[0:8] + out[8:16] + out[16:24]


def group_matrices(channels):
    width = channels // GROUPS
    chan = lax.broadcasted_iota(jnp.int32, (channels, LANES), 0)
    grp = lax.broadcasted_iota(jnp.int32, (channels, LANES), 1) * width
    gather = jnp.where((chan >= grp) & (chan < grp + width), 1.0, 0.0).astype(BF16)
    chan_t = lax.broadcasted_iota(jnp.int32, (LANES, channels), 1)
    grp_t = lax.broadcasted_iota(jnp.int32, (LANES, channels), 0) * width
    spread = jnp.where((chan_t >= grp_t) & (chan_t < grp_t + width), 1.0, 0.0).astype(BF16)
    return gather, spread


def spread_groups(group_sums, spread, count):
    mean = group_sums[0:1] / count
    inv_std = lax.rsqrt(group_sums[1:2] / count - mean * mean + NORM_EPS)
    stacked = jnp.concatenate([mean, inv_std, jnp.zeros((6, LANES), F32)], axis=0)
    per_channel = exact_dot(stacked, spread)
    return per_channel[0:1], per_channel[1:2]


def norm_params(sums, count):
    gather, spread = group_matrices(sums.shape[1])
    return spread_groups(exact_dot(sums, gather)[0:2], spread, count)


def fold_rows(value):
    rows, channels = value.shape
    return jnp.sum(value.reshape(rows // 8, 8, channels), axis=0)


def add_moments(acc_ref, value):
    acc_ref[0] += fold_rows(value)
    acc_ref[1] += fold_rows(value * value)


def moment_rows(acc_ref):
    total = jnp.sum(acc_ref[0], axis=0, keepdims=True)
    square = jnp.sum(acc_ref[1], axis=0, keepdims=True)
    return jnp.concatenate([total, square, jnp.zeros((6, total.shape[1]), F32)], axis=0)


def exchange(slot, send_ref, recv_ref, send_sem, recv_sem, meanwhile=None):
    copy = pltpu.make_async_remote_copy(
        src_ref=send_ref.at[slot],
        dst_ref=recv_ref.at[slot],
        send_sem=send_sem.at[slot],
        recv_sem=recv_sem.at[slot],
        device_id=partner_id(),
        device_id_type=MESH,
    )
    copy.start()
    if meanwhile is not None:
        meanwhile()
    copy.wait()
    return send_ref[slot] + recv_ref[slot]


def silu(value):
    half = 0.5 * value
    return half + half * jnp.tanh(half)


def fill_chunk(u_ref, src_ref, chunk, params, top_edge, bottom_edge):
    mean, gain, shift = params
    _, cols, channels = src_ref.shape
    place = lax.broadcasted_iota(jnp.int32, (cols, channels), 0)
    last = CHUNK_ROWS + 1
    for j in range(CHUNK_ROWS + 2):
        value = silu((src_ref[chunk * CHUNK_ROWS + j].astype(F32) - mean) * gain + shift)
        if j == 0:
            value = jnp.where(top_edge & (chunk == 0), 0.0, value)
        if j == last:
            value = jnp.where(bottom_edge & (chunk == CHUNKS - 1), 0.0, value)
        before = jnp.where(place == 0, 0.0, pltpu.roll(value, 1, 0))
        after = jnp.where(place == cols - 1, 0.0, pltpu.roll(value, cols - 1, 0))
        u_ref[j, :, 0:channels] = before.astype(BF16)
        u_ref[j, :, channels:2 * channels] = value.astype(BF16)
        u_ref[j, :, 2 * channels:3 * channels] = after.astype(BF16)


def conv_chunk(u_ref, w):
    _, cols, depth = u_ref.shape
    rows, split = CHUNK_ROWS * cols, w.shape[1] - LANES
    taps = [u_ref[dy:dy + CHUNK_ROWS].reshape(rows, depth) for dy in range(3)]
    main = jnp.dot(jnp.concatenate(taps, axis=1), w[:, 0:split], preferred_element_type=F32)
    both = jnp.concatenate([w[0:depth, split:], w[depth:2 * depth, split:]], axis=1)
    pair = jnp.dot(u_ref[0:CHUNK_ROWS + 1].reshape(rows + cols, depth), both, preferred_element_type=F32)
    third = jnp.dot(taps[2], w[2 * depth:, split:], preferred_element_type=F32)
    rest = pair[0:rows, 0:LANES] + pair[cols:, LANES:] + third
    return jnp.concatenate([main, rest], axis=1)


def conv_loop(order, ready, fill, finish, u_even, u_odd, w, arriving=False):
    def step(i, half, parity, u_now, u_next):
        after = jnp.minimum(i + 1, CHUNKS - 1)
        if arriving:
            finish(order(i), conv_chunk(u_now, w))
            ready(half, parity)
            fill(u_next, order(after))
        else:
            ready(half, parity)
            fill(u_next, order(after))
            finish(order(i), conv_chunk(u_now, w))

    def pair(half, carry):
        step(2 * half, half, 0, u_even, u_odd)
        step(2 * half + 1, half, 1, u_odd, u_even)
        return carry

    fill(u_even, order(jnp.int32(0)))
    lax.fori_loop(0, CHUNKS // 2, pair, 0)


def in_order(i):
    return i


def from_ends(i):
    return lax.rem(i + 1, 2) * lax.div(i, 2) + lax.rem(i, 2) * (CHUNKS - 1 - lax.div(i, 2))


def rows_of(ref, chunk, first=0):
    value = ref[pl.ds(chunk * CHUNK_ROWS + first, CHUNK_ROWS)]
    return value.reshape(value.shape[0] * value.shape[1], value.shape[2])


def send_edge_row(ref, send_sem, recv_sem, src_ref=None, src_row=None):
    rows = ref.shape[0] - 2
    core = position()[1]
    src = ref.at[rows - (rows - 1) * core] if src_ref is None else src_ref.at[src_row]
    return pltpu.make_async_remote_copy(
        src_ref=src, dst_ref=ref.at[(rows + 1) * core],
        send_sem=send_sem, recv_sem=recv_sem, device_id=partner_id(), device_id_type=MESH)


def first_kernel(count, x_ref, emb_ref, scale_ref, shift_ref, w_ref, tw_ref, out_ref, stat_ref, time_ref,
                 x_vmem, a_ref, h_ref, u_even, u_odd, w_vmem, tw_vmem, acc_ref, time_all, grp_recv, grp_total, st_send, st_recv,
                 load_sem, grp_ssem, grp_rsem, st_ssem, st_rsem, edge_ssem, edge_rsem, piece_ssem, piece_rsem, halo_ssem, halo_rsem):
    images, tile_rows, tile_cols, channels = x_ref.shape
    rows = 2 * tile_rows
    chip_x, core, chip_y = position()
    sp = lax.axis_index("sp")
    me = 2 * sp + chip_y
    image = 2 * chip_x + chip_y

    signal_all()
    x_load = pltpu.make_async_copy(x_ref, x_vmem, load_sem.at[0])
    x_load.start()
    weights = [pltpu.make_async_copy(w_ref.at[k], w_vmem.at[k], load_sem.at[1 + k]) for k in range(2)]
    tw_load = pltpu.make_async_copy(tw_ref, tw_vmem, load_sem.at[3])
    tw_load.start()

    def piece(part, source_core):
        low, high = PIECES[part]
        start = (1 - source_core) * low + source_core * (tile_rows - low - high)
        return pl.ds(start, high), pl.ds(1 + source_core * tile_rows + start, high)

    def piece_copies(k, part):
        to_x, to_y = lax.rem(chip_x + k // 2, 2), lax.rem(chip_y + k % 2, 2)
        src_rows, dst_rows = piece(part, core)
        src = x_ref.at[2 * to_x + to_y, src_rows]
        dst = a_ref.at[dst_rows, pl.ds(chip_y * tile_cols, tile_cols)]
        landed = piece_rsem.at[part, 2 * chip_y + core]
        remote = pltpu.make_async_remote_copy(
            src_ref=src, dst_ref=dst, send_sem=piece_ssem.at[k, part], recv_sem=landed,
            device_id={"sp": 2 * to_x + chip_x, "sp2": to_y}, device_id_type=MESH)
        return remote, pltpu.make_async_copy(src, dst, landed)

    def halo_copies(k):
        to_x, to_y = lax.rem(chip_x + k // 2, 2), lax.rem(chip_y + k % 2, 2)
        src = x_ref.at[2 * to_x + to_y, (tile_rows - 1) * core]
        dst = a_ref.at[(rows + 1) * chip_x, pl.ds(chip_y * tile_cols, tile_cols)]
        remote = pltpu.make_async_remote_copy(
            src_ref=src, dst_ref=dst, send_sem=halo_ssem.at[k], recv_sem=halo_rsem.at[chip_y],
            device_id={"sp": 2 * to_x + 1 - chip_x, "sp2": to_y}, device_id_type=MESH)
        return remote, pltpu.make_async_copy(src, dst, halo_rsem.at[chip_y])

    at_home = core == chip_x
    far_first = (3, 2, 1, 0)

    def send_piece(part):
        for k in far_first:
            remote, local = piece_copies(k, part)
            if k:
                remote.start()
            else:
                pl.when(at_home)(local.start)
                pl.when(jnp.logical_not(at_home))(remote.start)

    wait_all()

    @pl.when(jnp.logical_not(at_home))
    def _():
        for k in far_first:
            halo_copies(k)[0 if k else 1].start()

    send_piece(0)
    for copy in weights:
        copy.start()

    gather, spread = group_matrices(channels)
    x_load.wait()
    moments = []
    for i in range(images):
        acc_ref[...] = jnp.zeros_like(acc_ref)

        def add_row(row, carry):
            add_moments(acc_ref, x_vmem[i, row].astype(F32))
            return carry

        lax.fori_loop(0, tile_rows, add_row, 0)
        moments += [jnp.sum(acc_ref[0], axis=0, keepdims=True), jnp.sum(acc_ref[1], axis=0, keepdims=True)]
    grp_recv[me] = exact_dot(jnp.concatenate(moments, axis=0), gather)
    group_copies = []
    for k, (to_sp, to_y) in enumerate(others()):
        copy = pltpu.make_async_remote_copy(
            src_ref=grp_recv.at[me], dst_ref=grp_recv.at[me], send_sem=grp_ssem.at[k], recv_sem=grp_rsem.at[me],
            device_id={"sp": to_sp, "sp2": to_y}, device_id_type=MESH)
        copy.start()
        group_copies.append((copy, 2 * to_sp + to_y))

    for part in range(1, len(PIECES)):
        send_piece(part)

    tw_load.wait()
    emb = silu(emb_ref[...].astype(F32)).astype(BF16)
    for k in range(2):
        time_all[k, 0:images] = jnp.dot(emb, tw_vmem[k], preferred_element_type=F32)
    time_ref[...] = jnp.broadcast_to(time_all[1, pl.ds(image, 1)], time_ref.shape)
    time_vec = time_all[0, pl.ds(image, 1)]

    total = jnp.zeros((8, LANES), F32)
    for copy, _ in group_copies:
        copy.wait_send()
    for copy, sender in group_copies:
        pltpu.make_async_copy(grp_recv.at[sender], grp_recv.at[sender], grp_rsem.at[sender]).wait()
    for slot in range(8):
        total = total + grp_recv[slot]
    grp_total[...] = total
    mean, inv_std = spread_groups(grp_total[pl.ds(2 * image, 2)], spread, count)

    def wait_piece(part, source_core):
        for col in range(2):
            landed = a_ref.at[piece(part, source_core)[1], pl.ds(col * tile_cols, tile_cols)]
            pltpu.make_async_copy(landed, landed, piece_rsem.at[part, 2 * col + source_core]).wait()

    def ready(half, parity):
        if parity:
            for part in range(1, len(PIECES)):
                @pl.when(half + 1 == part)
                def _():
                    wait_piece(part, 0)
                    wait_piece(part, 1)

    top_edge, bottom_edge = core == 0, core == 1

    def norm(k, mean, inv_std):
        return mean, inv_std * scale_ref[k:k + 1].astype(F32), shift_ref[k:k + 1].astype(F32)

    params = norm(0, mean, inv_std)
    for col in range(2):
        landed = a_ref.at[(rows + 1) * (1 - core), pl.ds(col * tile_cols, tile_cols)]
        pltpu.make_async_copy(landed, landed, halo_rsem.at[col]).wait()
    wait_piece(0, 0)
    wait_piece(0, 1)
    acc_ref[...] = jnp.zeros_like(acc_ref)
    weights[0].wait()

    def finish_first(chunk, total):
        hidden = (total + time_vec).astype(BF16)
        h_ref[pl.ds(chunk * CHUNK_ROWS + 1, CHUNK_ROWS)] = hidden.reshape(CHUNK_ROWS, 2 * tile_cols, channels)
        add_moments(acc_ref, hidden.astype(F32))

    conv_loop(from_ends, ready, lambda u_ref, chunk: fill_chunk(u_ref, a_ref, chunk, params, top_edge, bottom_edge),
              finish_first, u_even, u_odd, w_vmem.at[0], arriving=True)

    edge = send_edge_row(h_ref, edge_ssem, edge_rsem)
    edge.start()
    st_send[0] = moment_rows(acc_ref)
    acc_ref[...] = jnp.zeros_like(acc_ref)
    weights[1].wait()
    second = norm(1, *norm_params(exchange(0, st_send, st_recv, st_ssem, st_rsem), count))
    edge.wait()

    def finish_second(chunk, total):
        new = (rows_of(a_ref, chunk, 1).astype(F32) + total).astype(BF16)
        out_ref[pl.ds(chunk * CHUNK_ROWS, CHUNK_ROWS)] = new.reshape(CHUNK_ROWS, 2 * tile_cols, channels)
        add_moments(acc_ref, new.astype(F32))

    conv_loop(in_order, lambda half, parity: None,
              lambda u_ref, chunk: fill_chunk(u_ref, h_ref, chunk, second, top_edge, bottom_edge),
              finish_second, u_even, u_odd, w_vmem.at[1])
    stat_ref[...] = moment_rows(acc_ref)

    @pl.when(jnp.logical_not(at_home))
    def _():
        for k in (1, 2, 3):
            halo_copies(k)[0].wait_send()

    for part in range(len(PIECES)):
        for k in range(4):
            remote, _ = piece_copies(k, part)
            if k:
                remote.wait_send()
            else:
                pl.when(jnp.logical_not(at_home))(remote.wait_send)


def second_kernel(count, a_hbm, stat_in, time_ref, scale_ref, shift_ref, w_ref, out_ref,
                  a_ref, h_ref, u_even, u_odd, w_vmem, acc_ref, res_ref, st_send, st_recv,
                  load_sem, st_ssem, st_rsem, edge_ssem, edge_rsem, tile_ssem, tile_rsem):
    rows, cols, channels = res_ref.shape
    tile_rows, tile_cols = rows // 2, cols // 2
    chip_x, core, chip_y = position()
    sp = lax.axis_index("sp")
    image = 2 * chip_x + chip_y

    signal_all()
    a_load = pltpu.make_async_copy(a_hbm, a_ref.at[pl.ds(1, rows)], load_sem.at[0])
    a_load.start()
    weights = [pltpu.make_async_copy(w_ref.at[2 + k], w_vmem.at[k], load_sem.at[1 + k]) for k in range(2)]
    for copy in weights:
        copy.start()
    st_send[0] = stat_in[...]
    acc_ref[...] = jnp.zeros_like(acc_ref)
    wait_all()
    edge = send_edge_row(a_ref, edge_ssem.at[0], edge_rsem.at[0], a_hbm, (rows - 1) * (1 - core))
    edge.start()
    top_edge, bottom_edge = core == 0, core == 1

    def norm(k, sums):
        mean, inv_std = norm_params(sums, count)
        return mean, inv_std * scale_ref[3 + k:4 + k].astype(F32), shift_ref[3 + k:4 + k].astype(F32)

    params = norm(0, exchange(0, st_send, st_recv, st_ssem, st_rsem))
    a_load.wait()
    edge.wait()
    weights[0].wait()
    time_vec = time_ref[0:1]

    def finish_first(chunk, total):
        hidden = (total + time_vec).astype(BF16)
        h_ref[pl.ds(chunk * CHUNK_ROWS + 1, CHUNK_ROWS)] = hidden.reshape(CHUNK_ROWS, cols, channels)
        add_moments(acc_ref, hidden.astype(F32))

    conv_loop(in_order, lambda half, parity: None,
              lambda u_ref, chunk: fill_chunk(u_ref, a_ref, chunk, params, top_edge, bottom_edge),
              finish_first, u_even, u_odd, w_vmem.at[0])

    edge = send_edge_row(h_ref, edge_ssem.at[1], edge_rsem.at[1])
    edge.start()
    st_send[1] = moment_rows(acc_ref)
    weights[1].wait()
    second = norm(1, exchange(1, st_send, st_recv, st_ssem, st_rsem))
    edge.wait()

    per_tile = CHUNKS // 2

    def home_copies(chunk, col):
        to_sp = 2 * core + lax.div(chunk, per_tile)
        slot = lax.rem(chunk, per_tile)
        here = (to_sp == sp) & (chip_y == col)
        src = res_ref.at[pl.ds(chunk * CHUNK_ROWS, CHUNK_ROWS), pl.ds(col * tile_cols, tile_cols)]
        dst = out_ref.at[image, pl.ds(slot * CHUNK_ROWS, CHUNK_ROWS)]
        landed = tile_rsem.at[image, slot]
        remote = pltpu.make_async_remote_copy(
            src_ref=src, dst_ref=dst, send_sem=tile_ssem.at[chunk, col], recv_sem=landed,
            device_id={"sp": to_sp, "sp2": col}, device_id_type=MESH)
        return here, remote, pltpu.make_async_copy(src, dst, landed)

    def send_home(chunk):
        for col in range(2):
            here, remote, local = home_copies(chunk, col)
            pl.when(here)(local.start)
            pl.when(jnp.logical_not(here))(remote.start)

    def ready(half, parity):
        if parity:
            send_home(2 * half)
        else:
            pl.when(half > 0)(lambda: send_home(2 * half - 1))

    def finish_second(chunk, total):
        new = (rows_of(a_ref, chunk, 1).astype(F32) + total).astype(BF16)
        res_ref[pl.ds(chunk * CHUNK_ROWS, CHUNK_ROWS)] = new.reshape(CHUNK_ROWS, cols, channels)

    conv_loop(in_order, ready, lambda u_ref, chunk: fill_chunk(u_ref, h_ref, chunk, second, top_edge, bottom_edge),
              finish_second, u_even, u_odd, w_vmem.at[1])
    send_home(jnp.int32(CHUNKS - 1))
    for chunk in range(CHUNKS):
        for col in range(2):
            here, remote, _ = home_copies(jnp.int32(chunk), col)
            pl.when(jnp.logical_not(here))(remote.wait_send)
    for slot in range(4):
        for part in range(per_tile):
            landed = out_ref.at[slot, pl.ds(part * CHUNK_ROWS, CHUNK_ROWS)]
            pltpu.make_async_copy(landed, landed, tile_rsem.at[slot, part]).wait()


def attention_kernel(norm_idx, count, logit_scale, a_hbm, stat_in, scale_ref, shift_ref, w_hbm, wo_hbm,
                     out_ref, stat_ref, a_ref, n_ref, q_ref, k_ref, v_ref, s_even, s_odd, peak_ref, total_ref, part_ref, o_ref,
                     wq_ref, wk_ref, wv_ref, wo_ref, acc_ref,
                     st_send, st_recv, load_sem, st_ssem, st_rsem, kv_ssem, kv_rsem):
    tokens, channels = a_ref.shape
    heads, head_dim, _ = v_ref.shape
    pairs = ((a_hbm, a_ref), (w_hbm.at[1], wk_ref), (w_hbm.at[2], wv_ref), (w_hbm.at[0], wq_ref), (wo_hbm, wo_ref))
    loads = [pltpu.make_async_copy(src, dst, load_sem.at[i]) for i, (src, dst) in enumerate(pairs)]
    for load in loads:
        load.start()

    def clear_padding():
        for head in range(heads):
            k_ref[head, 0:tokens, head_dim:] = jnp.zeros((tokens, LANES - head_dim), BF16)
            q_ref[head, head_dim:] = jnp.zeros((LANES - head_dim, tokens), BF16)

    st_send[0] = stat_in[...]
    barrier_pair()
    sums = exchange(0, st_send, st_recv, st_ssem, st_rsem, clear_padding)
    mean, inv_std = norm_params(sums, count)
    gain = inv_std * scale_ref[norm_idx:norm_idx + 1].astype(F32)
    shift = shift_ref[norm_idx:norm_idx + 1].astype(F32)
    for load in loads[:3]:
        load.wait()

    step = TOKEN_BLOCK
    chunks = tokens // step
    transposed = (((1,), (1,)), ((), ()))

    def head_copy(which, head, chunk=None):
        first, size = (0, tokens) if chunk is None else (pl.multiple_of(chunk * step, step), step)
        src, dst = pl.ds(first, size), pl.ds(tokens + first, size)
        if which:
            src_ref, dst_ref = v_ref.at[head, :, src], v_ref.at[head, :, dst]
        else:
            src_ref, dst_ref = k_ref.at[head, src], k_ref.at[head, dst]
        slot = head if chunk is None else heads + chunk
        return pltpu.make_async_remote_copy(
            src_ref=src_ref, dst_ref=dst_ref, send_sem=kv_ssem.at[which, slot], recv_sem=kv_rsem.at[which, slot],
            device_id=partner_id(), device_id_type=MESH)

    def both(act, head, chunk=None):
        for which in range(2):
            getattr(head_copy(which, head, chunk), act)()

    def key_values(i, carry):
        here = pl.ds(pl.multiple_of(i * step, step), step)
        normed = ((a_ref[here].astype(F32) - mean) * gain + shift).astype(BF16)
        n_ref[here] = normed
        part = lax.dot_general(normed, wk_ref[...], transposed, preferred_element_type=F32).astype(BF16)
        for head in range(heads):
            k_ref[head, here, 0:head_dim] = part[:, head * head_dim:(head + 1) * head_dim]
        part = lax.dot_general(wv_ref[...], normed, transposed, preferred_element_type=F32).astype(BF16)
        for head in range(heads):
            v_ref[head, :, here] = part[head * head_dim:(head + 1) * head_dim]

        @pl.when(i > 0)
        def _():
            both("start", 0, i - 1)
        return carry

    lax.fori_loop(0, chunks, key_values, 0)
    loads[3].wait()

    def query_chunk(i):
        here = pl.ds(pl.multiple_of(i * step, step), step)
        part = lax.dot_general(wq_ref[...], n_ref[here], transposed, preferred_element_type=F32).astype(BF16)
        for head in range(heads):
            q_ref[head, 0:head_dim, here] = part[head * head_dim:(head + 1) * head_dim]

    def queries(i, carry):
        query_chunk(2 * i)
        query_chunk(2 * i + 1)

        @pl.when(i == 0)
        def _():
            both("start", 0, chunks - 1)
            for head in range(1, heads):
                both("start", head)
        return carry

    lax.fori_loop(0, chunks // 2, queries, 0)

    for i in range(chunks):
        both("wait_recv", 0, i)

    blocks = tokens // QUERY_BLOCK
    key_blocks = 2 * tokens // KEY_BLOCK

    def fold(value, combine):
        return combine(value.reshape(KEY_BLOCK // 8, 8, QUERY_BLOCK), axis=0)

    def place_of(block):
        first = pl.multiple_of(lax.rem(block, blocks) * QUERY_BLOCK, QUERY_BLOCK)
        return lax.div(block, blocks), pl.ds(first, QUERY_BLOCK)

    def keys_of(j):
        return slice(j * KEY_BLOCK, (j + 1) * KEY_BLOCK)

    def score(j, head, query, s_ref, peak):
        scores = jnp.dot(k_ref[head, keys_of(j)], query, preferred_element_type=F32)
        s_ref[keys_of(j)] = scores
        piece = fold(scores, jnp.max)
        return piece if peak is None else jnp.maximum(peak, piece)

    def absorb(j, head, peak, s_ref, state):
        weights = jnp.exp2((s_ref[keys_of(j)] - peak) * logit_scale)
        total = fold(weights, jnp.sum)
        attended = jnp.dot(v_ref[head, :, keys_of(j)], weights.astype(BF16), preferred_element_type=F32)
        return (total, attended) if state is None else (state[0] + total, state[1] + attended)

    def finish_block(block, peak, s_ref, state):
        head, here = place_of(block)
        total, attended = absorb(key_blocks - 1, head, peak, s_ref, state)
        total = jnp.sum(total, axis=0, keepdims=True)
        o_ref[pl.ds(pl.multiple_of(head * head_dim, 16), head_dim), here] = (attended / total).astype(BF16)

    def peak_of(slot):
        return jnp.max(peak_ref[slot], axis=0, keepdims=True)

    def advance(i, s_ref, s_next, slot, state):
        head, _ = place_of(i)
        next_head, next_here = place_of(jnp.minimum(i + 1, heads * blocks - 1))
        query = q_ref[next_head, :, next_here]
        peak, next_peak, new_state = peak_of(slot), None, None
        for j in range(key_blocks):
            next_peak = score(j, next_head, query, s_next, next_peak)
            if j == 0:
                finish_block(jnp.maximum(i - 1, 0), peak_of(1 - slot), s_next, state)
            if j:
                new_state = absorb(j - 1, head, peak, s_ref, new_state)
        peak_ref[1 - slot] = next_peak
        return new_state

    s_odd[keys_of(key_blocks - 1)] = jnp.zeros((KEY_BLOCK, QUERY_BLOCK), F32)
    peak_ref[1] = jnp.zeros((8, QUERY_BLOCK), F32)
    total_ref[...] = jnp.zeros_like(total_ref)
    part_ref[...] = jnp.zeros_like(part_ref)
    query = q_ref[0, :, 0:QUERY_BLOCK]
    first_peak = None
    for j in range(key_blocks):
        first_peak = score(j, 0, query, s_even, first_peak)
    peak_ref[0] = first_peak

    def attend(head, carry):
        pl.when(head + 1 < heads)(lambda: both("wait_recv", head + 1))
        state = (total_ref[...], part_ref[...])
        for j in range(0, blocks, 2):
            state = advance(blocks * head + j, s_even, s_odd, 0, state)
            state = advance(blocks * head + j + 1, s_odd, s_even, 1, state)
        total_ref[...], part_ref[...] = state
        return carry

    lax.fori_loop(0, heads, attend, 0)
    finish_block(jnp.int32(heads * blocks - 1), peak_of(1), s_odd, (total_ref[...], part_ref[...]))
    for i in range(chunks):
        both("wait_send", 0, i)
    for head in range(1, heads):
        both("wait_send", head)
    loads[4].wait()
    acc_ref[...] = jnp.zeros_like(acc_ref)

    def project_chunk(i):
        here = pl.ds(pl.multiple_of(i * step, step), step)
        added = lax.dot_general(o_ref[:, here], wo_ref[...], (((0,), (0,)), ((), ())), preferred_element_type=F32)
        new = (a_ref[here].astype(F32) + added).astype(BF16)
        a_ref[here] = new
        add_moments(acc_ref, new.astype(F32))

    def leave(i):
        here = pl.ds(pl.multiple_of(i * 2 * step, 2 * step), 2 * step)
        return pltpu.make_async_copy(a_ref.at[here], out_ref.at[here], load_sem.at[i])

    def project(i, carry):
        pl.when(i > 0)(lambda: leave(i - 1).start())
        project_chunk(2 * i)
        project_chunk(2 * i + 1)
        return carry

    lax.fori_loop(0, chunks // 2, project, 0)
    stat_ref[...] = moment_rows(acc_ref)
    leave(chunks // 2 - 1).start()
    for i in range(chunks // 2):
        leave(i).wait()


VMEM_SPEC = pl.BlockSpec(memory_space=pltpu.VMEM)
ANY_SPEC = pl.BlockSpec(memory_space=pl.ANY)


def params(collective_id):
    return pltpu.CompilerParams(collective_id=collective_id, has_side_effects=True, vmem_limit_bytes=60 * 2**20)


def conv_scratch(rows, cols, channels):
    return [
        pltpu.VMEM((rows + 2, cols, channels), BF16),
        pltpu.VMEM((rows + 2, cols, channels), BF16),
        pltpu.VMEM((CHUNK_ROWS + 2, cols, 3 * channels), BF16),
        pltpu.VMEM((CHUNK_ROWS + 2, cols, 3 * channels), BF16),
        pltpu.VMEM((2, 9 * channels, channels), BF16),
    ]


def first_call(count, rows, cols, x, time_emb, scale, shift, w, time_w):
    channels = x.shape[3]
    dma = pltpu.SemaphoreType.DMA
    return pl.pallas_call(
        functools.partial(first_kernel, count),
        out_shape=[
            jax.ShapeDtypeStruct((rows, cols, channels), BF16),
            jax.ShapeDtypeStruct((8, channels), F32),
            jax.ShapeDtypeStruct((8, channels), F32),
        ],
        in_specs=[ANY_SPEC, VMEM_SPEC, VMEM_SPEC, VMEM_SPEC, ANY_SPEC, ANY_SPEC],
        out_specs=[VMEM_SPEC, VMEM_SPEC, VMEM_SPEC],
        scratch_shapes=[pltpu.VMEM(x.shape, BF16)] + conv_scratch(rows, cols, channels) + [
            pltpu.VMEM(time_w.shape, BF16),
            pltpu.VMEM((2, 8, channels), F32),
            pltpu.VMEM((2, 8, channels), F32),
            pltpu.VMEM((8, 8, LANES), F32),
            pltpu.VMEM((8, LANES), F32),
            pltpu.VMEM((1, 8, channels), F32),
            pltpu.VMEM((1, 8, channels), F32),
            dma((4,)), dma((7,)), dma((8,)), dma((1,)), dma((1,)), dma, dma,
            dma((4, len(PIECES))), dma((len(PIECES), 4)), dma((4,)), dma((2,)),
        ],
        compiler_params=params(0),
        name="res_first",
    )(x, time_emb, scale, shift, w, time_w)


def second_call(count, tile_shape, a, stats, time_vec, scale, shift, w):
    rows, cols, channels = a.shape
    dma = pltpu.SemaphoreType.DMA
    return pl.pallas_call(
        functools.partial(second_kernel, count),
        out_shape=jax.ShapeDtypeStruct(tile_shape, BF16),
        in_specs=[ANY_SPEC, VMEM_SPEC, VMEM_SPEC, VMEM_SPEC, VMEM_SPEC, ANY_SPEC],
        out_specs=ANY_SPEC,
        scratch_shapes=conv_scratch(rows, cols, channels) + [
            pltpu.VMEM((2, 8, channels), F32),
            pltpu.VMEM((rows, cols, channels), BF16),
            pltpu.VMEM((2, 8, channels), F32),
            pltpu.VMEM((2, 8, channels), F32),
            dma((3,)), dma((2,)), dma((2,)), dma((2,)), dma((2,)), dma((CHUNKS, 2)), dma((4, CHUNKS // 2)),
        ],
        compiler_params=params(2),
        name="res_second",
    )(a, stats, time_vec, scale, shift, w)


def copy_kernel(src_ref, out_ref, buf_ref, in_sem, out_sem):
    parts = [(i, slice(j * 4, (j + 1) * 4)) for i in range(src_ref.shape[0]) for j in range(src_ref.shape[1] // 4)]
    reads = [pltpu.make_async_copy(src_ref.at[i, rows], buf_ref.at[i, rows], in_sem.at[n]) for n, (i, rows) in enumerate(parts)]
    writes = [pltpu.make_async_copy(buf_ref.at[i, rows], out_ref.at[i, rows], out_sem.at[n]) for n, (i, rows) in enumerate(parts)]
    for read in reads:
        read.start()
    for read, write in zip(reads, writes):
        read.wait()
        write.start()
    for write in writes:
        write.wait()


def copy_call(src):
    parts = src.shape[0] * (src.shape[1] // 4)
    return pl.pallas_call(
        copy_kernel,
        out_shape=jax.ShapeDtypeStruct(src.shape, src.dtype),
        in_specs=[ANY_SPEC],
        out_specs=ANY_SPEC,
        scratch_shapes=[pltpu.VMEM(src.shape, src.dtype), pltpu.SemaphoreType.DMA((parts,)), pltpu.SemaphoreType.DMA((parts,))],
        name="copy_out",
    )(src)


def attention_call(norm_idx, count, heads, a, stats, scale, shift, w, wo):
    tokens, channels = a.shape
    head_dim = channels // heads
    logit_scale = head_dim ** -0.5 * 1.4426950408889634
    return pl.pallas_call(
        functools.partial(attention_kernel, norm_idx, count, logit_scale),
        out_shape=[jax.ShapeDtypeStruct((tokens, channels), BF16), jax.ShapeDtypeStruct((8, channels), F32)],
        in_specs=[ANY_SPEC, VMEM_SPEC, VMEM_SPEC, VMEM_SPEC, ANY_SPEC, ANY_SPEC],
        out_specs=[ANY_SPEC, VMEM_SPEC],
        scratch_shapes=[
            pltpu.VMEM((tokens, channels), BF16),
            pltpu.VMEM((tokens, channels), BF16),
            pltpu.VMEM((heads, LANES, tokens), BF16),
            pltpu.VMEM((heads, 2 * tokens, LANES), BF16),
            pltpu.VMEM((heads, head_dim, 2 * tokens), BF16),
            pltpu.VMEM((2 * tokens, QUERY_BLOCK), F32),
            pltpu.VMEM((2 * tokens, QUERY_BLOCK), F32),
            pltpu.VMEM((2, 8, QUERY_BLOCK), F32),
            pltpu.VMEM((8, QUERY_BLOCK), F32),
            pltpu.VMEM((head_dim, QUERY_BLOCK), F32),
            pltpu.VMEM((channels, tokens), BF16),
            pltpu.VMEM((channels, channels), BF16),
            pltpu.VMEM((channels, channels), BF16),
            pltpu.VMEM((channels, channels), BF16),
            pltpu.VMEM((channels, channels), BF16),
            pltpu.VMEM((2, 8, channels), F32),
            pltpu.VMEM((1, 8, channels), F32),
            pltpu.VMEM((1, 8, channels), F32),
            pltpu.SemaphoreType.DMA((5,)),
            pltpu.SemaphoreType.DMA((1,)),
            pltpu.SemaphoreType.DMA((1,)),
            pltpu.SemaphoreType.DMA((2, heads + tokens // TOKEN_BLOCK)),
            pltpu.SemaphoreType.DMA((2, heads + tokens // TOKEN_BLOCK)),
        ],
        compiler_params=params(1),
        name="attention",
    )(a, stats, scale, shift, w, wo)


def solution(mesh):
    lat_spec = P("dp", "sp", "sp2", None)

    def local(x, time_emb, gn_scale, gn_shift, conv_w, time_w, w_qkv, w_out):
        images, tile_rows, tile_cols, channels = x.shape
        rows, cols = 2 * tile_rows, 2 * tile_cols
        count = 2 * rows * cols * (channels // GROUPS)
        heads = w_out.shape[0]
        w = conv_w.reshape(4, 9 * channels, channels)
        qkv = jnp.transpose(w_qkv, (0, 2, 3, 1)).reshape(3, channels, channels)
        wo = w_out.reshape(channels, channels)
        first, stats, time_vec = first_call(count, rows, cols, x, time_emb, gn_scale, gn_shift, w, time_w)
        middle, stats = attention_call(2, count, heads, first.reshape(rows * cols, channels), stats, gn_scale, gn_shift, qkv, wo)
        return copy_call(second_call(count, x.shape, middle.reshape(rows, cols, channels), stats, time_vec, gn_scale, gn_shift, w))

    return jax.shard_map(local, mesh=mesh, in_specs=(lat_spec, P("dp", None), P(), P(), P(), P(), P(), P()), out_specs=lat_spec, check_vma=False)
```
